32 devices in a mesh: group: 2 (over y), sample: 16 (over z, x, core).
Axes of the slice: x: 2, y: 2, z: 4, core: 2. Of those that a mesh axis runs over, the one named last changes fastest.
Arguments:
- patches: bfloat16 [16, 256, 588], P('group', 'sample'), parts along dimension 0, may hold values from -6 to 6
- patch_weight: bfloat16 [16, 588, 1280], P('sample'), may hold values from -0.25 to 0.25
- cls_token: bfloat16 [16, 1280], P('sample'), may hold values from -6 to 6
- pos_embed: bfloat16 [16, 257, 1280], P('sample'), may hold values from -3 to 3
- ln1_gain: float32 [16, 1280], P('sample'), may hold values from 0.5 to 1.5
- ln1_bias: float32 [16, 1280], P('sample'), may hold values from -2 to 2
- w_query: bfloat16 [16, 1280, 640], P('sample'), may hold values from -8 to 8
- w_key: bfloat16 [16, 1280, 640], P('sample'), may hold values from -2 to 2
- w_value: bfloat16 [16, 1280, 640], P('sample'), may hold values from -0.15625 to 0.15625
- w_out: bfloat16 [16, 640, 1280], P('sample'), may hold values from -1 to 1
- lnf_gain: float32 [16, 1280], P('sample'), may hold values from 0.5 to 1.5
- lnf_bias: float32 [16, 1280], P('sample'), may hold values from -2 to 2
- head_w: bfloat16 [16, 1280, 1000], P('sample'), may hold values from -0.875 to 0.875
- head_bias: float32 [16, 1000], P('sample'), may hold values from -6 to 290
Outputs:
- predictive: float32 [16, 1000], P('group'), parts along dimension 0
The draws below stay inside these ranges and needn't reach their ends.
There are 2 independent parts, one for each index of `group`. The reference program is written for one: setup_inputs(seed, part) draws one part's arguments, and reference() takes and returns one part's arrays. A program takes and returns all parts, laid end to end along the dimension named above; an argument that names none is the same for every part. Nothing has to cross between parts.
All inputs are finite; a program needn't handle non-finite values.
Results may differ from the reference program's by a relative error of at most 0.0023.
Values may be sent and summed in bfloat16 or wider, within the bound.
A program may use at most 64 MiB of HBM per device.

```python
import math
import jax
import jax.numpy as jnp
from jax import lax

D = 1280
HEADS = 8
HEAD_DIM = 80
PATCH_DIM = 588
PATCHES = 256
CLASSES = 1000
IMAGES = 8
TOKENS = 257
SAMPLES = 16


def key_matrix(key):
    drawn_keys = jax.random.truncated_normal(jax.random.fold_in(key, 7101), -6.0, 6.0, (SAMPLES, D, HEADS * HEAD_DIM), jnp.float32)
    return drawn_keys * D ** (-0.5)


def draw_w_key(key, part):
    return key_matrix(key).astype(jnp.bfloat16)


def draw_w_query(key, part):
    drawn_query = jax.random.truncated_normal(jax.random.fold_in(key, 7102), -6.0, 6.0, (SAMPLES, D, HEADS * HEAD_DIM), jnp.float32) * D ** (-0.5)
    return drawn_query.astype(jnp.bfloat16)


def draw_head_bias(key, part):
    values_drawn = jax.random.truncated_normal(jax.random.fold_in(key, 7201), -6.0, 6.0, (SAMPLES, CLASSES), jnp.float32)
    return values_drawn


def level_of(stream_key, dims, cuts, smallest, high):
    level, own = 1.0, jax.random.fold_in(stream_key, 6)
    for dim, shards_of in cuts:
        heights = jnp.exp(jax.random.uniform(jax.random.fold_in(own, dim), (shards_of,), jnp.float32, smallest / len(cuts), high / len(cuts)))
        level = level * jnp.repeat(heights, dims[dim] // shards_of).reshape([-1 if axis == dim else 1 for axis in range(len(dims))])
    return level


def noise(own_key, shape, scale, most, pieces=(), dtype=jnp.bfloat16):
    drawn = scale * jax.random.normal(own_key, shape, jnp.float32)
    if pieces:
        drawn = drawn * level_of(own_key, shape, pieces, -0.22, 0.18)
    return jnp.clip(drawn, -most, most).astype(dtype)


def setup_inputs(seed: int = 0, part: int = 0) -> dict:
    keys = jax.random.split(jax.random.key(seed), 15)
    part_splits = jax.random.split(jax.random.fold_in(keys[14], part), 15)
    patches = noise(part_splits[0], (IMAGES, PATCHES, PATCH_DIM), 1.0, 6.0, ((1, 16),))
    patch_weight = noise(keys[1], (SAMPLES, PATCH_DIM, D), PATCH_DIM ** -0.5, 0.25, ((0, 16),))
    cls_token = noise(keys[2], (SAMPLES, D), 1.0, 6.0, ((0, 16),))
    pos_embed = noise(keys[3], (SAMPLES, TOKENS, D), 0.5, 3.0, ((0, 16),))
    ln1_gain = jnp.clip(1.0 + 0.1 * jax.random.normal(keys[4], (SAMPLES, D), jnp.float32), 0.5, 1.5)
    ln1_bias = noise(keys[5], (SAMPLES, D), 0.3, 2.0, ((0, 16),), jnp.float32)
    w_query = draw_w_query(jax.random.fold_in(keys[14], 71), part)
    w_key = draw_w_key(jax.random.fold_in(keys[14], 71), part)
    w_value = noise(keys[8], (SAMPLES, D, HEADS * HEAD_DIM), D ** -0.5, 0.15625, ((0, 16),))
    w_out = noise(keys[9], (SAMPLES, HEADS * HEAD_DIM, D), (HEADS * HEAD_DIM // 16) ** -0.5, 1.0, ((0, 16),))
    lnf_gain = jnp.clip(1.0 + 0.1 * jax.random.normal(keys[10], (SAMPLES, D), jnp.float32), 0.5, 1.5)
    lnf_bias = noise(keys[11], (SAMPLES, D), 0.3, 2.0, ((0, 16),), jnp.float32)
    head_w = noise(keys[12], (SAMPLES, D, CLASSES), (D // 25) ** -0.5, 0.875, ((0, 16),))
    head_bias = draw_head_bias(jax.random.fold_in(keys[14], 71), part)
    return dict(patches=patches, patch_weight=patch_weight, cls_token=cls_token, pos_embed=pos_embed, ln1_gain=ln1_gain, ln1_bias=ln1_bias, w_query=w_query, w_key=w_key, w_value=w_value, w_out=w_out, lnf_gain=lnf_gain, lnf_bias=lnf_bias, head_w=head_w, head_bias=head_bias)


epsilon = 1e-06

def layer_norm(values, gain, shift):
    center = values - lax.optimization_barrier(jnp.mean(values, axis=-1, keepdims=True))
    spread = lax.optimization_barrier(jnp.mean(center * center, axis=-1, keepdims=True))
    return center * lax.rsqrt(spread + epsilon) * gain + shift

def one_sample(patches, packed):
    patch_weight, cls_token, pos_embed, ln1_gain, ln1_bias, w_query, w_key, w_value, w_out, lnf_gain, lnf_bias, head_w, head_bias = packed
    width = patch_weight.shape[1]
    image_count = patches.shape[0]
    flat = patches.reshape(-1, patches.shape[2])
    tokens = jnp.dot(flat, patch_weight, preferred_element_type=jnp.float32).reshape(image_count, -1, width)
    tokens = tokens + pos_embed[1:].astype(jnp.float32)[None]
    leading = cls_token.astype(jnp.float32) + pos_embed[0].astype(jnp.float32)
    lead_norm = layer_norm(leading, ln1_gain, ln1_bias).astype(jnp.bfloat16)
    token_norm = layer_norm(tokens, ln1_gain, ln1_bias).astype(jnp.bfloat16)
    all_norm = jnp.concatenate([jnp.broadcast_to(lead_norm[None, None], (image_count, 1, width)), token_norm], axis=1)
    key_rows = jnp.dot(all_norm.reshape(-1, width), w_key, preferred_element_type=jnp.float32).astype(jnp.bfloat16)
    value_rows = jnp.dot(all_norm.reshape(-1, width), w_value, preferred_element_type=jnp.float32).astype(jnp.bfloat16)
    key_rows = key_rows.reshape(image_count, -1, HEADS, HEAD_DIM)
    value_rows = value_rows.reshape(image_count, -1, HEADS, HEAD_DIM)
    query = jnp.dot(lead_norm[None], w_query, preferred_element_type=jnp.float32).astype(jnp.bfloat16)
    query = query.reshape(HEADS, HEAD_DIM)
    scores = jnp.einsum('hd,ithd->iht', query.astype(jnp.float32), key_rows.astype(jnp.float32)) / math.sqrt(HEAD_DIM)
    attention = jax.nn.softmax(scores, axis=-1).astype(jnp.bfloat16)
    mixed = jnp.einsum('iht,ithd->ihd', attention.astype(jnp.float32), value_rows.astype(jnp.float32))
    mixed = mixed.astype(jnp.bfloat16).reshape(image_count, HEADS * HEAD_DIM)
    hidden = leading[None] + jnp.dot(mixed, w_out, preferred_element_type=jnp.float32)
    final = layer_norm(hidden, lnf_gain, lnf_bias).astype(jnp.bfloat16)
    logits = jnp.dot(final, head_w, preferred_element_type=jnp.float32) + head_bias
    return jax.nn.log_softmax(logits, axis=-1)

def reference(patches, patch_weight, cls_token, pos_embed, ln1_gain, ln1_bias, w_query, w_key, w_value, w_out, lnf_gain, lnf_bias, head_w, head_bias):
    packed = (patch_weight, cls_token, pos_embed, ln1_gain, ln1_bias, w_query, w_key, w_value, w_out, lnf_gain, lnf_bias, head_w, head_bias)
    logp = lax.map(lambda single: one_sample(patches, single), packed)
    peak = lax.optimization_barrier(jnp.max(logp, axis=0))
    total = lax.optimization_barrier(jnp.sum(jnp.exp(logp - peak[None]), axis=0))
    return peak + jnp.log(total) - math.log(logp.shape[0])
```

```python
import functools
import math

import jax
import jax.numpy as jnp
from jax import lax
from jax.experimental import pallas as pl
from jax.experimental.pallas import tpu as pltpu
from jax.sharding import PartitionSpec as P

HEAD_DIM = 80


epsilon = 1e-06


def combined_all(part, axis, combine):
    gathered = jax.tree.map(lambda a: lax.all_gather(a, axis), part)

    def take(source):
        return jax.tree.map(lambda a: lax.dynamic_index_in_dim(a, source, 0, False), gathered)

    return lax.fori_loop(
        1, lax.axis_size(axis), lambda source, state: combine(state, take(source)), take(0)
    )


def layer_norm(values, gain, shift):
    center = values - jnp.mean(values, axis=-1, keepdims=True)
    spread = jnp.mean(center * center, axis=-1, keepdims=True)
    return center * lax.rsqrt(spread + epsilon) * gain + shift


def shards(
    patches,
    patch_weight,
    cls_token,
    pos_embed,
    ln1_gain,
    ln1_bias,
    w_query,
    w_key,
    w_value,
    w_out,
    lnf_gain,
    lnf_bias,
    head_w,
    head_bias,
):
    embed_weight = patch_weight[0]
    position = pos_embed[0]
    gain_first = ln1_gain[0]
    bias_first = ln1_bias[0]
    query_weight = w_query[0]
    pair_weight = jnp.concatenate([w_key[0], w_value[0]], axis=1)
    out_weight = w_out[0]
    width = embed_weight.shape[1]
    inner = query_weight.shape[1]
    head_count = inner // HEAD_DIM
    leading = cls_token[0].astype(jnp.float32) + position[0].astype(jnp.float32)
    lead_norm = layer_norm(leading, gain_first, bias_first).astype(jnp.bfloat16)
    lead_pair = jnp.dot(lead_norm[None], pair_weight, preferred_element_type=jnp.float32).astype(
        jnp.bfloat16
    )
    query = jnp.dot(lead_norm[None], query_weight, preferred_element_type=jnp.float32).astype(
        jnp.bfloat16
    )
    query = query.reshape(head_count, HEAD_DIM)
    portion = lax.all_gather(patches, "sample", axis=1, tiled=True)
    image_count = portion.shape[0]
    row_count = portion.shape[1]
    flat = portion.reshape(-1, portion.shape[2])
    tokens = jnp.dot(flat, embed_weight, preferred_element_type=jnp.float32).reshape(
        image_count, row_count, width
    )
    placed = lax.dynamic_slice_in_dim(position, 1, row_count, 0)
    tokens = tokens + placed.astype(jnp.float32)[None]
    normed = layer_norm(tokens, gain_first, bias_first).astype(jnp.bfloat16)
    paired = jnp.dot(normed.reshape(-1, width), pair_weight, preferred_element_type=jnp.float32)
    key_values = paired.astype(jnp.bfloat16).reshape(image_count, row_count, 2 * inner)
    image_count = key_values.shape[0]
    lead_rows = jnp.broadcast_to(lead_pair[None], (image_count, 1, 2 * inner))
    full_rows = jnp.concatenate([lead_rows, key_values], axis=1)
    key_rows = full_rows[:, :, :inner].reshape(image_count, -1, head_count, HEAD_DIM)
    value_rows = full_rows[:, :, inner:].reshape(image_count, -1, head_count, HEAD_DIM)
    scores = jnp.einsum(
        "hd,ithd->iht", query, key_rows, preferred_element_type=jnp.float32
    ) / math.sqrt(HEAD_DIM)
    attention = jax.nn.softmax(scores, axis=-1).astype(jnp.bfloat16)
    mixed = jnp.einsum("iht,ithd->ihd", attention, value_rows, preferred_element_type=jnp.float32)
    mixed = mixed.astype(jnp.bfloat16).reshape(image_count, inner)
    hidden = leading[None] + jnp.dot(mixed, out_weight, preferred_element_type=jnp.float32)
    final = layer_norm(hidden, lnf_gain[0], lnf_bias[0]).astype(jnp.bfloat16)
    logits = jnp.dot(final, head_w[0], preferred_element_type=jnp.float32) + head_bias[0]
    logp = jax.nn.log_softmax(logits, axis=-1)
    count = lax.axis_size("sample")

    def combine(earlier, later):
        highest = jnp.maximum(earlier[0], later[0])
        summed = earlier[1] * jnp.exp(earlier[0] - highest) + later[1] * jnp.exp(later[0] - highest)
        return (highest, summed)

    peak, total = combined_all((logp, jnp.ones_like(logp)), "sample", combine)
    return peak + jnp.log(total) - math.log(count)


MESH = pl.DeviceIdType.MESH
PLANE = 4
LINE = 4
TILE_ROWS = 16
LOWEST = -1e30


def split_in_two(values):
    high = values.astype(jnp.bfloat16)
    low = (values - high.astype(jnp.float32)).astype(jnp.bfloat16)
    return jnp.concatenate([high, low], axis=0)


def pick(index, values):
    packed = sum(value << (3 * place) for place, value in enumerate(values))
    return ((index * 0 + packed) >> (3 * index)) % 8


def contract_last(left, right):
    return lax.dot_general(
        left, right, (((1,), (1,)), ((), ())), preferred_element_type=jnp.float32
    )


def whole_kernel(
    count,
    heads,
    patches,
    cls_token,
    pos_embed,
    ln1_gain,
    ln1_bias,
    patch_weight,
    w_query,
    w_key,
    w_value,
    w_out,
    head_w,
    lnf_gain,
    lnf_bias,
    head_bias,
    out,
    own_patches,
    cls_row,
    position,
    gain_row,
    bias_row,
    embed,
    query_w,
    key_w,
    value_w,
    out_w,
    class_w,
    last_gain,
    last_bias,
    class_bias,
    slots,
    basis,
    scaled,
    form,
    folded,
    constants,
    gathered,
    peak,
    total,
    part,
    from_pair,
    ring,
    result,
    load_sem,
    recv_sem,
    sent_sem,
    tail_send,
    tail_recv,
    spread_sem,
):
    f32, bf16 = jnp.float32, jnp.bfloat16
    me = lax.axis_index("sample")
    core = me % 2
    side = (me // 2) % 2
    chip = me // 2
    chips = count // 2
    plane = me // PLANE
    upper = plane // (LINE // 2)
    depth_in = plane * (1 - upper) + (LINE - 1 - plane) * upper
    inward = 1 - 2 * upper
    images, rows, depth = own_patches.shape
    padded = slots.shape[1]
    lanes = slots.shape[2]
    half = pl.cdiv(padded // TILE_ROWS, 2) * TILE_ROWS
    width = embed.shape[1]
    inner = query_w.shape[1]
    head_dim = inner // heads
    pairs = heads * images
    spots = position.shape[0] - 1

    loads = []
    for index, (source, target) in enumerate(
        (
            (patches, own_patches),
            (pos_embed.at[0], position),
            (cls_token, cls_row),
            (ln1_gain, gain_row),
            (ln1_bias, bias_row),
            (patch_weight.at[0], embed),
            (w_query.at[0], query_w),
            (w_key.at[0], key_w),
            (w_value.at[0], value_w),
            (w_out.at[0], out_w),
            (head_w.at[0], class_w),
            (lnf_gain, last_gain),
            (lnf_bias, last_bias),
            (head_bias, class_bias),
        )
    ):
        load = pltpu.make_async_copy(source, target, load_sem.at[index])
        load.start()
        loads.append(load)

    twin = me + 1 - 2 * core
    beside = plane * PLANE + (1 - side) * 2 + core

    def line(where):
        return where * PLANE + side * 2 + core

    def cross(where):
        return where * PLANE + (1 - side) * 2 + core

    span = LINE - 1
    line_at = {step: line(plane + step * inward) for step in range(-1, LINE)}
    cross_at = {step: cross(plane + step * inward) for step in range(-1, LINE)}
    nearer = line_at[1]
    farther = line_at[-1]
    opposite = line_at[span]

    barrier = pltpu.get_barrier_semaphore()

    def greet(target):
        pl.semaphore_signal(barrier, inc=1, device_id={"sample": target}, device_id_type=MESH)

    greet(twin)
    greet(beside)
    greet(nearer)

    @pl.when(depth_in == 1)
    def _():
        greet(farther)

    loads[0].wait()
    eye = (
        lax.broadcasted_iota(jnp.int32, (padded, depth), 0)
        == lax.broadcasted_iota(jnp.int32, (padded, depth), 1)
    ).astype(bf16)
    flat = own_patches[...].reshape(images * rows, depth)
    slots[me] = contract_last(eye, flat).astype(bf16)
    pl.semaphore_wait(barrier, 3 + depth_in)

    FAR, NEAR, ACROSS, TWIN, DIRECT = range(5)

    def piece(way, target, origin, part_of):
        ref = slots.at[origin, pl.ds(0, half)] if part_of == 0 else slots.at[origin, pl.ds(half, padded - half)]
        return pltpu.make_async_remote_copy(
            src_ref=ref,
            dst_ref=ref,
            send_sem=sent_sem.at[way, origin, part_of],
            recv_sem=recv_sem.at[origin, part_of],
            device_id={"sample": target},
            device_id_type=MESH,
        )

    def arrived(origin, part_of):
        piece(TWIN, twin, origin, part_of).wait_recv()

    issued = []

    def send(way, target, origin, part_of, when=None):
        issued.append((way, target, origin, part_of, when))
        piece(way, target, origin, part_of).start()

    end = depth_in == 0
    middle = depth_in == 1
    def own_sends():
        @pl.when(end)
        def _():
            send(NEAR, nearer, me, 0, end)
            send(NEAR, nearer, me, 1, end)

        @pl.when(middle)
        def _():
            send(FAR, farther, me, 0, middle)
            send(NEAR, nearer, me, 0, middle)
            send(NEAR, nearer, me, 1, middle)

        send(ACROSS, beside, me, 0)
        send(ACROSS, beside, me, 1)
        send(TWIN, twin, me, 0)
        send(TWIN, twin, me, 1)

    def on_line(which, step, part_of, crosses, relay=None, then=()):
        origin = line_at[step]
        arrived(origin, part_of)
        if relay is not None:
            target = nearer if relay == NEAR else farther
            send(relay, target, origin, part_of, which)
        if crosses:
            send(ACROSS, beside, origin, part_of, which)
        send(TWIN, twin, origin, part_of, which)

    def on_cross(which, step, part_of, relay=None):
        origin = cross_at[step]
        arrived(origin, part_of)
        if relay is not None:
            target = nearer if relay == NEAR else farther
            send(relay, target, origin, part_of, which)
        send(TWIN, twin, origin, part_of, which)

    def both(at_end, at_middle):
        pl.when(end)(at_end)
        pl.when(middle)(at_middle)

    def end_events(group):
        if group == 0:
            on_line(end, 1, 0, True)
            on_cross(end, 0, 0, NEAR)
        if group == 1:
            on_line(end, 2, 0, True)
            send(DIRECT, opposite, me, 0, end)
            send(DIRECT, opposite, me, 1, end)
            on_cross(end, 0, 1, NEAR)
        if group == 2:
            on_line(end, 2, 1, True)
        if group == 3:
            on_cross(end, 1, 0)
            on_line(end, 1, 1, False)
        if group == 4:
            on_cross(end, 2, 0)
            on_line(end, 3, 0, True)
            on_cross(end, 2, 1)
        if group == 5:
            on_line(end, 3, 1, True)
        if group == 6:
            on_cross(end, 1, 1)
        if group == 7:
            on_cross(end, 3, 0)
            on_cross(end, 3, 1)

    def middle_events(group):
        if group == 0:
            on_line(middle, -1, 0, False, NEAR)
            on_line(middle, 1, 0, True, FAR)
            on_cross(middle, 0, 0)
        if group == 1:
            on_line(middle, -1, 1, False, NEAR)
            on_line(middle, 1, 1, True, FAR)
            send(FAR, farther, me, 1, middle)
            on_cross(middle, 0, 1, FAR)
        if group == 2:
            on_line(middle, 2, 0, True)
        if group == 3:
            on_cross(middle, 1, 0)
            on_line(middle, 2, 1, True)
        if group == 4:
            on_cross(middle, 1, 1)
            on_cross(middle, -1, 0)
        if group == 5:
            on_cross(middle, -1, 1)
        if group == 6:
            on_cross(middle, 2, 0)
        if group == 7:
            on_cross(middle, 2, 1)

    def events(group):
        both(functools.partial(end_events, group), functools.partial(middle_events, group))

    own_sends()

    for index in (1, 2, 3, 4):
        loads[index].wait()
    gain = gain_row[...]
    bias = bias_row[...]
    leading = cls_row[...].astype(f32) + position[0:1, :].astype(f32)
    lead = jnp.broadcast_to(layer_norm(leading, gain, bias), (TILE_ROWS, width)).astype(bf16)
    lead_row = lead[:1].astype(f32)

    placed = position[...].astype(f32)[1:]
    placed = placed - jnp.mean(placed, axis=1, keepdims=True)
    basis[padded:, :] = placed.astype(bf16)
    scaled[padded:, :] = (placed * gain).astype(bf16)
    weight = jnp.sum(placed * placed, axis=1, keepdims=True)
    weight = jnp.transpose(jnp.broadcast_to(weight, (spots, 128)))[:1]

    loads[5].wait()
    table = embed[...].astype(f32)
    table = table - jnp.mean(table, axis=1, keepdims=True)
    table = jnp.concatenate([table, jnp.zeros((padded - depth, width), f32)], axis=0)
    basis[:padded, :] = table.astype(bf16)
    scaled[:padded, :] = (table * gain).astype(bf16)

    loads[6].wait()
    query = jnp.dot(lead, query_w[...], preferred_element_type=f32)[:1]
    head_row = lax.broadcasted_iota(jnp.int32, (TILE_ROWS, inner), 0)
    column = lax.broadcasted_iota(jnp.int32, (TILE_ROWS, inner), 1)
    own_head = (column >= head_row * head_dim) & (column < (head_row + 1) * head_dim)
    spread = jnp.where(own_head, jnp.broadcast_to(query, (TILE_ROWS, inner)), 0.0).astype(bf16)
    loads[7].wait()
    turned = contract_last(spread, key_w[...])[:heads] * (1.0 / math.sqrt(head_dim))
    first = jnp.sum(turned * lead_row, axis=1, keepdims=True)
    level = jnp.sum(turned * bias, axis=1, keepdims=True)
    constants[...] = jnp.broadcast_to(level, constants.shape)
    probe = split_in_two(turned * gain)

    events(0)

    square = contract_last(basis[:padded, :], basis[...])
    square = jnp.concatenate([square[:, :padded], 2.0 * square[:, padded:]], axis=1)
    form[:padded, :] = square.astype(bf16)
    reach = contract_last(probe, basis[...])
    reach = split_in_two(reach[:heads] + reach[heads:])
    form[padded : padded + 2 * heads, :] = reach
    sizes = jnp.concatenate([jnp.zeros((1, padded), f32), weight], axis=1)
    sizes_high = sizes.astype(bf16).astype(f32)
    sizes = jnp.concatenate(
        [sizes_high, sizes - sizes_high, jnp.zeros((TILE_ROWS - 2, padded + spots), f32)], axis=0
    )
    form[padded + 2 * heads :, :] = sizes.astype(bf16)

    events(1)

    loads[8].wait()
    folded[...] = jnp.dot(scaled[...], value_w[...], preferred_element_type=f32).astype(bf16)
    ends = jnp.concatenate([split_in_two(bias), lead[:1], jnp.zeros((TILE_ROWS - 3, width), bf16)], axis=0)
    ends = jnp.dot(ends, value_w[...], preferred_element_type=f32)
    plain = ends[0:1] + ends[1:2]
    lead_value = ends[2:3]

    first = jnp.broadcast_to(first[None], (images, heads, 1)).reshape(pairs, 1)
    peak[...] = jnp.broadcast_to(first, peak.shape)
    total[...] = jnp.ones(total.shape, f32)
    gathered[...] = jnp.zeros(gathered.shape, f32)

    cells = 2 * lanes
    lane = lax.broadcasted_iota(jnp.int32, (pairs, cells), 1)
    row_image = lax.broadcasted_iota(jnp.int32, (pairs, cells), 0) // heads
    same = (lane % lanes) // rows == row_image
    spot_row = lax.broadcasted_iota(jnp.int32, (spots, cells), 0)
    spot_lane = lax.broadcasted_iota(jnp.int32, (spots, cells), 1)
    spot_at = spot_row - (spot_lane // lanes) * rows - spot_lane % rows

    delta_end = (0, 0, 2, 1, 2, 3, 1, 3)
    delta_middle = (1, 1, 0, 2, 2, 0, 3, 3)
    across_end = (0, 1, 0, 0, 1, 0, 1, 1)
    across_middle = (0, 1, 0, 0, 1, 1, 0, 1)

    def chip_step(turn, carry):
        for index, group in ((2, 2), (3, 3), (4, 4), (5, 5), (6, 6), (7, 7)):
            pl.when(turn == index)(functools.partial(events, group))
        step = pick(turn, delta_end) * (1 - depth_in) + (pick(turn, delta_middle) - 1) * depth_in
        across = pick(turn, across_end) * (1 - depth_in) + pick(turn, across_middle) * depth_in
        where = plane + inward * step
        base = where * PLANE + 2 * (side * (1 - across) + (1 - side) * across)
        arrived(base + 1 - core, 0)
        arrived(base + 1 - core, 1)
        block = jnp.concatenate([slots[base], slots[base + 1]], axis=1)
        spot = jnp.where(spot_at == base * rows, 1.0, 0.0).astype(bf16)
        block = jnp.concatenate([block, spot], axis=0)
        image = jnp.dot(form[...], block, preferred_element_type=f32)
        norm = jnp.sum(image[:padded] * block[:padded].astype(f32), axis=0, keepdims=True)
        tail = padded + 2 * heads
        norm = norm + image[tail : tail + 1] + image[tail + 1 : tail + 2]
        rate = lax.rsqrt(norm * (1.0 / width) + epsilon)
        scores = image[padded : padded + heads] + image[padded + heads : tail]
        scores = scores * rate + constants[:, :1]
        scores = jnp.broadcast_to(scores[None], (images, heads, cells)).reshape(pairs, cells)
        scores = jnp.where(same, scores, LOWEST)
        before = peak[:, :1]
        now = jnp.maximum(before, jnp.max(scores, axis=1, keepdims=True))
        shrink = jnp.exp(before - now)
        chance = jnp.where(same, jnp.exp(scores - now), 0.0)
        peak[...] = jnp.broadcast_to(now, peak.shape)
        total[...] = total[...] * shrink + jnp.sum(chance, axis=1, keepdims=True)
        gathered[...] = gathered[...] * shrink + contract_last((chance * rate).astype(bf16), block)
        return carry

    lax.fori_loop(0, 2 * LINE, chip_step, 0)

    whole = total[:, :1]
    lead_chance = jnp.exp(first - peak[:, :1]) / whole
    pooled = split_in_two(gathered[...] / whole)
    values = jnp.dot(pooled, folded[...], preferred_element_type=f32)
    values = values[:pairs] + values[pairs:] + plain * (1.0 - lead_chance) + lead_value * lead_chance
    pair_head = lax.broadcasted_iota(jnp.int32, (pairs, inner), 0) % heads
    pair_column = lax.broadcasted_iota(jnp.int32, (pairs, inner), 1)
    mine_only = (pair_column >= pair_head * head_dim) & (pair_column < (pair_head + 1) * head_dim)
    values = jnp.where(mine_only, values, 0.0)
    mixed = jnp.sum(values.reshape(images, heads, inner), axis=1).astype(bf16)
    loads[9].wait()
    hidden = leading + jnp.dot(mixed, out_w[...], preferred_element_type=f32)
    for index in (10, 11, 12, 13):
        loads[index].wait()
    final = layer_norm(hidden, last_gain[...], last_bias[...]).astype(bf16)
    logits = contract_last(final, class_w[...]) + class_bias[...]
    lifted = logits - jnp.max(logits, axis=-1, keepdims=True)
    logp = lifted - jnp.log(jnp.sum(jnp.exp(lifted), axis=-1, keepdims=True))

    piece_width = part.shape[2]
    classes = out.shape[1]
    part[0] = logp[:, :piece_width]
    part[1] = jnp.concatenate(
        [logp[:, piece_width:], jnp.zeros((images, 2 * piece_width - classes), f32)], axis=1
    )
    swap = pltpu.make_async_remote_copy(
        src_ref=part.at[1 - core],
        dst_ref=from_pair,
        send_sem=tail_send.at[0],
        recv_sem=tail_recv.at[0],
        device_id={"sample": twin},
        device_id_type=MESH,
    )
    swap.start()
    swap.wait_recv()
    mine = part[core]
    theirs = from_pair[...]
    high = jnp.maximum(mine, theirs)
    ring[chip] = high + jnp.log(jnp.exp(mine - high) + jnp.exp(theirs - high))

    def pass_on(origin, target, step):
        return pltpu.make_async_remote_copy(
            src_ref=ring.at[origin],
            dst_ref=ring.at[origin],
            send_sem=spread_sem.at[step],
            recv_sem=tail_recv.at[2 + origin],
            device_id={"sample": target},
            device_id_type=MESH,
        )

    for step in range(1, chips):
        pass_on(chip, 2 * ((chip + step) % chips) + core, step).start()
    for step in range(1, chips):
        pass_on((chip + step) % chips, me, step).wait_recv()
    every = ring[...]
    high = jnp.max(every, axis=0)
    result[core] = high + jnp.log(jnp.sum(jnp.exp(every - high[None]), axis=0)) - math.log(count)
    share = pltpu.make_async_remote_copy(
        src_ref=result.at[core],
        dst_ref=result.at[core],
        send_sem=tail_send.at[1],
        recv_sem=tail_recv.at[1],
        device_id={"sample": twin},
        device_id_type=MESH,
    )
    share.start()

    def settle(way, target, origin, part_of):
        piece(way, target, origin, part_of).wait_send()

    for way, target, origin, part_of, when in issued:
        if when is None:
            settle(way, target, origin, part_of)
    for which in (end, middle):

        @pl.when(which)
        def _(which=which):
            for way, target, origin, part_of, when in issued:
                if when is which:
                    settle(way, target, origin, part_of)

    swap.wait_send()
    for step in range(1, chips):
        pass_on(chip, twin, step).wait_send()
    pltpu.make_async_remote_copy(
        src_ref=result.at[core],
        dst_ref=result.at[1 - core],
        send_sem=tail_send.at[1],
        recv_sem=tail_recv.at[1],
        device_id={"sample": twin},
        device_id_type=MESH,
    ).wait_recv()
    share.wait_send()
    out[:, :piece_width] = result[0]
    out[:, piece_width:] = result[1][:, : classes - piece_width]


def kernel_shards(
    patches,
    patch_weight,
    cls_token,
    pos_embed,
    ln1_gain,
    ln1_bias,
    w_query,
    w_key,
    w_value,
    w_out,
    lnf_gain,
    lnf_bias,
    head_w,
    head_bias,
):
    count = lax.axis_size("sample")
    images, rows, depth = patches.shape
    width = patch_weight.shape[2]
    inner = w_query.shape[2]
    heads = inner // HEAD_DIM
    pairs = heads * images
    chips = count // 2
    classes = head_w.shape[2]
    piece_width = pl.cdiv(classes, 256) * 128
    padded = pl.cdiv(depth, TILE_ROWS) * TILE_ROWS
    spots = pos_embed.shape[1] - 1
    far = pl.BlockSpec(memory_space=pl.ANY)
    dma = pltpu.SemaphoreType.DMA
    f32, bf16 = jnp.float32, jnp.bfloat16
    class_rows = jnp.swapaxes(head_w, 1, 2)
    given = (
        patches,
        cls_token,
        pos_embed,
        ln1_gain,
        ln1_bias,
        patch_weight,
        w_query,
        w_key,
        w_value,
        w_out,
        class_rows,
        lnf_gain,
        lnf_bias,
        head_bias,
    )
    whole = (True, False)
    held = [
        pltpu.VMEM(a.shape[1:] if a.ndim == 3 and place else a.shape, a.dtype)
        for place, a in enumerate(given)
    ]
    return pl.pallas_call(
        functools.partial(whole_kernel, count, heads),
        out_shape=jax.ShapeDtypeStruct((images, classes), f32),
        in_specs=[far] * len(given),
        out_specs=pl.BlockSpec(memory_space=pltpu.VMEM),
        scratch_shapes=[
            *held,
            pltpu.VMEM((count, padded, images * rows), bf16),
            pltpu.VMEM((padded + spots, width), bf16),
            pltpu.VMEM((padded + spots, width), bf16),
            pltpu.VMEM((padded + 2 * heads + TILE_ROWS, padded + spots), bf16),
            pltpu.VMEM((padded + spots, inner), bf16),
            pltpu.VMEM((heads, 128), f32),
            pltpu.VMEM((pairs, padded + spots), f32),
            pltpu.VMEM((pairs, 128), f32),
            pltpu.VMEM((pairs, 128), f32),
            pltpu.VMEM((2, images, piece_width), f32),
            pltpu.VMEM((images, piece_width), f32),
            pltpu.VMEM((chips, images, piece_width), f32),
            pltpu.VMEM((2, images, piece_width), f32),
            dma((len(given),)),
            dma((count, 2)),
            dma((5, count, 2)),
            dma((2,)),
            dma((2 + chips,)),
            dma((chips,)),
        ],
        compiler_params=pltpu.CompilerParams(
            collective_id=0, has_side_effects=True, vmem_limit_bytes=60 << 20
        ),
    )(*given)


def takes_kernel(mesh, patches):
    count = mesh.shape["sample"]
    rows = patches.shape[1] // count
    images = patches.shape[0] // mesh.shape["group"]
    return count == PLANE * LINE and rows % TILE_ROWS == 0 and images * rows == 128


def solution(mesh):
    placed = (
        P("group", "sample", None),
        P("sample", None, None),
        P("sample", None),
        P("sample", None, None),
        P("sample", None),
        P("sample", None),
        P("sample", None, None),
        P("sample", None, None),
        P("sample", None, None),
        P("sample", None, None),
        P("sample", None),
        P("sample", None),
        P("sample", None, None),
        P("sample", None),
    )

    def run(*arrays):
        step = kernel_shards if takes_kernel(mesh, arrays[0]) else shards
        return jax.shard_map(
            step, mesh=mesh, in_specs=placed, out_specs=P("group", None), check_vma=False
        )(*arrays)

    return run
```

```python
import functools
import math

import jax
import jax.numpy as jnp
from jax import lax
from jax.experimental import pallas as pl
from jax.experimental.pallas import tpu as pltpu
from jax.sharding import PartitionSpec as P

HEAD_DIM = 80


epsilon = 1e-06


def combined_all(part, axis, combine):
    gathered = jax.tree.map(lambda a: lax.all_gather(a, axis), part)

    def take(source):
        return jax.tree.map(lambda a: lax.dynamic_index_in_dim(a, source, 0, False), gathered)

    return lax.fori_loop(
        1, lax.axis_size(axis), lambda source, state: combine(state, take(source)), take(0)
    )


def layer_norm(values, gain, shift):
    center = values - jnp.mean(values, axis=-1, keepdims=True)
    spread = jnp.mean(center * center, axis=-1, keepdims=True)
    return center * lax.rsqrt(spread + epsilon) * gain + shift


def shards(
    patches,
    patch_weight,
    cls_token,
    pos_embed,
    ln1_gain,
    ln1_bias,
    w_query,
    w_key,
    w_value,
    w_out,
    lnf_gain,
    lnf_bias,
    head_w,
    head_bias,
):
    embed_weight = patch_weight[0]
    position = pos_embed[0]
    gain_first = ln1_gain[0]
    bias_first = ln1_bias[0]
    query_weight = w_query[0]
    pair_weight = jnp.concatenate([w_key[0], w_value[0]], axis=1)
    out_weight = w_out[0]
    width = embed_weight.shape[1]
    inner = query_weight.shape[1]
    head_count = inner // HEAD_DIM
    leading = cls_token[0].astype(jnp.float32) + position[0].astype(jnp.float32)
    lead_norm = layer_norm(leading, gain_first, bias_first).astype(jnp.bfloat16)
    lead_pair = jnp.dot(lead_norm[None], pair_weight, preferred_element_type=jnp.float32).astype(
        jnp.bfloat16
    )
    query = jnp.dot(lead_norm[None], query_weight, preferred_element_type=jnp.float32).astype(
        jnp.bfloat16
    )
    query = query.reshape(head_count, HEAD_DIM)
    portion = lax.all_gather(patches, "sample", axis=1, tiled=True)
    image_count = portion.shape[0]
    row_count = portion.shape[1]
    flat = portion.reshape(-1, portion.shape[2])
    tokens = jnp.dot(flat, embed_weight, preferred_element_type=jnp.float32).reshape(
        image_count, row_count, width
    )
    placed = lax.dynamic_slice_in_dim(position, 1, row_count, 0)
    tokens = tokens + placed.astype(jnp.float32)[None]
    normed = layer_norm(tokens, gain_first, bias_first).astype(jnp.bfloat16)
    paired = jnp.dot(normed.reshape(-1, width), pair_weight, preferred_element_type=jnp.float32)
    key_values = paired.astype(jnp.bfloat16).reshape(image_count, row_count, 2 * inner)
    image_count = key_values.shape[0]
    lead_rows = jnp.broadcast_to(lead_pair[None], (image_count, 1, 2 * inner))
    full_rows = jnp.concatenate([lead_rows, key_values], axis=1)
    key_rows = full_rows[:, :, :inner].reshape(image_count, -1, head_count, HEAD_DIM)
    value_rows = full_rows[:, :, inner:].reshape(image_count, -1, head_count, HEAD_DIM)
    scores = jnp.einsum(
        "hd,ithd->iht", query, key_rows, preferred_element_type=jnp.float32
    ) / math.sqrt(HEAD_DIM)
    attention = jax.nn.softmax(scores, axis=-1).astype(jnp.bfloat16)
    mixed = jnp.einsum("iht,ithd->ihd", attention, value_rows, preferred_element_type=jnp.float32)
    mixed = mixed.astype(jnp.bfloat16).reshape(image_count, inner)
    hidden = leading[None] + jnp.dot(mixed, out_weight, preferred_element_type=jnp.float32)
    final = layer_norm(hidden, lnf_gain[0], lnf_bias[0]).astype(jnp.bfloat16)
    logits = jnp.dot(final, head_w[0], preferred_element_type=jnp.float32) + head_bias[0]
    logp = jax.nn.log_softmax(logits, axis=-1)
    count = lax.axis_size("sample")

    def combine(earlier, later):
        highest = jnp.maximum(earlier[0], later[0])
        summed = earlier[1] * jnp.exp(earlier[0] - highest) + later[1] * jnp.exp(later[0] - highest)
        return (highest, summed)

    peak, total = combined_all((logp, jnp.ones_like(logp)), "sample", combine)
    return peak + jnp.log(total) - math.log(count)


MESH = pl.DeviceIdType.MESH
PLANE = 4
LINE = 4
TILE_ROWS = 16
LOWEST = -1e30
GRAM_PARTS = 4
FOLD_PARTS = 6


def split_in_two(values):
    high = values.astype(jnp.bfloat16)
    low = (values - high.astype(jnp.float32)).astype(jnp.bfloat16)
    return jnp.concatenate([high, low], axis=0)


PIECES = 3
SENDS = (
    (
        (1,1,0,1,0), (1,1,0,1,1), (0,0,0,1,0), (1,1,0,1,2), (0,0,0,1,2), (0,0,0,1,1), (0,2,0,1,0),
        (0,2,0,1,1), (0,2,0,1,2), (3,1,0,1,0), (1,1,0,0,0), (2,1,0,1,2), (0,2,0,0,0), (0,0,1,1,0),
        (0,2,1,1,0), (1,1,0,0,2), (3,1,0,0,2), (0,2,0,0,2), (0,0,1,1,2), (0,2,1,1,2), (3,1,0,0,1),
        (0,2,0,0,1), (0,0,1,1,1), (0,2,1,1,1), (0,2,1,0,0), (0,2,1,0,2), (0,0,2,1,2), (0,2,2,1,2),
        (0,2,1,0,1), (0,0,3,1,0), (0,2,3,1,0), (0,0,2,1,1), (0,2,2,1,1), (0,0,2,1,0), (0,2,2,1,0),
        (0,2,2,0,2), (0,2,3,0,0), (0,2,3,0,2), (0,2,2,0,1), (0,2,3,1,1), (0,2,3,0,1), (0,2,2,0,0),
        (0,2,3,1,2),
    ),
    (
        (0,1,1,1,0), (1,0,1,1,1), (0,1,1,1,2), (0,1,1,1,1), (2,1,1,1,2), (2,1,1,1,1), (1,0,1,1,0),
        (2,1,1,1,0), (1,2,1,1,0), (1,2,1,1,1), (1,2,1,1,2), (2,1,0,1,0), (1,2,0,1,0), (1,2,1,0,1),
        (1,0,0,1,1), (2,1,0,1,1), (1,2,0,1,1), (1,0,2,1,2), (0,1,2,1,2), (1,2,2,1,2), (1,2,1,0,0),
        (1,2,0,1,2), (1,0,1,1,2), (0,1,2,1,1), (1,0,2,1,1), (1,2,2,1,1), (1,0,2,1,0), (0,1,2,1,0),
        (1,2,2,1,0), (1,2,0,0,1), (1,2,0,0,0), (1,2,2,0,2), (1,0,3,1,0), (1,2,3,1,0), (1,2,1,0,2),
        (1,2,0,0,2), (0,1,3,1,1), (1,0,3,1,1), (1,2,3,1,1), (1,2,2,0,1), (1,0,3,1,2), (0,1,3,1,2),
        (1,2,3,1,2), (1,2,2,0,0), (1,2,3,0,0), (1,2,3,0,1), (1,2,3,0,2),
    ),
    (
        (3,1,2,1,0), (2,0,2,1,1), (3,1,2,1,2), (3,1,2,1,1), (1,1,2,1,2), (1,1,2,1,1), (2,0,2,1,0),
        (1,1,2,1,0), (2,2,2,1,0), (2,2,2,1,1), (2,2,2,1,2), (2,0,1,1,2), (3,1,1,1,2), (2,2,1,1,2),
        (2,2,2,0,1), (2,0,2,1,2), (3,1,1,1,1), (2,0,1,1,1), (2,2,1,1,1), (1,1,3,1,0), (2,2,3,1,0),
        (2,2,2,0,0), (2,0,1,1,0), (3,1,1,1,0), (2,2,1,1,0), (2,0,3,1,1), (1,1,3,1,1), (2,2,3,1,1),
        (2,2,3,1,2), (2,2,1,0,2), (2,0,0,1,0), (2,2,0,1,0), (2,2,2,0,2), (3,1,0,1,1), (2,0,0,1,1),
        (2,2,0,1,1), (2,2,1,0,1), (2,2,3,0,0), (2,0,0,1,2), (3,1,0,1,2), (2,2,0,1,2), (2,2,1,0,0),
        (2,2,3,0,1), (2,2,0,0,0), (2,2,3,0,2), (2,2,0,0,1), (2,2,0,0,2),
    ),
    (
        (2,1,3,1,0), (2,1,3,1,1), (3,0,3,1,0), (2,1,3,1,2), (3,0,3,1,2), (3,0,3,1,1), (3,2,3,1,0),
        (3,2,3,1,1), (3,2,3,1,2), (0,1,3,1,0), (3,0,2,1,0), (3,2,2,1,0), (2,1,3,0,0), (1,1,3,1,2),
        (3,2,3,0,0), (3,0,2,1,2), (3,2,2,1,2), (2,1,3,0,2), (0,1,3,0,2), (3,2,3,0,2), (0,1,3,0,1),
        (3,2,3,0,1), (3,0,2,1,1), (3,2,2,1,1), (3,2,2,0,0), (3,0,0,1,0), (3,2,0,1,0), (3,0,1,1,2),
        (3,2,1,1,2), (3,0,1,1,1), (3,2,1,1,1), (3,2,2,0,2), (3,0,1,1,0), (3,2,1,1,0), (3,2,2,0,1),
        (3,2,0,0,0), (3,2,0,0,2), (3,2,1,0,2), (3,2,0,1,1), (3,2,1,0,1), (3,2,0,0,1), (3,2,0,1,2),
        (3,2,1,0,0),
    ),
)
EVENTS = (
    (
        ((-1,0,0,0,9),), (), (), ((-2,2,0,9,0),), (), ((-2,3,0,9,1),), (), ((0,0,0,10,3),(1,1,0,13,2)), (),
        ((0,0,2,15,3),(1,1,2,18,2)), (), ((0,0,1,20,2),(1,1,1,22,2)), (),
        ((1,0,0,24,1),(1,0,2,25,1),(2,1,2,26,2),(1,0,1,28,1)), ((3,1,0,29,2),(2,1,1,31,2),(2,1,0,33,2)),
        ((2,0,2,35,1),(3,0,0,36,1),(3,0,2,37,1),(2,0,1,38,1),(3,1,1,39,1),(3,0,1,40,1)),
        ((2,0,0,41,1),(3,1,2,42,1)), (),
    ),
    (
        ((-1,0,0,0,11),), (), (), (), ((-2,3,0,11,0),), (), (), ((0,1,0,11,2),(1,0,1,13,1)), (),
        ((0,1,1,14,3),(2,1,2,17,3),(1,0,0,20,1)), (), ((0,1,2,21,1),(2,1,1,22,4)), ((2,1,0,26,3),),
        ((0,0,1,29,1),(0,0,0,30,1),(2,0,2,31,1),(3,1,0,32,2),(1,0,2,34,1)),
        ((0,0,2,35,1),(3,1,1,36,3),(2,0,1,39,1),(3,1,2,40,3),(2,0,0,43,1)), (), ((3,0,0,44,1),),
        ((3,0,1,45,1),(3,0,2,46,1)),
    ),
    (
        ((-1,0,0,0,11),), ((-2,0,0,11,0),), (), (), (), ((1,1,2,11,3),), (), ((2,0,1,14,1),(1,1,1,15,4)), (),
        ((3,1,0,19,2),(2,0,0,21,1)), ((1,1,0,22,3),), ((3,1,1,25,3),),
        ((3,1,2,28,1),(1,0,2,29,1),(0,1,0,30,2)), ((2,0,2,32,1),),
        ((0,1,1,33,3),(1,0,1,36,1),(3,0,0,37,1),(0,1,2,38,3),(1,0,0,41,1)), ((3,0,1,42,1),),
        ((0,0,0,43,1),(3,0,2,44,1)), ((0,0,1,45,1),(0,0,2,46,1)),
    ),
    (
        ((-1,0,0,0,9),), ((-2,0,0,9,1),(-2,1,0,10,0)), (), (), (), (), ((2,1,0,10,2),), ((3,0,0,12,3),),
        ((2,1,2,15,2),), ((3,0,2,17,3),), (), ((3,0,1,20,2),(2,1,1,22,2)),
        ((2,0,0,24,1),(0,1,0,25,2),(1,1,2,27,2)), ((1,1,1,29,2),(2,0,2,31,1),(1,1,0,32,2)),
        ((2,0,1,34,1),(0,0,0,35,1)), ((0,0,2,36,1),(1,0,2,37,1),(0,1,1,38,1),(1,0,1,39,1),(0,0,1,40,1)),
        ((0,1,2,41,1),(1,0,0,42,1)), (),
    ),
)
ORDER = (15946945, 13862219, 1645021, 4474743)


def contract_last(left, right):
    return lax.dot_general(
        left, right, (((1,), (1,)), ((), ())), preferred_element_type=jnp.float32
    )


def whole_kernel(
    count,
    heads,
    patches,
    cls_token,
    pos_embed,
    ln1_gain,
    ln1_bias,
    patch_weight,
    w_query,
    w_key,
    w_value,
    w_out,
    head_w,
    lnf_gain,
    lnf_bias,
    head_bias,
    out,
    own_patches,
    cls_row,
    position,
    gain_row,
    bias_row,
    embed,
    query_w,
    key_w,
    value_w,
    out_w,
    class_w,
    last_gain,
    last_bias,
    class_bias,
    slots,
    basis,
    scaled,
    form,
    folded,
    constants,
    kept,
    gathered,
    peak,
    total,
    part,
    from_pair,
    ring,
    result,
    load_sem,
    recv_sem,
    sent_sem,
    known_sem,
    tail_send,
    tail_recv,
    spread_sem,
):
    f32, bf16 = jnp.float32, jnp.bfloat16
    me = lax.axis_index("sample")
    core = me % 2
    side = (me // 2) % 2
    chip = me // 2
    chips = count // 2
    plane = me // PLANE
    images, rows, depth = own_patches.shape
    padded = slots.shape[1]
    lanes = slots.shape[2]
    tiles = padded // TILE_ROWS
    cuts = tuple(TILE_ROWS * (tiles * place // PIECES) for place in range(PIECES + 1))
    width = embed.shape[1]
    inner = query_w.shape[1]
    head_dim = inner // heads
    pairs = heads * images
    spots = position.shape[0] - 1

    loads = []
    for index, (source, target) in enumerate(
        (
            (patches, own_patches),
            (pos_embed.at[0], position),
            (cls_token, cls_row),
            (ln1_gain, gain_row),
            (ln1_bias, bias_row),
            (patch_weight.at[0], embed),
            (w_query.at[0], query_w),
            (w_key.at[0], key_w),
            (w_value.at[0], value_w),
            (w_out.at[0], out_w),
            (head_w.at[0], class_w),
            (lnf_gain, last_gain),
            (lnf_bias, last_bias),
            (head_bias, class_bias),
        )
    ):
        load = pltpu.make_async_copy(source, target, load_sem.at[index])
        load.start()
        loads.append(load)

    twin = me + 1 - 2 * core
    beside = plane * PLANE + (1 - side) * 2 + core
    here = tuple(lax.convert_element_type(plane == place, jnp.int32) for place in range(LINE))
    line_of = tuple(
        (place * PLANE + (1 - side) * 2 + core, place * PLANE + side * 2 + core)
        for place in range(LINE)
    )

    barrier = pltpu.get_barrier_semaphore()

    def greet(target):
        pl.semaphore_signal(barrier, inc=1, device_id={"sample": target}, device_id_type=MESH)

    greet(twin)
    greet(beside)

    @pl.when(plane > 0)
    def _():
        greet(me - PLANE)

    @pl.when(plane < LINE - 1)
    def _():
        greet(me + PLANE)

    loads[0].wait()
    eye = (
        lax.broadcasted_iota(jnp.int32, (padded, depth), 0)
        == lax.broadcasted_iota(jnp.int32, (padded, depth), 1)
    ).astype(bf16)
    flat = own_patches[...].reshape(images * rows, depth)
    slots[me] = contract_last(eye, flat).astype(bf16)
    pl.semaphore_wait(barrier, LINE - here[0] - here[LINE - 1])

    def piece(slot, target, origin, part_of):
        low, high = cuts[part_of], cuts[part_of + 1]
        ref = slots.at[origin, pl.ds(low, high - low)]
        return pltpu.make_async_remote_copy(
            src_ref=ref,
            dst_ref=ref,
            send_sem=sent_sem.at[slot],
            recv_sem=recv_sem.at[origin, part_of],
            device_id={"sample": target},
            device_id_type=MESH,
        )

    def sent(place, slot):
        to, aside, origin, own, part_of = SENDS[place][slot]
        target = twin if aside == 2 else line_of[to][aside]
        return piece(slot, target, line_of[origin][own], part_of)

    def tell(target, entered):
        pl.semaphore_signal(
            known_sem.at[entered], inc=1, device_id={"sample": target}, device_id_type=MESH
        )

    def learn(place, entered):
        pl.semaphore_wait(known_sem.at[entered], 1)
        if place == 1 and entered == 3:
            tell(me - PLANE, 3)
        if place == 2 and entered == 0:
            tell(me + PLANE, 0)

    for place in (1, 2):

        @pl.when(plane == place)
        def _(place=place):
            tell(me - PLANE, place + 1)
            tell(me + PLANE, place - 1)

    def events(group):
        for place in range(LINE):
            entries = EVENTS[place][group]
            if entries:

                @pl.when(plane == place)
                def _(place=place, entries=entries):
                    for origin, own, part_of, low, number in entries:
                        if origin == -2:
                            learn(place, own)
                        if origin >= 0:
                            piece(0, twin, line_of[origin][own], part_of).wait_recv()
                        for slot in range(low, low + number):
                            sent(place, slot).start()

    events(0)

    for index in (1, 2, 3, 4):
        loads[index].wait()
    events(1)
    gain = gain_row[...]
    bias = bias_row[...]
    leading = cls_row[...].astype(f32) + position[0:1, :].astype(f32)
    lead = jnp.broadcast_to(layer_norm(leading, gain, bias), (TILE_ROWS, width)).astype(bf16)
    lead_row = lead[:1].astype(f32)

    events(2)
    placed = position[...].astype(f32)[1:]
    placed = placed - jnp.mean(placed, axis=1, keepdims=True)
    basis[padded:, :] = placed.astype(bf16)
    scaled[padded : padded + spots, :] = (placed * gain).astype(bf16)
    scaled[padded + spots :, :] = jnp.zeros((scaled.shape[0] - padded - spots, width), bf16)
    weight = jnp.sum(placed * placed, axis=1, keepdims=True)
    weight = jnp.transpose(jnp.broadcast_to(weight, (spots, 128)))[:1]

    loads[5].wait()
    table = embed[...].astype(f32)
    table = table - jnp.mean(table, axis=1, keepdims=True)
    table = jnp.concatenate([table, jnp.zeros((padded - depth, width), f32)], axis=0)
    basis[:padded, :] = table.astype(bf16)
    scaled[:padded, :] = (table * gain).astype(bf16)

    events(3)
    loads[6].wait()
    query = jnp.dot(lead, query_w[...], preferred_element_type=f32)[:1]
    head_row = lax.broadcasted_iota(jnp.int32, (TILE_ROWS, inner), 0)
    column = lax.broadcasted_iota(jnp.int32, (TILE_ROWS, inner), 1)
    own_head = (column >= head_row * head_dim) & (column < (head_row + 1) * head_dim)
    spread = jnp.where(own_head, jnp.broadcast_to(query, (TILE_ROWS, inner)), 0.0).astype(bf16)
    events(4)
    loads[7].wait()
    turned = contract_last(spread, key_w[...])[:heads] * (1.0 / math.sqrt(head_dim))
    first = jnp.sum(turned * lead_row, axis=1, keepdims=True)
    level = jnp.sum(turned * bias, axis=1, keepdims=True)
    constants[...] = jnp.broadcast_to(level, constants.shape)
    probe = split_in_two(turned * gain)

    for part_of in range(GRAM_PARTS):
        events(5 + part_of)
        low = TILE_ROWS * (tiles * part_of // GRAM_PARTS)
        high = TILE_ROWS * (tiles * (part_of + 1) // GRAM_PARTS)
        square = contract_last(basis[low:high, :], basis[...])
        square = jnp.concatenate([square[:, :padded], 2.0 * square[:, padded:]], axis=1)
        form[low:high, :] = square.astype(bf16)
    events(5 + GRAM_PARTS)
    reach = contract_last(probe, basis[...])
    reach = split_in_two(reach[:heads] + reach[heads:])
    form[padded : padded + 2 * heads, :] = reach
    sizes = jnp.concatenate([jnp.zeros((1, padded), f32), weight], axis=1)
    sizes_high = sizes.astype(bf16).astype(f32)
    sizes = jnp.concatenate(
        [sizes_high, sizes - sizes_high, jnp.zeros((TILE_ROWS - 2, padded + spots), f32)], axis=0
    )
    form[padded + 2 * heads :, :] = sizes.astype(bf16)

    loads[8].wait()
    ends = jnp.concatenate([split_in_two(bias), lead[:1], jnp.zeros((TILE_ROWS - 3, width), bf16)], axis=0)
    ends = jnp.dot(ends, value_w[...], preferred_element_type=f32)
    plain = ends[0:1] + ends[1:2]
    lead_value = ends[2:3]

    first = jnp.broadcast_to(first[None], (images, heads, 1)).reshape(pairs, 1)
    peak[...] = jnp.broadcast_to(first, peak.shape)
    total[...] = jnp.ones(total.shape, f32)
    gathered[...] = jnp.zeros(gathered.shape, f32)

    cells = 2 * lanes
    lane = lax.broadcasted_iota(jnp.int32, (pairs, cells), 1)
    row_image = lax.broadcasted_iota(jnp.int32, (pairs, cells), 0) // heads
    same = (lane % lanes) // rows == row_image
    spot_row = lax.broadcasted_iota(jnp.int32, (spots, cells), 0)
    spot_lane = lax.broadcasted_iota(jnp.int32, (spots, cells), 1)
    spot_at = spot_row - (spot_lane // lanes) * rows - spot_lane % rows

    order = sum(mine * packed for mine, packed in zip(here, ORDER, strict=True))
    first_step = 6 + GRAM_PARTS
    fold_rows = scaled.shape[0] // FOLD_PARTS

    def base_of(turn):
        code = (order >> (3 * turn)) % 8
        where, own = code // 2, code % 2
        return where * PLANE + 2 * (side * own + (1 - side) * (1 - own))

    def block_of(base):
        block = jnp.concatenate([slots[base], slots[base + 1]], axis=1)
        spot = jnp.where(spot_at == base * rows, 1.0, 0.0).astype(bf16)
        return jnp.concatenate([block, spot], axis=0)

    def front(base):
        block = block_of(base)
        image = jnp.dot(form[...], block, preferred_element_type=f32)
        norm = jnp.sum(image[:padded] * block[:padded].astype(f32), axis=0, keepdims=True)
        tail = padded + 2 * heads
        norm = norm + image[tail : tail + 1] + image[tail + 1 : tail + 2]
        rate = lax.rsqrt(norm * (1.0 / width) + epsilon)
        scores = image[padded : padded + heads] + image[padded + heads : tail]
        kept[:heads, :] = scores * rate + constants[:, :1]
        kept[heads:, :] = jnp.broadcast_to(rate, (heads, cells))

    def back(base, scores, rate):
        block = block_of(base)
        scores = jnp.broadcast_to(scores[None], (images, heads, cells)).reshape(pairs, cells)
        scores = jnp.where(same, scores, LOWEST)
        before = peak[:, :1]
        now = jnp.maximum(before, jnp.max(scores, axis=1, keepdims=True))
        shrink = jnp.exp(before - now)
        chance = jnp.where(same, jnp.exp(scores - now), 0.0)
        peak[...] = jnp.broadcast_to(now, peak.shape)
        total[...] = total[...] * shrink + jnp.sum(chance, axis=1, keepdims=True)
        gathered[...] = gathered[...] * shrink + contract_last((chance * rate).astype(bf16), block)

    def twin_pieces(base):
        for part_of in range(PIECES):
            piece(0, twin, base + 1 - core, part_of).wait_recv()

    def chip_step(turn, carry):
        for index in range(1, 2 * LINE):
            pl.when(turn == index)(functools.partial(events, first_step + index))
        base = base_of(turn)
        twin_pieces(base)
        scores = kept[:heads, :]
        rate = kept[heads : heads + 1, :]
        back(base_of(turn - 1), scores, rate)
        front(base)

        @pl.when(turn <= FOLD_PARTS)
        def _():
            low = pl.multiple_of((turn - 1) * fold_rows, TILE_ROWS)
            folded[pl.ds(low, fold_rows), :] = jnp.dot(
                scaled[pl.ds(low, fold_rows), :], value_w[...], preferred_element_type=f32
            ).astype(bf16)

        return carry

    events(first_step)
    twin_pieces(base_of(0))
    front(base_of(0))
    lax.fori_loop(1, 2 * LINE, chip_step, 0)
    back(base_of(2 * LINE - 1), kept[:heads, :], kept[heads : heads + 1, :])

    whole = total[:, :1]
    lead_chance = jnp.exp(first - peak[:, :1]) / whole
    pooled = split_in_two(gathered[...] / whole)
    values = jnp.dot(pooled, folded[: padded + spots, :], preferred_element_type=f32)
    values = values[:pairs] + values[pairs:] + plain * (1.0 - lead_chance) + lead_value * lead_chance
    pair_head = lax.broadcasted_iota(jnp.int32, (pairs, inner), 0) % heads
    pair_column = lax.broadcasted_iota(jnp.int32, (pairs, inner), 1)
    mine_only = (pair_column >= pair_head * head_dim) & (pair_column < (pair_head + 1) * head_dim)
    values = jnp.where(mine_only, values, 0.0)
    mixed = jnp.sum(values.reshape(images, heads, inner), axis=1).astype(bf16)
    loads[9].wait()
    hidden = leading + jnp.dot(mixed, out_w[...], preferred_element_type=f32)
    for index in (10, 11, 12, 13):
        loads[index].wait()
    final = layer_norm(hidden, last_gain[...], last_bias[...]).astype(bf16)
    logits = contract_last(final, class_w[...]) + class_bias[...]
    lifted = logits - jnp.max(logits, axis=-1, keepdims=True)
    logp = lifted - jnp.log(jnp.sum(jnp.exp(lifted), axis=-1, keepdims=True))

    piece_width = part.shape[2]
    classes = out.shape[1]
    part[0] = logp[:, :piece_width]
    part[1] = jnp.concatenate(
        [logp[:, piece_width:], jnp.zeros((images, 2 * piece_width - classes), f32)], axis=1
    )
    swap = pltpu.make_async_remote_copy(
        src_ref=part.at[1 - core],
        dst_ref=from_pair,
        send_sem=tail_send.at[0],
        recv_sem=tail_recv.at[0],
        device_id={"sample": twin},
        device_id_type=MESH,
    )
    swap.start()
    swap.wait_recv()
    mine = part[core]
    theirs = from_pair[...]
    high = jnp.maximum(mine, theirs)
    ring[chip] = high + jnp.log(jnp.exp(mine - high) + jnp.exp(theirs - high))

    def pass_on(origin, target, step):
        return pltpu.make_async_remote_copy(
            src_ref=ring.at[origin],
            dst_ref=ring.at[origin],
            send_sem=spread_sem.at[step],
            recv_sem=tail_recv.at[2 + origin],
            device_id={"sample": target},
            device_id_type=MESH,
        )

    for step in range(1, chips):
        other = step - 1 + jnp.minimum(step // jnp.maximum(chip + 1, 1), 1)
        pass_on(chip, 2 * other + core, step).start()
    for step in range(1, chips):
        pass_on((chip + step) % chips, me, step).wait_recv()
    every = ring[...]
    high = jnp.max(every, axis=0)
    result[core] = high + jnp.log(jnp.sum(jnp.exp(every - high[None]), axis=0)) - math.log(count)
    share = pltpu.make_async_remote_copy(
        src_ref=result.at[core],
        dst_ref=result.at[core],
        send_sem=tail_send.at[1],
        recv_sem=tail_recv.at[1],
        device_id={"sample": twin},
        device_id_type=MESH,
    )
    share.start()

    for place in range(LINE):

        @pl.when(plane == place)
        def _(place=place):
            for slot in range(len(SENDS[place])):
                sent(place, slot).wait_send()

    swap.wait_send()
    for step in range(1, chips):
        pass_on(chip, twin, step).wait_send()
    pltpu.make_async_remote_copy(
        src_ref=result.at[core],
        dst_ref=result.at[1 - core],
        send_sem=tail_send.at[1],
        recv_sem=tail_recv.at[1],
        device_id={"sample": twin},
        device_id_type=MESH,
    ).wait_recv()
    share.wait_send()
    out[:, :piece_width] = result[0]
    out[:, piece_width:] = result[1][:, : classes - piece_width]


def kernel_shards(
    patches,
    patch_weight,
    cls_token,
    pos_embed,
    ln1_gain,
    ln1_bias,
    w_query,
    w_key,
    w_value,
    w_out,
    lnf_gain,
    lnf_bias,
    head_w,
    head_bias,
):
    count = lax.axis_size("sample")
    images, rows, depth = patches.shape
    width = patch_weight.shape[2]
    inner = w_query.shape[2]
    heads = inner // HEAD_DIM
    pairs = heads * images
    chips = count // 2
    classes = head_w.shape[2]
    piece_width = pl.cdiv(classes, 256) * 128
    padded = pl.cdiv(depth, TILE_ROWS) * TILE_ROWS
    spots = pos_embed.shape[1] - 1
    fold_rows = pl.cdiv(padded + spots, FOLD_PARTS * TILE_ROWS) * FOLD_PARTS * TILE_ROWS
    far = pl.BlockSpec(memory_space=pl.ANY)
    dma = pltpu.SemaphoreType.DMA
    f32, bf16 = jnp.float32, jnp.bfloat16
    class_rows = jnp.swapaxes(head_w, 1, 2)
    given = (
        patches,
        cls_token,
        pos_embed,
        ln1_gain,
        ln1_bias,
        patch_weight,
        w_query,
        w_key,
        w_value,
        w_out,
        class_rows,
        lnf_gain,
        lnf_bias,
        head_bias,
    )
    held = [
        pltpu.VMEM(a.shape[1:] if place and a.ndim == 3 else a.shape, a.dtype)
        for place, a in enumerate(given)
    ]
    return pl.pallas_call(
        functools.partial(whole_kernel, count, heads),
        out_shape=jax.ShapeDtypeStruct((images, classes), f32),
        in_specs=[far] * len(given),
        out_specs=pl.BlockSpec(memory_space=pltpu.VMEM),
        scratch_shapes=[
            *held,
            pltpu.VMEM((count, padded, images * rows), bf16),
            pltpu.VMEM((padded + spots, width), bf16),
            pltpu.VMEM((fold_rows, width), bf16),
            pltpu.VMEM((padded + 2 * heads + TILE_ROWS, padded + spots), bf16),
            pltpu.VMEM((fold_rows, inner), bf16),
            pltpu.VMEM((heads, 128), f32),
            pltpu.VMEM((2 * heads, 2 * images * rows), f32),
            pltpu.VMEM((pairs, padded + spots), f32),
            pltpu.VMEM((pairs, 128), f32),
            pltpu.VMEM((pairs, 128), f32),
            pltpu.VMEM((2, images, piece_width), f32),
            pltpu.VMEM((images, piece_width), f32),
            pltpu.VMEM((chips, images, piece_width), f32),
            pltpu.VMEM((2, images, piece_width), f32),
            dma((len(given),)),
            dma((count, PIECES)),
            dma((max(len(place) for place in SENDS),)),
            pltpu.SemaphoreType.REGULAR((LINE,)),
            dma((2,)),
            dma((2 + chips,)),
            dma((chips,)),
        ],
        compiler_params=pltpu.CompilerParams(
            collective_id=0, has_side_effects=True, vmem_limit_bytes=60 << 20
        ),
    )(*given)


def takes_kernel(mesh, patches):
    count = mesh.shape["sample"]
    rows = patches.shape[1] // count
    images = patches.shape[0] // mesh.shape["group"]
    return count == PLANE * LINE and rows % TILE_ROWS == 0 and images * rows == 128


def solution(mesh):
    placed = (
        P("group", "sample", None),
        P("sample", None, None),
        P("sample", None),
        P("sample", None, None),
        P("sample", None),
        P("sample", None),
        P("sample", None, None),
        P("sample", None, None),
        P("sample", None, None),
        P("sample", None, None),
        P("sample", None),
        P("sample", None),
        P("sample", None, None),
        P("sample", None),
    )

    def run(*arrays):
        step = kernel_shards if takes_kernel(mesh, arrays[0]) else shards
        return jax.shard_map(
            step, mesh=mesh, in_specs=placed, out_specs=P("group", None), check_vma=False
        )(*arrays)

    return run
```

```python
import functools
import math

import jax
import jax.numpy as jnp
from jax import lax
from jax.experimental import pallas as pl
from jax.experimental.pallas import tpu as pltpu
from jax.sharding import PartitionSpec as P

HEAD_DIM = 80


epsilon = 1e-06


def combined_all(part, axis, combine):
    gathered = jax.tree.map(lambda a: lax.all_gather(a, axis), part)

    def take(source):
        return jax.tree.map(lambda a: lax.dynamic_index_in_dim(a, source, 0, False), gathered)

    return lax.fori_loop(
        1, lax.axis_size(axis), lambda source, state: combine(state, take(source)), take(0)
    )


def layer_norm(values, gain, shift):
    center = values - jnp.mean(values, axis=-1, keepdims=True)
    spread = jnp.mean(center * center, axis=-1, keepdims=True)
    return center * lax.rsqrt(spread + epsilon) * gain + shift


def shards(
    patches,
    patch_weight,
    cls_token,
    pos_embed,
    ln1_gain,
    ln1_bias,
    w_query,
    w_key,
    w_value,
    w_out,
    lnf_gain,
    lnf_bias,
    head_w,
    head_bias,
):
    embed_weight = patch_weight[0]
    position = pos_embed[0]
    gain_first = ln1_gain[0]
    bias_first = ln1_bias[0]
    query_weight = w_query[0]
    pair_weight = jnp.concatenate([w_key[0], w_value[0]], axis=1)
    out_weight = w_out[0]
    width = embed_weight.shape[1]
    inner = query_weight.shape[1]
    head_count = inner // HEAD_DIM
    leading = cls_token[0].astype(jnp.float32) + position[0].astype(jnp.float32)
    lead_norm = layer_norm(leading, gain_first, bias_first).astype(jnp.bfloat16)
    lead_pair = jnp.dot(lead_norm[None], pair_weight, preferred_element_type=jnp.float32).astype(
        jnp.bfloat16
    )
    query = jnp.dot(lead_norm[None], query_weight, preferred_element_type=jnp.float32).astype(
        jnp.bfloat16
    )
    query = query.reshape(head_count, HEAD_DIM)
    portion = lax.all_gather(patches, "sample", axis=1, tiled=True)
    image_count = portion.shape[0]
    row_count = portion.shape[1]
    flat = portion.reshape(-1, portion.shape[2])
    tokens = jnp.dot(flat, embed_weight, preferred_element_type=jnp.float32).reshape(
        image_count, row_count, width
    )
    placed = lax.dynamic_slice_in_dim(position, 1, row_count, 0)
    tokens = tokens + placed.astype(jnp.float32)[None]
    normed = layer_norm(tokens, gain_first, bias_first).astype(jnp.bfloat16)
    paired = jnp.dot(normed.reshape(-1, width), pair_weight, preferred_element_type=jnp.float32)
    key_values = paired.astype(jnp.bfloat16).reshape(image_count, row_count, 2 * inner)
    image_count = key_values.shape[0]
    lead_rows = jnp.broadcast_to(lead_pair[None], (image_count, 1, 2 * inner))
    full_rows = jnp.concatenate([lead_rows, key_values], axis=1)
    key_rows = full_rows[:, :, :inner].reshape(image_count, -1, head_count, HEAD_DIM)
    value_rows = full_rows[:, :, inner:].reshape(image_count, -1, head_count, HEAD_DIM)
    scores = jnp.einsum(
        "hd,ithd->iht", query, key_rows, preferred_element_type=jnp.float32
    ) / math.sqrt(HEAD_DIM)
    attention = jax.nn.softmax(scores, axis=-1).astype(jnp.bfloat16)
    mixed = jnp.einsum("iht,ithd->ihd", attention, value_rows, preferred_element_type=jnp.float32)
    mixed = mixed.astype(jnp.bfloat16).reshape(image_count, inner)
    hidden = leading[None] + jnp.dot(mixed, out_weight, preferred_element_type=jnp.float32)
    final = layer_norm(hidden, lnf_gain[0], lnf_bias[0]).astype(jnp.bfloat16)
    logits = jnp.dot(final, head_w[0], preferred_element_type=jnp.float32) + head_bias[0]
    logp = jax.nn.log_softmax(logits, axis=-1)
    count = lax.axis_size("sample")

    def combine(earlier, later):
        highest = jnp.maximum(earlier[0], later[0])
        summed = earlier[1] * jnp.exp(earlier[0] - highest) + later[1] * jnp.exp(later[0] - highest)
        return (highest, summed)

    peak, total = combined_all((logp, jnp.ones_like(logp)), "sample", combine)
    return peak + jnp.log(total) - math.log(count)


MESH = pl.DeviceIdType.MESH
PLANE = 4
LINE = 4
TILE_ROWS = 16
LOWEST = -1e30
GRAM_PARTS = 2
FOLD_PARTS = 6


def split_in_two(values):
    high = values.astype(jnp.bfloat16)
    low = (values - high.astype(jnp.float32)).astype(jnp.bfloat16)
    return jnp.concatenate([high, low], axis=0)


PIECES = 4
SENDS = (
    (
        (0,0,0,1,0), (1,1,0,1,0), (1,1,0,1,2), (1,1,0,1,3), (0,0,0,1,3), (0,0,0,1,1), (1,1,0,1,1),
        (0,0,0,1,2), (0,2,0,1,0), (0,2,0,1,1), (0,2,0,1,2), (0,2,0,1,3), (2,1,0,1,1), (1,1,0,0,0),
        (0,2,0,0,0), (0,0,1,1,0), (0,2,1,1,0), (2,1,0,0,3), (3,1,0,0,3), (1,1,0,0,3), (0,2,0,0,3),
        (0,0,1,1,2), (0,2,1,1,2), (1,1,0,0,1), (2,1,0,0,1), (0,2,0,0,1), (0,0,1,1,1), (0,2,1,1,1),
        (2,1,0,0,2), (3,1,0,0,2), (0,2,0,0,2), (0,0,1,1,3), (0,2,1,1,3), (0,2,1,0,0), (0,2,1,0,2),
        (0,0,2,1,1), (0,2,2,1,1), (0,2,1,0,1), (0,0,2,1,2), (0,2,2,1,2), (0,2,1,0,3), (0,0,2,1,3),
        (0,2,2,1,3), (0,0,2,1,0), (0,2,2,1,0), (0,2,2,0,1), (0,2,3,1,3), (0,2,2,0,2), (0,2,3,0,1),
        (0,0,3,1,0), (0,2,3,1,0), (0,2,2,0,3), (0,2,3,0,3), (0,2,2,0,0), (0,2,3,1,2), (0,2,3,0,2),
        (0,2,3,1,1), (0,2,3,0,0),
    ),
    (
        (0,1,1,1,0), (2,1,1,1,1), (1,0,1,1,1), (2,1,1,1,0), (0,1,1,1,2), (2,1,1,1,2), (1,0,1,1,0),
        (0,1,1,1,1), (0,1,1,1,3), (1,0,1,1,3), (1,0,1,1,2), (2,1,1,1,3), (1,2,1,1,0), (1,2,1,1,1),
        (1,2,1,1,2), (1,2,1,1,3), (2,1,0,1,0), (1,2,0,1,0), (1,2,1,0,1), (2,1,0,1,2), (1,0,0,1,2),
        (1,2,0,1,2), (1,2,1,0,0), (1,0,2,1,1), (0,1,2,1,1), (1,2,2,1,1), (2,1,0,1,3), (1,2,0,1,3),
        (1,2,1,0,3), (0,1,2,1,2), (1,0,2,1,2), (1,2,2,1,2), (1,2,0,1,1), (1,2,1,0,2), (0,1,2,1,3),
        (1,0,2,1,3), (1,2,2,1,3), (0,1,2,1,0), (1,0,2,1,0), (1,2,2,1,0), (1,2,0,0,2), (1,2,0,0,0),
        (0,1,3,1,3), (1,0,3,1,3), (1,2,3,1,3), (1,2,2,0,1), (1,2,2,0,2), (0,1,3,1,0), (1,0,3,1,0),
        (1,2,3,1,0), (1,2,2,0,3), (1,2,2,0,0), (1,2,3,0,1), (1,2,0,0,3), (1,0,3,1,2), (0,1,3,1,2),
        (1,2,3,1,2), (1,2,3,0,3), (1,2,0,0,1), (0,1,3,1,1), (1,2,3,1,1), (1,2,3,0,0), (1,2,3,0,2),
    ),
    (
        (1,1,2,1,1), (2,0,2,1,1), (3,1,2,1,0), (1,1,2,1,2), (2,0,2,1,3), (1,1,2,1,3), (1,1,2,1,0),
        (3,1,2,1,2), (3,1,2,1,1), (2,0,2,1,2), (3,1,2,1,3), (2,2,2,1,0), (2,2,2,1,1), (2,2,2,1,2),
        (2,2,2,1,3), (3,1,1,1,1), (2,0,1,1,1), (2,2,1,1,1), (3,1,1,1,0), (2,0,1,1,0), (2,2,1,1,0),
        (2,2,2,0,1), (3,1,1,1,2), (2,0,1,1,2), (2,2,1,1,2), (1,1,3,1,0), (2,0,3,1,0), (2,2,3,1,0),
        (2,2,2,0,3), (1,1,3,1,2), (2,0,3,1,2), (2,2,3,1,2), (2,2,2,0,2), (3,1,1,1,3), (2,0,1,1,3),
        (2,2,1,1,3), (1,1,3,1,1), (2,2,3,1,1), (2,2,1,0,1), (3,1,0,1,1), (2,0,2,1,0), (2,2,0,1,1),
        (2,0,0,1,0), (3,1,0,1,0), (2,2,0,1,0), (2,2,3,1,3), (2,2,1,0,0), (3,1,0,1,2), (2,2,0,1,2),
        (2,2,1,0,2), (2,2,3,0,1), (2,2,0,0,3), (2,2,3,0,0), (3,1,0,1,3), (2,2,0,1,3), (2,2,3,0,2),
        (2,2,1,0,3), (2,2,2,0,0), (2,2,0,0,0), (2,2,3,0,3), (2,2,0,0,1), (2,2,0,0,2),
    ),
    (
        (2,1,3,1,0), (3,0,3,1,1), (2,1,3,1,2), (3,0,3,1,3), (2,1,3,1,1), (2,1,3,1,3), (3,0,3,1,2),
        (3,2,3,1,0), (3,2,3,1,1), (3,2,3,1,2), (3,2,3,1,3), (1,1,3,1,3), (3,0,2,1,0), (3,2,2,1,0),
        (3,0,3,1,0), (2,1,3,0,1), (1,1,3,0,1), (0,1,3,0,1), (3,2,3,0,1), (3,0,2,1,2), (3,2,2,1,2),
        (2,1,3,0,3), (0,1,3,0,3), (3,2,3,0,3), (3,0,2,1,1), (3,2,2,1,1), (0,1,3,0,2), (3,2,3,0,2),
        (3,0,2,1,3), (3,2,2,1,3), (3,0,1,1,1), (3,2,1,1,1), (3,2,2,0,0), (3,0,1,1,0), (3,2,1,1,0),
        (3,0,1,1,2), (3,2,1,1,2), (3,2,3,0,0), (3,2,2,0,2), (3,2,2,0,1), (3,0,1,1,3), (3,2,1,1,3),
        (3,2,2,0,3), (3,0,0,1,1), (3,2,0,1,1), (3,2,0,0,3), (3,2,1,0,1), (3,0,0,1,0), (3,2,0,1,0),
        (3,2,1,0,0), (3,2,0,1,2), (3,2,1,0,2), (3,2,0,1,3), (3,2,1,0,3), (3,2,0,0,1), (3,2,0,0,2),
        (3,2,0,0,0),
    ),
)
EVENTS = (
    (
        ((-1,0,0,0,12),), (), (), ((-2,2,0,12,1),), (), (), ((0,0,0,13,2),(-2,3,0,15,0),(1,1,0,15,2)),
        ((0,0,3,17,4),(1,1,2,21,2),(0,0,1,23,3)), ((1,1,1,26,2),(0,0,2,28,3),(1,1,3,31,2)), (),
        ((1,0,0,33,1),), (), ((1,0,2,34,1),(2,1,1,35,2)), ((1,0,1,37,1),(2,1,2,38,2),(1,0,3,40,1)),
        ((2,1,3,41,2),(2,1,0,43,2)), (), ((2,0,1,45,1),(3,1,3,46,1),(2,0,2,47,1),(3,0,1,48,1)),
        ((3,1,0,49,2),(2,0,3,51,1),(3,0,3,52,1),(2,0,0,53,1)), ((3,1,2,54,1),(3,0,2,55,1),(3,1,1,56,1)),
        ((3,0,0,57,1),), (), (),
    ),
    (
        ((-1,0,0,0,16),), (), (), (), ((-2,3,0,16,0),), ((0,1,0,16,2),), ((1,0,1,18,1),(0,1,2,19,3)),
        ((1,0,0,22,1),(2,1,1,23,3),(0,1,3,26,2),(1,0,3,28,1),(2,1,2,29,3),(0,1,1,32,1)),
        ((1,0,2,33,1),(2,1,3,34,3)), ((2,1,0,37,3),), ((0,0,2,40,1),), ((0,0,0,41,1),),
        ((3,1,3,42,3),(2,0,1,45,1)), (), ((2,0,2,46,1),(3,1,0,47,3)), ((2,0,3,50,1),(2,0,0,51,1)),
        ((3,0,1,52,1),(0,0,3,53,1),(3,1,2,54,3),(3,0,3,57,1),(0,0,1,58,1)), ((3,1,1,59,2),), ((3,0,0,61,1),),
        (), (), ((3,0,2,62,1),),
    ),
    (
        ((-1,0,0,0,15),), ((-2,0,0,15,0),), (), (), (), ((1,1,1,15,3),),
        ((1,1,0,18,3),(2,0,1,21,1),(1,1,2,22,3)),
        ((3,1,0,25,3),(2,0,3,28,1),(3,1,2,29,3),(2,0,2,32,1),(1,1,3,33,3)),
        ((3,1,1,36,2),(1,0,1,38,1),(0,1,1,39,3),(0,1,0,42,3),(3,1,3,45,1)), (), ((1,0,0,46,1),(0,1,2,47,2)),
        ((1,0,2,49,1),(3,0,1,50,1)), ((0,0,3,51,1),(3,0,0,52,1)), ((0,1,3,53,2),(3,0,2,55,1)),
        ((1,0,3,56,1),(2,0,0,57,1)), (), ((0,0,0,58,1),(3,0,3,59,1),(0,0,1,60,1)), ((0,0,2,61,1),), (), (),
        (), (),
    ),
    (
        ((-1,0,0,0,11),), ((-2,1,0,11,1),(-2,0,0,12,0)), (), (), (), ((2,1,0,12,2),),
        ((3,0,1,14,5),(2,1,2,19,2)), ((3,0,3,21,3),(2,1,1,24,2),(3,0,2,26,2),(2,1,3,28,2)),
        ((1,1,1,30,2),(2,0,0,32,1)), ((1,1,0,33,2),), ((1,1,2,35,2),(3,0,0,37,1)), (),
        ((2,0,2,38,1),(2,0,1,39,1),(1,1,3,40,2)), ((2,0,3,42,1),(0,1,1,43,2)),
        ((0,0,3,45,1),(1,0,1,46,1),(0,1,0,47,2)), ((1,0,0,49,1),(0,1,2,50,1)), ((1,0,2,51,1),(0,1,3,52,1)),
        ((1,0,3,53,1),), ((0,0,1,54,1),(0,0,2,55,1)), ((0,0,0,56,1),), (), (),
    ),
)
ORDER = (14570689, 14437003, 1713117, 575407)


def contract_last(left, right):
    return lax.dot_general(
        left, right, (((1,), (1,)), ((), ())), preferred_element_type=jnp.float32
    )


def whole_kernel(
    count,
    heads,
    patches,
    cls_token,
    pos_embed,
    ln1_gain,
    ln1_bias,
    patch_weight,
    w_query,
    w_key,
    w_value,
    w_out,
    head_w,
    lnf_gain,
    lnf_bias,
    head_bias,
    out,
    own_patches,
    cls_row,
    position,
    gain_row,
    bias_row,
    embed,
    query_w,
    key_w,
    value_w,
    out_w,
    class_w,
    last_gain,
    last_bias,
    class_bias,
    slots,
    basis,
    scaled,
    form,
    folded,
    constants,
    kept,
    gathered,
    peak,
    total,
    part,
    from_pair,
    ring,
    result,
    load_sem,
    recv_sem,
    sent_sem,
    known_sem,
    tail_send,
    tail_recv,
    spread_sem,
):
    f32, bf16 = jnp.float32, jnp.bfloat16
    me = lax.axis_index("sample")
    core = me % 2
    side = (me // 2) % 2
    chip = me // 2
    chips = count // 2
    plane = me // PLANE
    images, rows, depth = own_patches.shape
    padded = slots.shape[1]
    lanes = slots.shape[2]
    tiles = padded // TILE_ROWS
    cuts = tuple(TILE_ROWS * (tiles * place // PIECES) for place in range(PIECES + 1))
    width = embed.shape[1]
    inner = query_w.shape[1]
    head_dim = inner // heads
    pairs = heads * images
    spots = position.shape[0] - 1

    loads = []
    for index, (source, target) in enumerate(
        (
            (patches, own_patches),
            (pos_embed.at[0], position),
            (cls_token, cls_row),
            (ln1_gain, gain_row),
            (ln1_bias, bias_row),
            (patch_weight.at[0], embed),
            (w_query.at[0], query_w),
            (w_key.at[0], key_w),
            (w_value.at[0], value_w),
            (w_out.at[0], out_w),
            (head_w.at[0], class_w),
            (lnf_gain, last_gain),
            (lnf_bias, last_bias),
            (head_bias, class_bias),
        )
    ):
        load = pltpu.make_async_copy(source, target, load_sem.at[index])
        load.start()
        loads.append(load)

    twin = me + 1 - 2 * core
    beside = plane * PLANE + (1 - side) * 2 + core
    here = tuple(lax.convert_element_type(plane == place, jnp.int32) for place in range(LINE))
    line_of = tuple(
        (place * PLANE + (1 - side) * 2 + core, place * PLANE + side * 2 + core)
        for place in range(LINE)
    )

    barrier = pltpu.get_barrier_semaphore()

    def greet(target):
        pl.semaphore_signal(barrier, inc=1, device_id={"sample": target}, device_id_type=MESH)

    greet(twin)
    greet(beside)

    @pl.when(plane > 0)
    def _():
        greet(me - PLANE)

    @pl.when(plane < LINE - 1)
    def _():
        greet(me + PLANE)

    loads[0].wait()
    eye = (
        lax.broadcasted_iota(jnp.int32, (padded, depth), 0)
        == lax.broadcasted_iota(jnp.int32, (padded, depth), 1)
    ).astype(bf16)
    flat = own_patches[...].reshape(images * rows, depth)
    slots[me] = contract_last(eye, flat).astype(bf16)
    pl.semaphore_wait(barrier, LINE - here[0] - here[LINE - 1])

    def piece(slot, target, origin, part_of):
        low, high = cuts[part_of], cuts[part_of + 1]
        ref = slots.at[origin, pl.ds(low, high - low)]
        return pltpu.make_async_remote_copy(
            src_ref=ref,
            dst_ref=ref,
            send_sem=sent_sem.at[slot],
            recv_sem=recv_sem.at[origin, part_of],
            device_id={"sample": target},
            device_id_type=MESH,
        )

    def sent(place, slot):
        to, aside, origin, own, part_of = SENDS[place][slot]
        target = twin if aside == 2 else line_of[to][aside]
        return piece(slot, target, line_of[origin][own], part_of)

    def tell(target, entered):
        pl.semaphore_signal(
            known_sem.at[entered], inc=1, device_id={"sample": target}, device_id_type=MESH
        )

    def learn(place, entered):
        pl.semaphore_wait(known_sem.at[entered], 1)
        if place == 1 and entered == 3:
            tell(me - PLANE, 3)
        if place == 2 and entered == 0:
            tell(me + PLANE, 0)

    for place in (1, 2):

        @pl.when(plane == place)
        def _(place=place):
            tell(me - PLANE, place + 1)
            tell(me + PLANE, place - 1)

    def events(group):
        for place in range(LINE):
            entries = EVENTS[place][group]
            if entries:

                @pl.when(plane == place)
                def _(place=place, entries=entries):
                    for origin, own, part_of, low, number in entries:
                        if origin == -2:
                            learn(place, own)
                        if origin >= 0:
                            piece(0, twin, line_of[origin][own], part_of).wait_recv()
                        for slot in range(low, low + number):
                            sent(place, slot).start()

    events(0)

    for index in (1, 2, 3, 4):
        loads[index].wait()
    events(1)
    gain = gain_row[...]
    bias = bias_row[...]
    leading = cls_row[...].astype(f32) + position[0:1, :].astype(f32)
    lead = jnp.broadcast_to(layer_norm(leading, gain, bias), (TILE_ROWS, width)).astype(bf16)
    lead_row = lead[:1].astype(f32)

    events(2)
    placed = position[...].astype(f32)[1:]
    placed = placed - jnp.mean(placed, axis=1, keepdims=True)
    top = 2 * heads
    basis[top + padded :, :] = placed.astype(bf16)
    scaled[padded : padded + spots, :] = (placed * gain).astype(bf16)
    scaled[padded + spots :, :] = jnp.zeros((scaled.shape[0] - padded - spots, width), bf16)
    weight = jnp.sum(placed * placed, axis=1, keepdims=True)
    weight = jnp.transpose(jnp.broadcast_to(weight, (spots, 128)))[:1]

    loads[5].wait()
    table = embed[...].astype(f32)
    table = table - jnp.mean(table, axis=1, keepdims=True)
    table = jnp.concatenate([table, jnp.zeros((padded - depth, width), f32)], axis=0)
    basis[top : top + padded, :] = table.astype(bf16)
    scaled[:padded, :] = (table * gain).astype(bf16)

    events(3)
    loads[6].wait()
    query = jnp.dot(lead, query_w[...], preferred_element_type=f32)[:1]
    head_row = lax.broadcasted_iota(jnp.int32, (TILE_ROWS, inner), 0)
    column = lax.broadcasted_iota(jnp.int32, (TILE_ROWS, inner), 1)
    own_head = (column >= head_row * head_dim) & (column < (head_row + 1) * head_dim)
    spread = jnp.where(own_head, jnp.broadcast_to(query, (TILE_ROWS, inner)), 0.0).astype(bf16)
    events(4)
    loads[7].wait()
    turned = contract_last(spread, key_w[...])[:heads] * (1.0 / math.sqrt(head_dim))
    first = jnp.sum(turned * lead_row, axis=1, keepdims=True)
    level = jnp.sum(turned * bias, axis=1, keepdims=True)
    constants[...] = jnp.broadcast_to(level, constants.shape)
    basis[:top, :] = split_in_two(turned * gain)

    features = padded + spots
    for part_of in range(GRAM_PARTS):
        events(5 + part_of)
        low = 256 * (pl.cdiv(features, 256) * part_of // GRAM_PARTS)
        high = min(features, 256 * (pl.cdiv(features, 256) * (part_of + 1) // GRAM_PARTS))
        square = contract_last(basis[: top + padded, :], basis[top + low : top + high, :])
        place = low + lax.broadcasted_iota(jnp.int32, (padded, high - low), 1)
        form[top : top + padded, low:high] = jnp.where(
            place < padded, square[top:], 2.0 * square[top:]
        ).astype(bf16)
        form[:top, low:high] = split_in_two(square[:heads] + square[heads:top])
    sizes = jnp.concatenate([jnp.zeros((1, padded), f32), weight], axis=1)
    sizes_high = sizes.astype(bf16).astype(f32)
    sizes = jnp.concatenate(
        [sizes_high, sizes - sizes_high, jnp.zeros((TILE_ROWS - 2, padded + spots), f32)], axis=0
    )
    form[top + padded :, :] = sizes.astype(bf16)

    loads[8].wait()
    ends = jnp.concatenate([split_in_two(bias), lead[:1], jnp.zeros((TILE_ROWS - 3, width), bf16)], axis=0)
    ends = jnp.dot(ends, value_w[...], preferred_element_type=f32)
    plain = ends[0:1] + ends[1:2]
    lead_value = ends[2:3]

    first = jnp.broadcast_to(first[None], (images, heads, 1)).reshape(pairs, 1)
    peak[...] = jnp.broadcast_to(first, peak.shape)
    total[...] = jnp.ones(total.shape, f32)
    gathered[...] = jnp.zeros(gathered.shape, f32)

    cells = 2 * lanes
    lane = lax.broadcasted_iota(jnp.int32, (pairs, cells), 1)
    row_image = lax.broadcasted_iota(jnp.int32, (pairs, cells), 0) // heads
    same = (lane % lanes) // rows == row_image
    spot_row = lax.broadcasted_iota(jnp.int32, (spots, cells), 0)
    spot_lane = lax.broadcasted_iota(jnp.int32, (spots, cells), 1)
    spot_at = spot_row - (spot_lane // lanes) * rows - spot_lane % rows

    order = sum(mine * packed for mine, packed in zip(here, ORDER, strict=True))
    first_step = 5 + GRAM_PARTS
    fold_rows = scaled.shape[0] // FOLD_PARTS

    def base_of(turn):
        code = (order >> (3 * turn)) % 8
        where, own = code // 2, code % 2
        return where * PLANE + 2 * (side * own + (1 - side) * (1 - own))

    def block_of(base):
        block = jnp.concatenate([slots[base], slots[base + 1]], axis=1)
        spot = jnp.where(spot_at == base * rows, 1.0, 0.0).astype(bf16)
        return jnp.concatenate([block, spot], axis=0)

    def front(base):
        block = block_of(base)
        image = jnp.dot(form[...], block, preferred_element_type=f32)
        norm = jnp.sum(
            image[top : top + padded] * block[:padded].astype(f32), axis=0, keepdims=True
        )
        tail = top + padded
        norm = norm + image[tail : tail + 1] + image[tail + 1 : tail + 2]
        rate = lax.rsqrt(norm * (1.0 / width) + epsilon)
        scores = image[:heads] + image[heads:top]
        kept[:heads, :] = scores * rate + constants[:, :1]
        kept[heads:, :] = jnp.broadcast_to(rate, (heads, cells))

    def back(base, scores, rate):
        block = block_of(base)
        scores = jnp.broadcast_to(scores[None], (images, heads, cells)).reshape(pairs, cells)
        scores = jnp.where(same, scores, LOWEST)
        before = peak[:, :1]
        now = jnp.maximum(before, jnp.max(scores, axis=1, keepdims=True))
        shrink = jnp.exp(before - now)
        chance = jnp.where(same, jnp.exp(scores - now), 0.0)
        peak[...] = jnp.broadcast_to(now, peak.shape)
        total[...] = total[...] * shrink + jnp.sum(chance, axis=1, keepdims=True)
        gathered[...] = gathered[...] * shrink + contract_last((chance * rate).astype(bf16), block)

    def twin_pieces(base):
        for part_of in range(PIECES):
            piece(0, twin, base + 1 - core, part_of).wait_recv()

    def chip_step(turn, carry):
        for index in range(1, 2 * LINE - 1):
            pl.when(turn == index)(functools.partial(events, first_step + 2 * index))
        base = base_of(turn)
        twin_pieces(base)
        scores = kept[:heads, :]
        rate = kept[heads : heads + 1, :]
        back(base_of(turn - 1), scores, rate)
        front(base)

        for index in range(1, FOLD_PARTS + 1):
            pl.when(turn == index)(functools.partial(events, first_step + 2 * index + 1))

        @pl.when(turn <= FOLD_PARTS)
        def _():
            low = pl.multiple_of((turn - 1) * fold_rows, TILE_ROWS)
            folded[pl.ds(low, fold_rows), :] = jnp.dot(
                scaled[pl.ds(low, fold_rows), :], value_w[...], preferred_element_type=f32
            ).astype(bf16)

        return carry

    events(first_step)
    twin_pieces(base_of(0))
    front(base_of(0))
    events(first_step + 1)
    lax.fori_loop(1, 2 * LINE - 1, chip_step, 0)
    back(base_of(2 * LINE - 2), kept[:heads, :], kept[heads : heads + 1, :])
    events(first_step + 4 * LINE - 2)
    twin_pieces(base_of(2 * LINE - 1))
    front(base_of(2 * LINE - 1))
    back(base_of(2 * LINE - 1), kept[:heads, :], kept[heads : heads + 1, :])

    whole = total[:, :1]
    lead_chance = jnp.exp(first - peak[:, :1]) / whole
    pooled = split_in_two(gathered[...] / whole)
    values = jnp.dot(pooled, folded[: padded + spots, :], preferred_element_type=f32)
    values = values[:pairs] + values[pairs:] + plain * (1.0 - lead_chance) + lead_value * lead_chance
    pair_head = lax.broadcasted_iota(jnp.int32, (pairs, inner), 0) % heads
    pair_column = lax.broadcasted_iota(jnp.int32, (pairs, inner), 1)
    mine_only = (pair_column >= pair_head * head_dim) & (pair_column < (pair_head + 1) * head_dim)
    values = jnp.where(mine_only, values, 0.0)
    mixed = jnp.sum(values.reshape(images, heads, inner), axis=1).astype(bf16)
    loads[9].wait()
    hidden = leading + jnp.dot(mixed, out_w[...], preferred_element_type=f32)
    for index in (10, 11, 12, 13):
        loads[index].wait()
    final = layer_norm(hidden, last_gain[...], last_bias[...]).astype(bf16)
    logits = contract_last(final, class_w[...]) + class_bias[...]
    lifted = logits - jnp.max(logits, axis=-1, keepdims=True)
    logp = lifted - jnp.log(jnp.sum(jnp.exp(lifted), axis=-1, keepdims=True))

    piece_width = part.shape[2]
    classes = out.shape[1]
    part[0] = logp[:, :piece_width]
    part[1] = jnp.concatenate(
        [logp[:, piece_width:], jnp.zeros((images, 2 * piece_width - classes), f32)], axis=1
    )
    swap = pltpu.make_async_remote_copy(
        src_ref=part.at[1 - core],
        dst_ref=from_pair,
        send_sem=tail_send.at[0],
        recv_sem=tail_recv.at[0],
        device_id={"sample": twin},
        device_id_type=MESH,
    )
    swap.start()
    swap.wait_recv()
    mine = part[core]
    theirs = from_pair[...]
    high = jnp.maximum(mine, theirs)
    ring[chip] = high + jnp.log(jnp.exp(mine - high) + jnp.exp(theirs - high))

    def pass_on(origin, target, step):
        return pltpu.make_async_remote_copy(
            src_ref=ring.at[origin],
            dst_ref=ring.at[origin],
            send_sem=spread_sem.at[step],
            recv_sem=tail_recv.at[2 + origin],
            device_id={"sample": target},
            device_id_type=MESH,
        )

    for step in range(1, chips):
        other = step - 1 + jnp.minimum(step // jnp.maximum(chip + 1, 1), 1)
        pass_on(chip, 2 * other + core, step).start()
    for step in range(1, chips):
        pass_on((chip + step) % chips, me, step).wait_recv()
    every = ring[...]
    high = jnp.max(every, axis=0)
    result[core] = high + jnp.log(jnp.sum(jnp.exp(every - high[None]), axis=0)) - math.log(count)
    share = pltpu.make_async_remote_copy(
        src_ref=result.at[core],
        dst_ref=result.at[core],
        send_sem=tail_send.at[1],
        recv_sem=tail_recv.at[1],
        device_id={"sample": twin},
        device_id_type=MESH,
    )
    share.start()

    for place in range(LINE):

        @pl.when(plane == place)
        def _(place=place):
            for slot in range(len(SENDS[place])):
                sent(place, slot).wait_send()

    swap.wait_send()
    for step in range(1, chips):
        pass_on(chip, twin, step).wait_send()
    pltpu.make_async_remote_copy(
        src_ref=result.at[core],
        dst_ref=result.at[1 - core],
        send_sem=tail_send.at[1],
        recv_sem=tail_recv.at[1],
        device_id={"sample": twin},
        device_id_type=MESH,
    ).wait_recv()
    share.wait_send()
    out[:, :piece_width] = result[0]
    out[:, piece_width:] = result[1][:, : classes - piece_width]


def kernel_shards(
    patches,
    patch_weight,
    cls_token,
    pos_embed,
    ln1_gain,
    ln1_bias,
    w_query,
    w_key,
    w_value,
    w_out,
    lnf_gain,
    lnf_bias,
    head_w,
    head_bias,
):
    count = lax.axis_size("sample")
    images, rows, depth = patches.shape
    width = patch_weight.shape[2]
    inner = w_query.shape[2]
    heads = inner // HEAD_DIM
    pairs = heads * images
    chips = count // 2
    classes = head_w.shape[2]
    piece_width = pl.cdiv(classes, 256) * 128
    padded = pl.cdiv(depth, TILE_ROWS) * TILE_ROWS
    spots = pos_embed.shape[1] - 1
    fold_rows = pl.cdiv(padded + spots, FOLD_PARTS * TILE_ROWS) * FOLD_PARTS * TILE_ROWS
    far = pl.BlockSpec(memory_space=pl.ANY)
    dma = pltpu.SemaphoreType.DMA
    f32, bf16 = jnp.float32, jnp.bfloat16
    class_rows = jnp.swapaxes(head_w, 1, 2)
    given = (
        patches,
        cls_token,
        pos_embed,
        ln1_gain,
        ln1_bias,
        patch_weight,
        w_query,
        w_key,
        w_value,
        w_out,
        class_rows,
        lnf_gain,
        lnf_bias,
        head_bias,
    )
    held = [
        pltpu.VMEM(a.shape[1:] if place and a.ndim == 3 else a.shape, a.dtype)
        for place, a in enumerate(given)
    ]
    return pl.pallas_call(
        functools.partial(whole_kernel, count, heads),
        out_shape=jax.ShapeDtypeStruct((images, classes), f32),
        in_specs=[far] * len(given),
        out_specs=pl.BlockSpec(memory_space=pltpu.VMEM),
        scratch_shapes=[
            *held,
            pltpu.VMEM((count, padded, images * rows), bf16),
            pltpu.VMEM((2 * heads + padded + spots, width), bf16),
            pltpu.VMEM((fold_rows, width), bf16),
            pltpu.VMEM((padded + 2 * heads + TILE_ROWS, padded + spots), bf16),
            pltpu.VMEM((fold_rows, inner), bf16),
            pltpu.VMEM((heads, 128), f32),
            pltpu.VMEM((2 * heads, 2 * images * rows), f32),
            pltpu.VMEM((pairs, padded + spots), f32),
            pltpu.VMEM((pairs, 128), f32),
            pltpu.VMEM((pairs, 128), f32),
            pltpu.VMEM((2, images, piece_width), f32),
            pltpu.VMEM((images, piece_width), f32),
            pltpu.VMEM((chips, images, piece_width), f32),
            pltpu.VMEM((2, images, piece_width), f32),
            dma((len(given),)),
            dma((count, PIECES)),
            dma((max(len(place) for place in SENDS),)),
            pltpu.SemaphoreType.REGULAR((LINE,)),
            dma((2,)),
            dma((2 + chips,)),
            dma((chips,)),
        ],
        compiler_params=pltpu.CompilerParams(
            collective_id=0, has_side_effects=True, vmem_limit_bytes=60 << 20
        ),
    )(*given)


def takes_kernel(mesh, patches):
    count = mesh.shape["sample"]
    rows = patches.shape[1] // count
    images = patches.shape[0] // mesh.shape["group"]
    return count == PLANE * LINE and rows % TILE_ROWS == 0 and images * rows == 128


def solution(mesh):
    placed = (
        P("group", "sample", None),
        P("sample", None, None),
        P("sample", None),
        P("sample", None, None),
        P("sample", None),
        P("sample", None),
        P("sample", None, None),
        P("sample", None, None),
        P("sample", None, None),
        P("sample", None, None),
        P("sample", None),
        P("sample", None),
        P("sample", None, None),
        P("sample", None),
    )

    def run(*arrays):
        step = kernel_shards if takes_kernel(mesh, arrays[0]) else shards
        return jax.shard_map(
            step, mesh=mesh, in_specs=placed, out_specs=P("group", None), check_vma=False
        )(*arrays)

    return run
```

```python
import functools
import math

import jax
import jax.numpy as jnp
from jax import lax
from jax.experimental import pallas as pl
from jax.experimental.pallas import tpu as pltpu
from jax.sharding import PartitionSpec as P

HEAD_DIM = 80


epsilon = 1e-06


def combined_all(part, axis, combine):
    gathered = jax.tree.map(lambda a: lax.all_gather(a, axis), part)

    def take(source):
        return jax.tree.map(lambda a: lax.dynamic_index_in_dim(a, source, 0, False), gathered)

    return lax.fori_loop(
        1, lax.axis_size(axis), lambda source, state: combine(state, take(source)), take(0)
    )


def layer_norm(values, gain, shift):
    center = values - jnp.mean(values, axis=-1, keepdims=True)
    spread = jnp.mean(center * center, axis=-1, keepdims=True)
    return center * lax.rsqrt(spread + epsilon) * gain + shift


def shards(
    patches,
    patch_weight,
    cls_token,
    pos_embed,
    ln1_gain,
    ln1_bias,
    w_query,
    w_key,
    w_value,
    w_out,
    lnf_gain,
    lnf_bias,
    head_w,
    head_bias,
):
    embed_weight = patch_weight[0]
    position = pos_embed[0]
    gain_first = ln1_gain[0]
    bias_first = ln1_bias[0]
    query_weight = w_query[0]
    pair_weight = jnp.concatenate([w_key[0], w_value[0]], axis=1)
    out_weight = w_out[0]
    width = embed_weight.shape[1]
    inner = query_weight.shape[1]
    head_count = inner // HEAD_DIM
    leading = cls_token[0].astype(jnp.float32) + position[0].astype(jnp.float32)
    lead_norm = layer_norm(leading, gain_first, bias_first).astype(jnp.bfloat16)
    lead_pair = jnp.dot(lead_norm[None], pair_weight, preferred_element_type=jnp.float32).astype(
        jnp.bfloat16
    )
    query = jnp.dot(lead_norm[None], query_weight, preferred_element_type=jnp.float32).astype(
        jnp.bfloat16
    )
    query = query.reshape(head_count, HEAD_DIM)
    portion = lax.all_gather(patches, "sample", axis=1, tiled=True)
    image_count = portion.shape[0]
    row_count = portion.shape[1]
    flat = portion.reshape(-1, portion.shape[2])
    tokens = jnp.dot(flat, embed_weight, preferred_element_type=jnp.float32).reshape(
        image_count, row_count, width
    )
    placed = lax.dynamic_slice_in_dim(position, 1, row_count, 0)
    tokens = tokens + placed.astype(jnp.float32)[None]
    normed = layer_norm(tokens, gain_first, bias_first).astype(jnp.bfloat16)
    paired = jnp.dot(normed.reshape(-1, width), pair_weight, preferred_element_type=jnp.float32)
    key_values = paired.astype(jnp.bfloat16).reshape(image_count, row_count, 2 * inner)
    image_count = key_values.shape[0]
    lead_rows = jnp.broadcast_to(lead_pair[None], (image_count, 1, 2 * inner))
    full_rows = jnp.concatenate([lead_rows, key_values], axis=1)
    key_rows = full_rows[:, :, :inner].reshape(image_count, -1, head_count, HEAD_DIM)
    value_rows = full_rows[:, :, inner:].reshape(image_count, -1, head_count, HEAD_DIM)
    scores = jnp.einsum(
        "hd,ithd->iht", query, key_rows, preferred_element_type=jnp.float32
    ) / math.sqrt(HEAD_DIM)
    attention = jax.nn.softmax(scores, axis=-1).astype(jnp.bfloat16)
    mixed = jnp.einsum("iht,ithd->ihd", attention, value_rows, preferred_element_type=jnp.float32)
    mixed = mixed.astype(jnp.bfloat16).reshape(image_count, inner)
    hidden = leading[None] + jnp.dot(mixed, out_weight, preferred_element_type=jnp.float32)
    final = layer_norm(hidden, lnf_gain[0], lnf_bias[0]).astype(jnp.bfloat16)
    logits = jnp.dot(final, head_w[0], preferred_element_type=jnp.float32) + head_bias[0]
    logp = jax.nn.log_softmax(logits, axis=-1)
    count = lax.axis_size("sample")

    def combine(earlier, later):
        highest = jnp.maximum(earlier[0], later[0])
        summed = earlier[1] * jnp.exp(earlier[0] - highest) + later[1] * jnp.exp(later[0] - highest)
        return (highest, summed)

    peak, total = combined_all((logp, jnp.ones_like(logp)), "sample", combine)
    return peak + jnp.log(total) - math.log(count)


MESH = pl.DeviceIdType.MESH
PLANE = 4
LINE = 4
TILE_ROWS = 16
LOWEST = -1e30
GRAM_PARTS = 2
FOLD_PARTS = 6


def split_in_two(values):
    high = values.astype(jnp.bfloat16)
    low = (values - high.astype(jnp.float32)).astype(jnp.bfloat16)
    return jnp.concatenate([high, low], axis=0)


PIECES = 4
SENDS = (
    (
        (0,0,0,1,0), (1,1,0,1,0), (1,1,0,1,2), (1,1,0,1,3), (0,0,0,1,3), (0,0,0,1,1), (1,1,0,1,1),
        (0,0,0,1,2), (0,2,0,1,0), (0,2,0,1,1), (0,2,0,1,2), (0,2,0,1,3), (2,1,0,1,1), (1,1,0,0,0),
        (0,2,0,0,0), (0,0,1,1,0), (0,2,1,1,0), (2,1,0,0,3), (3,1,0,0,3), (1,1,0,0,3), (0,2,0,0,3),
        (0,0,1,1,2), (0,2,1,1,2), (1,1,0,0,1), (2,1,0,0,1), (0,2,0,0,1), (0,0,1,1,1), (0,2,1,1,1),
        (2,1,0,0,2), (3,1,0,0,2), (0,2,0,0,2), (0,0,1,1,3), (0,2,1,1,3), (0,2,1,0,0), (0,2,1,0,2),
        (0,0,2,1,1), (0,2,2,1,1), (0,2,1,0,1), (0,0,2,1,2), (0,2,2,1,2), (0,2,1,0,3), (0,0,2,1,3),
        (0,2,2,1,3), (0,0,2,1,0), (0,2,2,1,0), (0,2,2,0,1), (0,2,3,1,3), (0,2,2,0,2), (0,2,3,0,1),
        (0,0,3,1,0), (0,2,3,1,0), (0,2,2,0,3), (0,2,3,0,3), (0,2,2,0,0), (0,2,3,1,2), (0,2,3,0,2),
        (0,2,3,1,1), (0,2,3,0,0),
    ),
    (
        (0,1,1,1,0), (2,1,1,1,1), (1,0,1,1,1), (2,1,1,1,0), (0,1,1,1,2), (2,1,1,1,2), (1,0,1,1,0),
        (0,1,1,1,1), (0,1,1,1,3), (1,0,1,1,3), (1,0,1,1,2), (2,1,1,1,3), (1,2,1,1,0), (1,2,1,1,1),
        (1,2,1,1,2), (1,2,1,1,3), (2,1,0,1,0), (1,2,0,1,0), (1,2,1,0,1), (2,1,0,1,2), (1,0,0,1,2),
        (1,2,0,1,2), (1,2,1,0,0), (1,0,2,1,1), (0,1,2,1,1), (1,2,2,1,1), (2,1,0,1,3), (1,2,0,1,3),
        (1,2,1,0,3), (0,1,2,1,2), (1,0,2,1,2), (1,2,2,1,2), (1,2,0,1,1), (1,2,1,0,2), (0,1,2,1,3),
        (1,0,2,1,3), (1,2,2,1,3), (0,1,2,1,0), (1,0,2,1,0), (1,2,2,1,0), (1,2,0,0,2), (1,2,0,0,0),
        (0,1,3,1,3), (1,0,3,1,3), (1,2,3,1,3), (1,2,2,0,1), (1,2,2,0,2), (0,1,3,1,0), (1,0,3,1,0),
        (1,2,3,1,0), (1,2,2,0,3), (1,2,2,0,0), (1,2,3,0,1), (1,2,0,0,3), (1,0,3,1,2), (0,1,3,1,2),
        (1,2,3,1,2), (1,2,3,0,3), (1,2,0,0,1), (0,1,3,1,1), (1,2,3,1,1), (1,2,3,0,0), (1,2,3,0,2),
    ),
    (
        (1,1,2,1,1), (2,0,2,1,1), (3,1,2,1,0), (1,1,2,1,2), (2,0,2,1,3), (1,1,2,1,3), (1,1,2,1,0),
        (3,1,2,1,2), (3,1,2,1,1), (2,0,2,1,2), (3,1,2,1,3), (2,2,2,1,0), (2,2,2,1,1), (2,2,2,1,2),
        (2,2,2,1,3), (3,1,1,1,1), (2,0,1,1,1), (2,2,1,1,1), (3,1,1,1,0), (2,0,1,1,0), (2,2,1,1,0),
        (2,2,2,0,1), (3,1,1,1,2), (2,0,1,1,2), (2,2,1,1,2), (1,1,3,1,0), (2,0,3,1,0), (2,2,3,1,0),
        (2,2,2,0,3), (1,1,3,1,2), (2,0,3,1,2), (2,2,3,1,2), (2,2,2,0,2), (3,1,1,1,3), (2,0,1,1,3),
        (2,2,1,1,3), (1,1,3,1,1), (2,2,3,1,1), (2,2,1,0,1), (3,1,0,1,1), (2,0,2,1,0), (2,2,0,1,1),
        (2,0,0,1,0), (3,1,0,1,0), (2,2,0,1,0), (2,2,3,1,3), (2,2,1,0,0), (3,1,0,1,2), (2,2,0,1,2),
        (2,2,1,0,2), (2,2,3,0,1), (2,2,0,0,3), (2,2,3,0,0), (3,1,0,1,3), (2,2,0,1,3), (2,2,3,0,2),
        (2,2,1,0,3), (2,2,2,0,0), (2,2,0,0,0), (2,2,3,0,3), (2,2,0,0,1), (2,2,0,0,2),
    ),
    (
        (2,1,3,1,0), (3,0,3,1,1), (2,1,3,1,2), (3,0,3,1,3), (2,1,3,1,1), (2,1,3,1,3), (3,0,3,1,2),
        (3,2,3,1,0), (3,2,3,1,1), (3,2,3,1,2), (3,2,3,1,3), (1,1,3,1,3), (3,0,2,1,0), (3,2,2,1,0),
        (3,0,3,1,0), (2,1,3,0,1), (1,1,3,0,1), (0,1,3,0,1), (3,2,3,0,1), (3,0,2,1,2), (3,2,2,1,2),
        (2,1,3,0,3), (0,1,3,0,3), (3,2,3,0,3), (3,0,2,1,1), (3,2,2,1,1), (0,1,3,0,2), (3,2,3,0,2),
        (3,0,2,1,3), (3,2,2,1,3), (3,0,1,1,1), (3,2,1,1,1), (3,2,2,0,0), (3,0,1,1,0), (3,2,1,1,0),
        (3,0,1,1,2), (3,2,1,1,2), (3,2,3,0,0), (3,2,2,0,2), (3,2,2,0,1), (3,0,1,1,3), (3,2,1,1,3),
        (3,2,2,0,3), (3,0,0,1,1), (3,2,0,1,1), (3,2,0,0,3), (3,2,1,0,1), (3,0,0,1,0), (3,2,0,1,0),
        (3,2,1,0,0), (3,2,0,1,2), (3,2,1,0,2), (3,2,0,1,3), (3,2,1,0,3), (3,2,0,0,1), (3,2,0,0,2),
        (3,2,0,0,0),
    ),
)
EVENTS = (
    (
        ((-1,0,0,0,12),), (), (), ((-2,2,0,12,1),), (), (), ((0,0,0,13,2),(-2,3,0,15,0),(1,1,0,15,2)),
        ((0,0,3,17,4),(1,1,2,21,2),(0,0,1,23,3)), ((1,1,1,26,2),(0,0,2,28,3),(1,1,3,31,2)), (),
        ((1,0,0,33,1),), (), ((1,0,2,34,1),(2,1,1,35,2)), ((1,0,1,37,1),(2,1,2,38,2),(1,0,3,40,1)),
        ((2,1,3,41,2),(2,1,0,43,2)), (), ((2,0,1,45,1),(3,1,3,46,1),(2,0,2,47,1),(3,0,1,48,1)),
        ((3,1,0,49,2),(2,0,3,51,1),(3,0,3,52,1),(2,0,0,53,1)), ((3,1,2,54,1),(3,0,2,55,1),(3,1,1,56,1)),
        ((3,0,0,57,1),), (), (),
    ),
    (
        ((-1,0,0,0,16),), (), (), (), ((-2,3,0,16,0),), ((0,1,0,16,2),), ((1,0,1,18,1),(0,1,2,19,3)),
        ((1,0,0,22,1),(2,1,1,23,3),(0,1,3,26,2),(1,0,3,28,1),(2,1,2,29,3),(0,1,1,32,1)),
        ((1,0,2,33,1),(2,1,3,34,3)), ((2,1,0,37,3),), ((0,0,2,40,1),), ((0,0,0,41,1),),
        ((3,1,3,42,3),(2,0,1,45,1)), (), ((2,0,2,46,1),(3,1,0,47,3)), ((2,0,3,50,1),(2,0,0,51,1)),
        ((3,0,1,52,1),(0,0,3,53,1),(3,1,2,54,3),(3,0,3,57,1),(0,0,1,58,1)), ((3,1,1,59,2),), ((3,0,0,61,1),),
        (), (), ((3,0,2,62,1),),
    ),
    (
        ((-1,0,0,0,15),), ((-2,0,0,15,0),), (), (), (), ((1,1,1,15,3),),
        ((1,1,0,18,3),(2,0,1,21,1),(1,1,2,22,3)),
        ((3,1,0,25,3),(2,0,3,28,1),(3,1,2,29,3),(2,0,2,32,1),(1,1,3,33,3)),
        ((3,1,1,36,2),(1,0,1,38,1),(0,1,1,39,3),(0,1,0,42,3),(3,1,3,45,1)), (), ((1,0,0,46,1),(0,1,2,47,2)),
        ((1,0,2,49,1),(3,0,1,50,1)), ((0,0,3,51,1),(3,0,0,52,1)), ((0,1,3,53,2),(3,0,2,55,1)),
        ((1,0,3,56,1),(2,0,0,57,1)), (), ((0,0,0,58,1),(3,0,3,59,1),(0,0,1,60,1)), ((0,0,2,61,1),), (), (),
        (), (),
    ),
    (
        ((-1,0,0,0,11),), ((-2,1,0,11,1),(-2,0,0,12,0)), (), (), (), ((2,1,0,12,2),),
        ((3,0,1,14,5),(2,1,2,19,2)), ((3,0,3,21,3),(2,1,1,24,2),(3,0,2,26,2),(2,1,3,28,2)),
        ((1,1,1,30,2),(2,0,0,32,1)), ((1,1,0,33,2),), ((1,1,2,35,2),(3,0,0,37,1)), (),
        ((2,0,2,38,1),(2,0,1,39,1),(1,1,3,40,2)), ((2,0,3,42,1),(0,1,1,43,2)),
        ((0,0,3,45,1),(1,0,1,46,1),(0,1,0,47,2)), ((1,0,0,49,1),(0,1,2,50,1)), ((1,0,2,51,1),(0,1,3,52,1)),
        ((1,0,3,53,1),), ((0,0,1,54,1),(0,0,2,55,1)), ((0,0,0,56,1),), (), (),
    ),
)
ORDER = (14570689, 14437003, 1713117, 575407)


def contract_last(left, right):
    return lax.dot_general(
        left, right, (((1,), (1,)), ((), ())), preferred_element_type=jnp.float32
    )


def whole_kernel(
    count,
    heads,
    patches,
    cls_token,
    pos_embed,
    ln1_gain,
    ln1_bias,
    patch_weight,
    w_query,
    w_key,
    w_value,
    w_out,
    head_w,
    lnf_gain,
    lnf_bias,
    head_bias,
    out,
    own_patches,
    cls_row,
    position,
    gain_row,
    bias_row,
    embed,
    query_w,
    key_w,
    value_w,
    out_w,
    class_w,
    last_gain,
    last_bias,
    class_bias,
    slots,
    basis,
    scaled,
    form,
    folded,
    ends,
    constants,
    kept,
    gathered,
    peak,
    total,
    part,
    from_pair,
    ring,
    result,
    load_sem,
    recv_sem,
    twin_sem,
    sent_sem,
    known_sem,
    tail_send,
    tail_recv,
):
    f32, bf16 = jnp.float32, jnp.bfloat16
    me = lax.axis_index("sample")
    core = me % 2
    side = (me // 2) % 2
    chip = me // 2
    chips = count // 2
    plane = me // PLANE
    images, rows, depth = own_patches.shape
    padded = slots.shape[1]
    lanes = slots.shape[2]
    tiles = padded // TILE_ROWS
    cuts = tuple(TILE_ROWS * (tiles * place // PIECES) for place in range(PIECES + 1))
    width = embed.shape[1]
    inner = query_w.shape[1]
    head_dim = inner // heads
    pairs = heads * images
    spots = position.shape[0] - 1

    loads = []
    for index, (source, target) in enumerate(
        (
            (patches, own_patches),
            (pos_embed.at[0], position),
            (cls_token, cls_row),
            (ln1_gain, gain_row),
            (ln1_bias, bias_row),
            (patch_weight.at[0], embed),
            (w_query.at[0], query_w),
            (w_key.at[0], key_w),
            (w_value.at[0], value_w),
            (w_out.at[0], out_w),
            (head_w.at[0], class_w),
            (lnf_gain, last_gain),
            (lnf_bias, last_bias),
            (head_bias, class_bias),
        )
    ):
        load = pltpu.make_async_copy(source, target, load_sem.at[index])
        load.start()
        loads.append(load)

    twin = me + 1 - 2 * core
    beside = plane * PLANE + (1 - side) * 2 + core
    here = tuple(lax.convert_element_type(plane == place, jnp.int32) for place in range(LINE))
    line_of = tuple(
        (place * PLANE + (1 - side) * 2 + core, place * PLANE + side * 2 + core)
        for place in range(LINE)
    )

    barrier = pltpu.get_barrier_semaphore()

    def greet(target):
        pl.semaphore_signal(barrier, inc=1, device_id={"sample": target}, device_id_type=MESH)

    greet(twin)
    greet(beside)

    @pl.when(plane > 0)
    def _():
        greet(me - PLANE)

    @pl.when(plane < LINE - 1)
    def _():
        greet(me + PLANE)

    loads[0].wait()
    eye = (
        lax.broadcasted_iota(jnp.int32, (padded, depth), 0)
        == lax.broadcasted_iota(jnp.int32, (padded, depth), 1)
    ).astype(bf16)
    flat = own_patches[...].reshape(images * rows, depth)
    slots[me] = contract_last(eye, flat).astype(bf16)
    pl.semaphore_wait(barrier, LINE - here[0] - here[LINE - 1])

    def passing(ref, target, sent_by, got_by):
        return pltpu.make_async_remote_copy(
            src_ref=ref,
            dst_ref=ref,
            send_sem=sent_by,
            recv_sem=got_by,
            device_id={"sample": target},
            device_id_type=MESH,
        )

    def rows_of(part_of):
        return pl.ds(cuts[part_of], cuts[part_of + 1] - cuts[part_of])

    def sent(place, slot):
        to, aside, origin, own, part_of = SENDS[place][slot]
        inside = aside // 2
        source = line_of[origin][own]
        got_by = twin_sem.at[source // 2] if inside else recv_sem.at[source // 2, part_of]
        target = twin if inside else line_of[to][aside]
        ref = slots.at[source, rows_of(part_of)]
        return passing(ref, target, sent_sem.at[inside, part_of], got_by)

    def got(source, part_of):
        ref = slots.at[source, rows_of(part_of)]
        passing(ref, twin, sent_sem.at[0, 0], recv_sem.at[source // 2, part_of]).wait_recv()

    def got_from_twin(base):
        ref = slots.at[base + 1 - core]
        passing(ref, twin, sent_sem.at[0, 0], twin_sem.at[base // 2]).wait_recv()

    def all_sent(place):
        for inside in range(2):
            for part_of in range(PIECES):
                number = sum(
                    1 for entry in SENDS[place] if (entry[1] // 2, entry[4]) == (inside, part_of)
                )
                ref = slots.at[pl.ds(0, number), rows_of(part_of)]
                passing(ref, twin, sent_sem.at[inside, part_of], twin_sem.at[0]).wait_send()

    def tell(target, entered):
        pl.semaphore_signal(
            known_sem.at[entered], inc=1, device_id={"sample": target}, device_id_type=MESH
        )

    def learn(place, entered):
        pl.semaphore_wait(known_sem.at[entered], 1)
        if place == 1 and entered == 3:
            tell(me - PLANE, 3)
        if place == 2 and entered == 0:
            tell(me + PLANE, 0)

    for place in (1, 2):

        @pl.when(plane == place)
        def _(place=place):
            tell(me - PLANE, place + 1)
            tell(me + PLANE, place - 1)

    def events(group):
        for place in range(LINE):
            entries = EVENTS[place][group]
            if entries:

                @pl.when(plane == place)
                def _(place=place, entries=entries):
                    for origin, own, part_of, low, number in entries:
                        if origin == -2:
                            learn(place, own)
                        if origin >= 0:
                            got(line_of[origin][own], part_of)
                        for slot in range(low, low + number):
                            sent(place, slot).start()

    events(0)

    for index in (1, 2, 3, 4):
        loads[index].wait()
    events(1)
    gain = gain_row[...]
    bias = bias_row[...]
    leading = cls_row[...].astype(f32) + position[0:1, :].astype(f32)
    lead = jnp.broadcast_to(layer_norm(leading, gain, bias), (TILE_ROWS, width)).astype(bf16)
    lead_row = lead[:1].astype(f32)

    events(2)
    placed = position[...].astype(f32)[1:]
    placed = placed - jnp.mean(placed, axis=1, keepdims=True)
    top = 2 * heads
    basis[top + padded :, :] = placed.astype(bf16)
    scaled[padded : padded + spots, :] = (placed * gain).astype(bf16)
    scaled[padded + spots :, :] = jnp.concatenate(
        [split_in_two(bias), lead[:1], jnp.zeros((ends.shape[0] - 3, width), bf16)], axis=0
    )
    weight = jnp.sum(placed * placed, axis=1, keepdims=True)
    weight = jnp.transpose(jnp.broadcast_to(weight, (spots, 128)))[:1]

    loads[5].wait()
    table = embed[...].astype(f32)
    table = table - jnp.mean(table, axis=1, keepdims=True)
    table = jnp.concatenate([table, jnp.zeros((padded - depth, width), f32)], axis=0)
    basis[top : top + padded, :] = table.astype(bf16)
    scaled[:padded, :] = (table * gain).astype(bf16)

    events(3)
    loads[6].wait()
    query = jnp.dot(lead, query_w[...], preferred_element_type=f32)[:1]
    head_row = lax.broadcasted_iota(jnp.int32, (TILE_ROWS, inner), 0)
    column = lax.broadcasted_iota(jnp.int32, (TILE_ROWS, inner), 1)
    own_head = (column >= head_row * head_dim) & (column < (head_row + 1) * head_dim)
    spread = jnp.where(own_head, jnp.broadcast_to(query, (TILE_ROWS, inner)), 0.0).astype(bf16)
    events(4)
    loads[7].wait()
    turned = contract_last(spread, key_w[...])[:heads] * (1.0 / math.sqrt(head_dim))
    first = jnp.sum(turned * lead_row, axis=1, keepdims=True)
    level = jnp.sum(turned * bias, axis=1, keepdims=True)
    constants[...] = jnp.broadcast_to(level, constants.shape)
    basis[:top, :] = split_in_two(turned * gain)

    features = padded + spots
    for part_of in range(GRAM_PARTS):
        events(5 + part_of)
        low = 256 * (pl.cdiv(features, 256) * part_of // GRAM_PARTS)
        high = min(features, 256 * (pl.cdiv(features, 256) * (part_of + 1) // GRAM_PARTS))
        square = contract_last(basis[: top + padded, :], basis[top + low : top + high, :])
        place = low + lax.broadcasted_iota(jnp.int32, (padded, high - low), 1)
        form[top : top + padded, low:high] = jnp.where(
            place < padded, square[top:], 2.0 * square[top:]
        ).astype(bf16)
        form[:top, low:high] = split_in_two(square[:heads] + square[heads:top])
    sizes = jnp.concatenate([jnp.zeros((1, padded), f32), weight], axis=1)
    sizes_high = sizes.astype(bf16).astype(f32)
    sizes = jnp.concatenate(
        [sizes_high, sizes - sizes_high, jnp.zeros((TILE_ROWS - 2, padded + spots), f32)], axis=0
    )
    form[top + padded :, :] = sizes.astype(bf16)

    loads[8].wait()
    first = jnp.broadcast_to(first[None], (images, heads, 1)).reshape(pairs, 1)
    peak[...] = jnp.broadcast_to(first, peak.shape)
    total[...] = jnp.ones(total.shape, f32)
    gathered[...] = jnp.zeros(gathered.shape, f32)

    cells = 2 * lanes
    lane = lax.broadcasted_iota(jnp.int32, (pairs, cells), 1)
    row_image = lax.broadcasted_iota(jnp.int32, (pairs, cells), 0) // heads
    same = (lane % lanes) // rows == row_image
    spot_row = lax.broadcasted_iota(jnp.int32, (spots, cells), 0)
    spot_lane = lax.broadcasted_iota(jnp.int32, (spots, cells), 1)
    spot_at = spot_row - (spot_lane // lanes) * rows - spot_lane % rows

    order = sum(mine * packed for mine, packed in zip(here, ORDER, strict=True))
    first_step = 5 + GRAM_PARTS
    fold_rows = scaled.shape[0] // FOLD_PARTS

    def base_of(turn):
        code = (order >> (3 * turn)) % 8
        where, own = code // 2, code % 2
        return where * PLANE + 2 * (side * own + (1 - side) * (1 - own))

    def block_of(base):
        block = jnp.concatenate([slots[base], slots[base + 1]], axis=1)
        spot = jnp.where(spot_at == base * rows, 1.0, 0.0).astype(bf16)
        return jnp.concatenate([block, spot], axis=0)

    def front(base):
        block = block_of(base)
        image = jnp.dot(form[...], block, preferred_element_type=f32)
        norm = jnp.sum(
            image[top : top + padded] * block[:padded].astype(f32), axis=0, keepdims=True
        )
        tail = top + padded
        norm = norm + image[tail : tail + 1] + image[tail + 1 : tail + 2]
        rate = lax.rsqrt(norm * (1.0 / width) + epsilon)
        scores = image[:heads] + image[heads:top]
        kept[:heads, :] = scores * rate + constants[:, :1]
        kept[heads:, :] = jnp.broadcast_to(rate, (heads, cells))

    def back(base, scores, rate):
        block = block_of(base)
        scores = jnp.broadcast_to(scores[None], (images, heads, cells)).reshape(pairs, cells)
        scores = jnp.where(same, scores, LOWEST)
        before = peak[:, :1]
        now = jnp.maximum(before, jnp.max(scores, axis=1, keepdims=True))
        shrink = jnp.exp(before - now)
        chance = jnp.where(same, jnp.exp(scores - now), 0.0)
        peak[...] = jnp.broadcast_to(now, peak.shape)
        total[...] = total[...] * shrink + jnp.sum(chance, axis=1, keepdims=True)
        gathered[...] = gathered[...] * shrink + contract_last((chance * rate).astype(bf16), block)

    def chip_step(turn, carry):
        for index in range(1, 2 * LINE):
            pl.when(turn == index)(functools.partial(events, first_step + 2 * index))
        base = base_of(turn)
        got_from_twin(base)
        scores = kept[:heads, :]
        rate = kept[heads : heads + 1, :]
        back(base_of(turn - 1), scores, rate)
        front(base)

        for index in range(1, FOLD_PARTS + 1):
            pl.when(turn == index)(functools.partial(events, first_step + 2 * index + 1))

        @pl.when(turn <= FOLD_PARTS)
        def _():
            low = pl.multiple_of((turn - 1) * fold_rows, TILE_ROWS)
            product = jnp.dot(
                scaled[pl.ds(low, fold_rows), :], value_w[...], preferred_element_type=f32
            )
            folded[pl.ds(low, fold_rows), :] = product.astype(bf16)
            ends[...] = product[fold_rows - ends.shape[0] :]

        return carry

    events(first_step)
    got_from_twin(base_of(0))
    front(base_of(0))
    events(first_step + 1)
    lax.fori_loop(1, 2 * LINE, chip_step, 0)
    back(base_of(2 * LINE - 1), kept[:heads, :], kept[heads : heads + 1, :])

    plain = ends[0:1, :] + ends[1:2, :]
    lead_value = ends[2:3, :]
    values = jnp.dot(
        split_in_two(gathered[...]), folded[: padded + spots, :], preferred_element_type=f32
    )
    share = 1.0 / total[:, :1]
    lead_chance = jnp.exp(first - peak[:, :1]) * share
    values = (values[:pairs] + values[pairs:]) * share
    values = values + plain + (lead_value - plain) * lead_chance
    pair_head = lax.broadcasted_iota(jnp.int32, (pairs, inner), 0) % heads
    pair_column = lax.broadcasted_iota(jnp.int32, (pairs, inner), 1)
    mine_only = (pair_column >= pair_head * head_dim) & (pair_column < (pair_head + 1) * head_dim)
    values = jnp.where(mine_only, values, 0.0)
    mixed = jnp.sum(values.reshape(images, heads, inner), axis=1).astype(bf16)
    loads[9].wait()
    hidden = leading + jnp.dot(mixed, out_w[...], preferred_element_type=f32)
    for index in (10, 11, 12, 13):
        loads[index].wait()
    final = layer_norm(hidden, last_gain[...], last_bias[...]).astype(bf16)
    logits = contract_last(final, class_w[...]) + class_bias[...]
    lifted = logits - jnp.max(logits, axis=-1, keepdims=True)
    logp = lifted - jnp.log(jnp.sum(jnp.exp(lifted), axis=-1, keepdims=True))

    piece_width = part.shape[2]
    classes = out.shape[1]
    part[0] = logp[:, :piece_width]
    part[1] = jnp.concatenate(
        [logp[:, piece_width:], jnp.zeros((images, 2 * piece_width - classes), f32)], axis=1
    )
    swap = pltpu.make_async_remote_copy(
        src_ref=part.at[1 - core],
        dst_ref=from_pair,
        send_sem=tail_send.at[0],
        recv_sem=tail_recv.at[0],
        device_id={"sample": twin},
        device_id_type=MESH,
    )
    swap.start()
    swap.wait_recv()
    mine = part[core]
    theirs = from_pair[...]
    high = jnp.maximum(mine, theirs)
    ring[chip] = high + jnp.log(jnp.exp(mine - high) + jnp.exp(theirs - high))

    def pass_on(ref, target):
        return passing(ref, target, tail_send.at[2], tail_recv.at[2])

    for step in range(1, chips):
        other = step - 1 + jnp.minimum(step // jnp.maximum(chip + 1, 1), 1)
        pass_on(ring.at[chip], 2 * other + core).start()
    pass_on(ring.at[pl.ds(0, chips - 1)], twin).wait_recv()
    every = ring[...]
    high = jnp.max(every, axis=0)
    result[core] = high + jnp.log(jnp.sum(jnp.exp(every - high[None]), axis=0)) - math.log(count)
    share = pltpu.make_async_remote_copy(
        src_ref=result.at[core],
        dst_ref=result.at[core],
        send_sem=tail_send.at[1],
        recv_sem=tail_recv.at[1],
        device_id={"sample": twin},
        device_id_type=MESH,
    )
    share.start()

    for place in range(LINE):

        @pl.when(plane == place)
        def _(place=place):
            all_sent(place)

    swap.wait_send()
    pass_on(ring.at[pl.ds(0, chips - 1)], twin).wait_send()
    pltpu.make_async_remote_copy(
        src_ref=result.at[core],
        dst_ref=result.at[1 - core],
        send_sem=tail_send.at[1],
        recv_sem=tail_recv.at[1],
        device_id={"sample": twin},
        device_id_type=MESH,
    ).wait_recv()
    share.wait_send()
    out[:, :piece_width] = result[0]
    out[:, piece_width:] = result[1][:, : classes - piece_width]


def kernel_shards(
    patches,
    patch_weight,
    cls_token,
    pos_embed,
    ln1_gain,
    ln1_bias,
    w_query,
    w_key,
    w_value,
    w_out,
    lnf_gain,
    lnf_bias,
    head_w,
    head_bias,
):
    count = lax.axis_size("sample")
    images, rows, depth = patches.shape
    width = patch_weight.shape[2]
    inner = w_query.shape[2]
    heads = inner // HEAD_DIM
    pairs = heads * images
    chips = count // 2
    classes = head_w.shape[2]
    piece_width = pl.cdiv(classes, 256) * 128
    padded = pl.cdiv(depth, TILE_ROWS) * TILE_ROWS
    spots = pos_embed.shape[1] - 1
    tall = FOLD_PARTS * TILE_ROWS
    fold_rows = pl.cdiv(padded + spots + TILE_ROWS, tall) * tall
    far = pl.BlockSpec(memory_space=pl.ANY)
    dma = pltpu.SemaphoreType.DMA
    f32, bf16 = jnp.float32, jnp.bfloat16
    class_rows = jnp.swapaxes(head_w, 1, 2)
    given = (
        patches,
        cls_token,
        pos_embed,
        ln1_gain,
        ln1_bias,
        patch_weight,
        w_query,
        w_key,
        w_value,
        w_out,
        class_rows,
        lnf_gain,
        lnf_bias,
        head_bias,
    )
    held = [
        pltpu.VMEM(a.shape[1:] if place and a.ndim == 3 else a.shape, a.dtype)
        for place, a in enumerate(given)
    ]
    return pl.pallas_call(
        functools.partial(whole_kernel, count, heads),
        out_shape=jax.ShapeDtypeStruct((images, classes), f32),
        in_specs=[far] * len(given),
        out_specs=pl.BlockSpec(memory_space=pltpu.VMEM),
        scratch_shapes=[
            *held,
            pltpu.VMEM((count, padded, images * rows), bf16),
            pltpu.VMEM((2 * heads + padded + spots, width), bf16),
            pltpu.VMEM((fold_rows, width), bf16),
            pltpu.VMEM((padded + 2 * heads + TILE_ROWS, padded + spots), bf16),
            pltpu.VMEM((fold_rows, inner), bf16),
            pltpu.VMEM((fold_rows - padded - spots, inner), f32),
            pltpu.VMEM((heads, 128), f32),
            pltpu.VMEM((2 * heads, 2 * images * rows), f32),
            pltpu.VMEM((pairs, padded + spots), f32),
            pltpu.VMEM((pairs, 128), f32),
            pltpu.VMEM((pairs, 128), f32),
            pltpu.VMEM((2, images, piece_width), f32),
            pltpu.VMEM((images, piece_width), f32),
            pltpu.VMEM((chips, images, piece_width), f32),
            pltpu.VMEM((2, images, piece_width), f32),
            dma((len(given),)),
            dma((chips, PIECES)),
            dma((chips,)),
            dma((2, PIECES)),
            pltpu.SemaphoreType.REGULAR((LINE,)),
            dma((3,)),
            dma((3,)),
        ],
        compiler_params=pltpu.CompilerParams(
            collective_id=0, has_side_effects=True, vmem_limit_bytes=60 << 20
        ),
    )(*given)


def takes_kernel(mesh, patches):
    count = mesh.shape["sample"]
    rows = patches.shape[1] // count
    images = patches.shape[0] // mesh.shape["group"]
    return count == PLANE * LINE and rows % TILE_ROWS == 0 and images * rows == 128


def solution(mesh):
    placed = (
        P("group", "sample", None),
        P("sample", None, None),
        P("sample", None),
        P("sample", None, None),
        P("sample", None),
        P("sample", None),
        P("sample", None, None),
        P("sample", None, None),
        P("sample", None, None),
        P("sample", None, None),
        P("sample", None),
        P("sample", None),
        P("sample", None, None),
        P("sample", None),
    )

    def run(*arrays):
        step = kernel_shards if takes_kernel(mesh, arrays[0]) else shards
        return jax.shard_map(
            step, mesh=mesh, in_specs=placed, out_specs=P("group", None), check_vma=False
        )(*arrays)

    return run
```

```python
import functools
import math

import jax
import jax.numpy as jnp
from jax import lax
from jax.experimental import pallas as pl
from jax.experimental.pallas import tpu as pltpu
from jax.sharding import PartitionSpec as P

HEAD_DIM = 80


epsilon = 1e-06


def combined_all(part, axis, combine):
    gathered = jax.tree.map(lambda a: lax.all_gather(a, axis), part)

    def take(source):
        return jax.tree.map(lambda a: lax.dynamic_index_in_dim(a, source, 0, False), gathered)

    return lax.fori_loop(
        1, lax.axis_size(axis), lambda source, state: combine(state, take(source)), take(0)
    )


def layer_norm(values, gain, shift):
    center = values - jnp.mean(values, axis=-1, keepdims=True)
    spread = jnp.mean(center * center, axis=-1, keepdims=True)
    return center * lax.rsqrt(spread + epsilon) * gain + shift


def shards(
    patches,
    patch_weight,
    cls_token,
    pos_embed,
    ln1_gain,
    ln1_bias,
    w_query,
    w_key,
    w_value,
    w_out,
    lnf_gain,
    lnf_bias,
    head_w,
    head_bias,
):
    embed_weight = patch_weight[0]
    position = pos_embed[0]
    gain_first = ln1_gain[0]
    bias_first = ln1_bias[0]
    query_weight = w_query[0]
    pair_weight = jnp.concatenate([w_key[0], w_value[0]], axis=1)
    out_weight = w_out[0]
    width = embed_weight.shape[1]
    inner = query_weight.shape[1]
    head_count = inner // HEAD_DIM
    leading = cls_token[0].astype(jnp.float32) + position[0].astype(jnp.float32)
    lead_norm = layer_norm(leading, gain_first, bias_first).astype(jnp.bfloat16)
    lead_pair = jnp.dot(lead_norm[None], pair_weight, preferred_element_type=jnp.float32).astype(
        jnp.bfloat16
    )
    query = jnp.dot(lead_norm[None], query_weight, preferred_element_type=jnp.float32).astype(
        jnp.bfloat16
    )
    query = query.reshape(head_count, HEAD_DIM)
    portion = lax.all_gather(patches, "sample", axis=1, tiled=True)
    image_count = portion.shape[0]
    row_count = portion.shape[1]
    flat = portion.reshape(-1, portion.shape[2])
    tokens = jnp.dot(flat, embed_weight, preferred_element_type=jnp.float32).reshape(
        image_count, row_count, width
    )
    placed = lax.dynamic_slice_in_dim(position, 1, row_count, 0)
    tokens = tokens + placed.astype(jnp.float32)[None]
    normed = layer_norm(tokens, gain_first, bias_first).astype(jnp.bfloat16)
    paired = jnp.dot(normed.reshape(-1, width), pair_weight, preferred_element_type=jnp.float32)
    key_values = paired.astype(jnp.bfloat16).reshape(image_count, row_count, 2 * inner)
    image_count = key_values.shape[0]
    lead_rows = jnp.broadcast_to(lead_pair[None], (image_count, 1, 2 * inner))
    full_rows = jnp.concatenate([lead_rows, key_values], axis=1)
    key_rows = full_rows[:, :, :inner].reshape(image_count, -1, head_count, HEAD_DIM)
    value_rows = full_rows[:, :, inner:].reshape(image_count, -1, head_count, HEAD_DIM)
    scores = jnp.einsum(
        "hd,ithd->iht", query, key_rows, preferred_element_type=jnp.float32
    ) / math.sqrt(HEAD_DIM)
    attention = jax.nn.softmax(scores, axis=-1).astype(jnp.bfloat16)
    mixed = jnp.einsum("iht,ithd->ihd", attention, value_rows, preferred_element_type=jnp.float32)
    mixed = mixed.astype(jnp.bfloat16).reshape(image_count, inner)
    hidden = leading[None] + jnp.dot(mixed, out_weight, preferred_element_type=jnp.float32)
    final = layer_norm(hidden, lnf_gain[0], lnf_bias[0]).astype(jnp.bfloat16)
    logits = jnp.dot(final, head_w[0], preferred_element_type=jnp.float32) + head_bias[0]
    logp = jax.nn.log_softmax(logits, axis=-1)
    count = lax.axis_size("sample")

    def combine(earlier, later):
        highest = jnp.maximum(earlier[0], later[0])
        summed = earlier[1] * jnp.exp(earlier[0] - highest) + later[1] * jnp.exp(later[0] - highest)
        return (highest, summed)

    peak, total = combined_all((logp, jnp.ones_like(logp)), "sample", combine)
    return peak + jnp.log(total) - math.log(count)


MESH = pl.DeviceIdType.MESH
PLANE = 4
LINE = 4
TILE_ROWS = 16
LOWEST = -1e30
GRAM_PARTS = 2
FOLD_PARTS = 3


def split_in_two(values):
    high = values.astype(jnp.bfloat16)
    low = (values - high.astype(jnp.float32)).astype(jnp.bfloat16)
    return jnp.concatenate([high, low], axis=0)


PIECES = 4
SENDS = (
    (
        (1,1,0,1,2), (1,1,0,1,1), (0,0,0,1,1), (0,0,0,1,3), (1,1,0,1,3), (1,1,0,1,0), (0,2,0,1,0),
        (0,2,0,1,1), (0,2,0,1,2), (0,2,0,1,3), (2,1,0,1,1), (2,1,0,1,0), (0,2,0,0,1), (0,0,1,1,1),
        (2,1,0,1,3), (0,2,1,1,1), (1,1,0,0,3), (3,1,0,0,3), (0,2,0,0,3), (0,0,0,1,0), (0,2,1,1,3),
        (0,0,1,1,2), (0,2,1,1,2), (0,0,1,1,0), (0,2,1,1,0), (0,0,0,1,2), (0,2,1,0,3), (0,2,1,0,1),
        (0,0,2,1,1), (0,2,2,1,1), (2,1,0,0,0), (3,1,0,0,0), (0,2,0,0,0), (0,0,2,1,0), (0,2,2,1,0),
        (0,2,1,0,2), (0,0,2,1,2), (0,2,2,1,2), (0,2,1,0,0), (0,0,2,1,3), (0,2,2,1,3), (3,1,0,0,2),
        (0,2,0,0,2), (0,2,2,0,1), (0,2,2,0,0), (0,2,3,1,0), (0,2,3,0,2), (0,2,2,0,2), (0,0,3,1,3),
        (0,2,3,1,3), (0,2,2,0,3), (0,2,3,1,1), (0,2,3,0,0), (0,2,3,1,2), (0,2,3,0,1), (0,2,3,0,3),
    ),
    (
        (0,1,1,1,1), (0,1,1,1,3), (1,0,1,1,3), (1,0,1,1,1), (2,1,1,1,0), (2,1,1,1,2), (2,1,1,1,1),
        (2,1,1,1,3), (0,1,1,1,2), (1,0,1,1,0), (0,1,1,1,0), (1,2,1,1,0), (1,2,1,1,1), (1,2,1,1,2),
        (1,2,1,1,3), (3,1,1,1,3), (1,0,1,1,2), (1,0,0,1,2), (2,1,0,1,2), (1,2,0,1,2), (0,1,1,0,3),
        (1,2,1,0,3), (1,0,0,1,1), (1,2,0,1,1), (1,2,1,0,1), (1,0,2,1,1), (0,1,2,1,1), (1,2,2,1,1),
        (1,2,0,1,3), (2,1,1,0,0), (1,2,1,0,0), (1,0,2,1,0), (0,1,2,1,0), (1,2,2,1,0), (1,0,0,1,0),
        (1,2,0,1,0), (1,0,2,1,2), (0,1,2,1,2), (1,2,2,1,2), (1,0,2,1,3), (0,1,2,1,3), (1,2,2,1,3),
        (1,2,1,0,2), (1,2,0,0,2), (1,2,0,0,3), (1,2,0,0,1), (0,1,3,1,0), (1,2,3,1,0), (1,2,2,0,1),
        (0,1,3,1,3), (1,0,3,1,3), (1,2,3,1,3), (1,2,2,0,0), (1,0,3,1,1), (0,1,3,1,1), (1,2,3,1,1),
        (1,2,0,0,0), (0,1,3,1,2), (1,2,3,1,2), (1,2,2,0,2), (1,2,2,0,3), (1,2,3,0,3), (1,2,3,0,2),
        (1,2,3,0,1), (1,2,3,0,0),
    ),
    (
        (1,1,2,1,1), (3,1,2,1,3), (1,1,2,1,0), (3,1,2,1,1), (1,1,2,1,2), (3,1,2,1,2), (2,0,2,1,3),
        (2,0,2,1,0), (3,1,2,1,0), (2,0,2,1,1), (1,1,2,1,3), (2,2,2,1,0), (2,2,2,1,1), (2,2,2,1,2),
        (2,2,2,1,3), (3,1,1,1,0), (2,2,1,1,0), (3,1,1,1,2), (2,0,1,1,2), (2,2,1,1,2), (2,2,2,0,3),
        (2,0,1,1,1), (3,1,1,1,1), (2,2,1,1,1), (2,0,3,1,1), (2,2,3,1,1), (2,2,2,0,0), (2,2,3,1,3),
        (2,2,2,0,1), (2,0,0,1,1), (3,1,0,1,1), (2,2,0,1,1), (2,0,3,1,0), (2,2,3,1,0), (3,1,0,1,0),
        (2,2,0,1,0), (2,0,2,1,2), (1,1,3,1,2), (2,2,3,1,2), (2,2,1,0,2), (2,0,1,1,3), (2,2,1,1,3),
        (3,1,0,1,3), (2,0,0,1,3), (2,2,0,1,3), (2,2,1,0,1), (2,2,3,0,1), (3,1,0,1,2), (2,0,0,1,2),
        (2,2,0,1,2), (2,2,3,0,3), (2,2,0,0,1), (2,2,1,0,0), (2,2,3,0,2), (2,2,3,0,0), (2,2,2,0,2),
        (2,2,0,0,0), (2,2,1,0,3), (2,2,0,0,3), (2,2,0,0,2),
    ),
    (
        (2,1,3,1,1), (3,0,3,1,3), (2,1,3,1,3), (2,1,3,1,0), (2,1,3,1,2), (3,0,3,1,2), (3,2,3,1,0),
        (3,2,3,1,1), (3,2,3,1,2), (3,2,3,1,3), (1,1,3,1,0), (1,1,3,1,3), (1,1,3,1,1), (3,0,2,1,3),
        (3,0,3,1,0), (3,2,2,1,3), (2,1,3,0,3), (3,2,3,0,3), (3,0,2,1,1), (3,2,2,1,1), (2,1,3,0,2),
        (0,1,3,0,2), (1,1,3,0,2), (3,2,3,0,2), (3,0,2,1,2), (3,2,2,1,2), (3,0,2,1,0), (3,2,2,1,0),
        (3,0,1,1,0), (3,2,1,1,0), (3,2,2,0,3), (1,1,3,0,0), (0,1,3,0,0), (3,2,3,0,0), (3,0,3,1,1),
        (3,2,2,0,1), (3,0,1,1,2), (3,2,1,1,2), (3,2,2,0,2), (3,0,1,1,3), (3,2,1,1,3), (3,2,0,0,3),
        (3,0,1,1,1), (3,2,1,1,1), (3,2,2,0,0), (3,0,0,1,1), (3,2,0,1,1), (3,2,1,0,0), (3,2,0,1,0),
        (0,1,3,0,1), (3,2,3,0,1), (3,2,1,0,2), (3,2,0,1,3), (3,2,0,0,0), (3,2,1,0,3), (3,2,0,1,2),
        (3,2,1,0,1), (3,2,0,0,1), (3,2,0,0,2),
    ),
)
EVENTS = (
    (
        ((-1,0,0,0,10),), (), (), ((-2,2,0,10,2),), (), (), ((-2,3,0,12,0),(0,0,1,12,1)),
        ((1,1,1,13,3),(0,0,3,16,3)), ((1,1,3,19,2),(1,1,2,21,2)), ((1,1,0,23,2),),
        ((1,0,3,25,2),(1,0,1,27,1)),
        ((2,1,1,28,2),(0,0,0,30,3),(2,1,0,33,2),(1,0,2,35,1),(2,1,2,36,2),(1,0,0,38,1)),
        ((2,1,3,39,2),(0,0,2,41,2)), ((2,0,1,43,1),), ((2,0,0,44,1),(3,1,0,45,1),(3,0,2,46,1),(2,0,2,47,1)),
        (), ((3,1,3,48,2),), ((2,0,3,50,1),), ((3,1,1,51,1),(3,0,0,52,1),(3,1,2,53,1)), (),
        ((3,0,1,54,1),(3,0,3,55,1)), (),
    ),
    (
        ((-1,0,0,0,15),), (), (), (), ((-2,3,0,15,1),), (), ((0,1,2,16,4),(1,0,3,20,2)),
        ((0,1,1,22,2),(1,0,1,24,1),(2,1,1,25,3),(0,1,3,28,1)), ((1,0,0,29,2),(2,1,0,31,3),(0,1,0,34,2)),
        ((2,1,2,36,3),), ((2,1,3,39,3),(1,0,2,42,1)), ((0,0,2,43,1),(0,0,3,44,1)),
        ((0,0,1,45,1),(3,1,0,46,2),(2,0,1,48,1),(3,1,3,49,3)), ((2,0,0,52,1),(3,1,1,53,3)),
        ((0,0,0,56,1),(3,1,2,57,2)), ((2,0,2,59,1),), ((2,0,3,60,1),(3,0,3,61,1),(3,0,2,62,1)), (),
        ((3,0,1,63,1),(3,0,0,64,1)), (), (), (),
    ),
    (
        ((-1,0,0,0,15),), ((-2,0,0,15,0),), (), (), (), ((1,1,0,15,2),), ((1,1,2,17,3),(2,0,3,20,1)),
        ((1,1,1,21,3),(3,1,1,24,2),(2,0,0,26,1)), ((3,1,3,27,1),(2,0,1,28,1),(0,1,1,29,3)),
        ((3,1,0,32,2),(0,1,0,34,2),(3,1,2,36,3)), ((1,0,2,39,1),(1,1,3,40,2),(0,1,3,42,3),(1,0,1,45,1)),
        ((3,0,1,46,1),(0,1,2,47,3)), ((3,0,3,50,1),(0,0,1,51,1),(1,0,0,52,1),(3,0,2,53,1),(3,0,0,54,1)),
        ((2,0,2,55,1),), ((0,0,0,56,1),(1,0,3,57,1)), (), ((0,0,3,58,1),(0,0,2,59,1)), (), (), (), (), (),
    ),
    (
        ((-1,0,0,0,10),), ((-2,1,0,10,3),(-2,0,0,13,0)), (), (), (), ((2,1,3,13,3),),
        ((3,0,3,16,2),(2,1,1,18,2)), ((3,0,2,20,4),(2,1,2,24,2)), ((2,1,0,26,2),),
        ((1,1,0,28,2),(2,0,3,30,1)), ((3,0,0,31,3),(2,0,1,34,2)),
        ((1,1,2,36,2),(2,0,2,38,1),(1,1,3,39,2),(0,0,3,41,1),(1,1,1,42,2)),
        ((2,0,0,44,1),(0,1,1,45,2),(1,0,0,47,1),(0,1,0,48,1)), ((3,0,1,49,2),),
        ((1,0,2,51,1),(0,1,3,52,1),(0,0,0,53,1),(1,0,3,54,1)), ((0,1,2,55,1),), ((1,0,1,56,1),), (),
        ((0,0,1,57,1),(0,0,2,58,1)), (), (), (),
    ),
)
ORDER = (14551705, 13862219, 680701, 583919)


def contract_last(left, right):
    return lax.dot_general(
        left, right, (((1,), (1,)), ((), ())), preferred_element_type=jnp.float32
    )


def whole_kernel(
    count,
    heads,
    patches,
    cls_token,
    pos_embed,
    ln1_gain,
    ln1_bias,
    patch_weight,
    w_query,
    w_key,
    w_value,
    w_out,
    head_w,
    lnf_gain,
    lnf_bias,
    head_bias,
    out,
    own_patches,
    cls_row,
    position,
    gain_row,
    bias_row,
    embed,
    query_w,
    key_w,
    value_w,
    out_w,
    class_w,
    last_gain,
    last_bias,
    class_bias,
    slots,
    basis,
    scaled,
    form,
    folded,
    ends,
    constants,
    kept,
    gathered,
    peak,
    total,
    part,
    from_pair,
    ring,
    result,
    load_sem,
    recv_sem,
    twin_sem,
    sent_sem,
    known_sem,
    tail_send,
    tail_recv,
):
    f32, bf16 = jnp.float32, jnp.bfloat16
    me = lax.axis_index("sample")
    core = me % 2
    side = (me // 2) % 2
    chip = me // 2
    chips = count // 2
    plane = me // PLANE
    images, rows, depth = own_patches.shape
    padded = slots.shape[1]
    lanes = slots.shape[2]
    tiles = padded // TILE_ROWS
    cuts = tuple(TILE_ROWS * (tiles * place // PIECES) for place in range(PIECES + 1))
    width = embed.shape[1]
    inner = query_w.shape[1]
    head_dim = inner // heads
    pairs = heads * images
    spots = basis.shape[0] - 2 * heads - padded
    held_rows = position.shape[0]

    loads = []
    for index, (source, target) in enumerate(
        (
            (patches, own_patches),
            (pos_embed.at[0], position),
            (cls_token, cls_row),
            (ln1_gain, gain_row),
            (ln1_bias, bias_row),
            (patch_weight.at[0], embed),
            (w_query.at[0], query_w),
            (w_key.at[0], key_w),
            (w_value.at[0], value_w),
            (w_out.at[0], out_w),
            (head_w.at[0], class_w),
            (lnf_gain, last_gain),
            (lnf_bias, last_bias),
            (head_bias, class_bias),
        )
    ):
        loads.append(pltpu.make_async_copy(source, target, load_sem.at[index]))
    for load in loads[:5]:
        load.start()

    twin = me + 1 - 2 * core
    beside = plane * PLANE + (1 - side) * 2 + core
    here = tuple(lax.convert_element_type(plane == place, jnp.int32) for place in range(LINE))
    line_of = tuple(
        (place * PLANE + (1 - side) * 2 + core, place * PLANE + side * 2 + core)
        for place in range(LINE)
    )

    barrier = pltpu.get_barrier_semaphore()

    def greet(target):
        pl.semaphore_signal(barrier, inc=1, device_id={"sample": target}, device_id_type=MESH)

    greet(twin)
    greet(beside)

    @pl.when(plane > 0)
    def _():
        greet(me - PLANE)

    @pl.when(plane < LINE - 1)
    def _():
        greet(me + PLANE)

    loads[0].wait()
    for load in loads[5:7]:
        load.start()
    eye = (
        lax.broadcasted_iota(jnp.int32, (padded, depth), 0)
        == lax.broadcasted_iota(jnp.int32, (padded, depth), 1)
    ).astype(bf16)
    flat = own_patches[...].reshape(images * rows, depth)
    slots[me] = contract_last(eye, flat).astype(bf16)
    pl.semaphore_wait(barrier, LINE - here[0] - here[LINE - 1])

    def passing(ref, target, sent_by, got_by):
        return pltpu.make_async_remote_copy(
            src_ref=ref,
            dst_ref=ref,
            send_sem=sent_by,
            recv_sem=got_by,
            device_id={"sample": target},
            device_id_type=MESH,
        )

    def rows_of(part_of):
        return pl.ds(cuts[part_of], cuts[part_of + 1] - cuts[part_of])

    def sent(place, slot):
        to, aside, origin, own, part_of = SENDS[place][slot]
        inside = aside // 2
        source = line_of[origin][own]
        got_by = twin_sem.at[source // 2] if inside else recv_sem.at[source // 2, part_of]
        target = twin if inside else line_of[to][aside]
        ref = slots.at[source, rows_of(part_of)]
        return passing(ref, target, sent_sem.at[inside, part_of], got_by)

    def got(source, part_of):
        ref = slots.at[source, rows_of(part_of)]
        passing(ref, twin, sent_sem.at[0, 0], recv_sem.at[source // 2, part_of]).wait_recv()

    def got_from_twin(base):
        ref = slots.at[base + 1 - core]
        passing(ref, twin, sent_sem.at[0, 0], twin_sem.at[base // 2]).wait_recv()

    def all_sent(place):
        for inside in range(2):
            for part_of in range(PIECES):
                number = sum(
                    1 for entry in SENDS[place] if (entry[1] // 2, entry[4]) == (inside, part_of)
                )
                ref = slots.at[pl.ds(0, number), rows_of(part_of)]
                passing(ref, twin, sent_sem.at[inside, part_of], twin_sem.at[0]).wait_send()

    def tell(target, entered):
        pl.semaphore_signal(
            known_sem.at[entered], inc=1, device_id={"sample": target}, device_id_type=MESH
        )

    def learn(place, entered):
        pl.semaphore_wait(known_sem.at[entered], 1)
        if place == 1 and entered == 3:
            tell(me - PLANE, 3)
        if place == 2 and entered == 0:
            tell(me + PLANE, 0)

    for place in (1, 2):

        @pl.when(plane == place)
        def _(place=place):
            tell(me - PLANE, place + 1)
            tell(me + PLANE, place - 1)

    def events(group):
        for place in range(LINE):
            entries = EVENTS[place][group]
            if entries:

                @pl.when(plane == place)
                def _(place=place, entries=entries):
                    for origin, own, part_of, low, number in entries:
                        if origin == -2:
                            learn(place, own)
                        if origin >= 0:
                            got(line_of[origin][own], part_of)
                        for slot in range(low, low + number):
                            sent(place, slot).start()

    events(0)
    for load in loads[7:]:
        load.start()

    for index in (1, 2, 3, 4):
        loads[index].wait()
    events(1)
    gain = gain_row[...]
    bias = bias_row[...]
    leading = cls_row[...].astype(f32) + position[0:1, :].astype(f32)
    lead = jnp.broadcast_to(layer_norm(leading, gain, bias), (TILE_ROWS, width)).astype(bf16)
    lead_row = lead[:1].astype(f32)

    events(2)
    placed = position[...].astype(f32)
    placed = placed - jnp.mean(placed, axis=1, keepdims=True)
    blank = jnp.zeros((spots - held_rows, width), f32)
    top = 2 * heads
    placed = jnp.concatenate([placed, blank], axis=0)
    basis[top + padded :, :] = placed.astype(bf16)
    bias_high = bias.astype(bf16).astype(f32)
    ending = jnp.concatenate([blank[3:], bias_high, bias - bias_high, lead_row], axis=0)
    ending = jnp.concatenate([jnp.zeros((held_rows, width), f32), ending], axis=0)
    scaled[padded:, :] = (placed * gain + ending).astype(bf16)
    weight = jnp.broadcast_to(jnp.sum(placed * placed, axis=1, keepdims=True), (spots, 128))
    weight = jnp.concatenate([weight, jnp.zeros((-spots % 128, 128), f32)], axis=0)
    weight = jnp.transpose(weight)[:1, :spots]

    loads[5].wait()
    table = embed[...].astype(f32)
    table = table - jnp.mean(table, axis=1, keepdims=True)
    table = jnp.concatenate([table, jnp.zeros((padded - depth, width), f32)], axis=0)
    basis[top : top + padded, :] = table.astype(bf16)
    scaled[:padded, :] = (table * gain).astype(bf16)

    events(3)
    loads[6].wait()
    query = jnp.dot(lead, query_w[...], preferred_element_type=f32)[:1]
    head_row = lax.broadcasted_iota(jnp.int32, (TILE_ROWS, inner), 0)
    column = lax.broadcasted_iota(jnp.int32, (TILE_ROWS, inner), 1)
    own_head = (column >= head_row * head_dim) & (column < (head_row + 1) * head_dim)
    spread = jnp.where(own_head, jnp.broadcast_to(query, (TILE_ROWS, inner)), 0.0).astype(bf16)
    events(4)
    loads[7].wait()
    turned = contract_last(spread, key_w[...])[:heads] * (1.0 / math.sqrt(head_dim))
    first = jnp.sum(turned * lead_row, axis=1, keepdims=True)
    level = jnp.sum(turned * bias, axis=1, keepdims=True)
    constants[...] = jnp.broadcast_to(level, constants.shape)
    basis[:top, :] = split_in_two(turned * gain)

    features = padded + spots
    for part_of in range(GRAM_PARTS):
        events(5 + part_of)
        low = 256 * (pl.cdiv(features, 256) * part_of // GRAM_PARTS)
        high = min(features, 256 * (pl.cdiv(features, 256) * (part_of + 1) // GRAM_PARTS))
        square = contract_last(basis[: top + padded, :], basis[top + low : top + high, :])
        place = low + lax.broadcasted_iota(jnp.int32, (padded, high - low), 1)
        form[top : top + padded, low:high] = jnp.where(
            place < padded, square[top:], 2.0 * square[top:]
        ).astype(bf16)
        form[:top, low:high] = split_in_two(square[:heads] + square[heads:top])
    sizes = jnp.concatenate([jnp.zeros((1, padded), f32), weight], axis=1)
    sizes_high = sizes.astype(bf16).astype(f32)
    sizes = jnp.concatenate(
        [sizes_high, sizes - sizes_high, jnp.zeros((TILE_ROWS - 2, padded + spots), f32)], axis=0
    )
    form[top + padded :, :] = sizes.astype(bf16)

    loads[8].wait()
    first = jnp.broadcast_to(first[None], (images, heads, 1)).reshape(pairs, 1)
    peak[...] = jnp.broadcast_to(first, peak.shape)
    total[...] = jnp.ones(total.shape, f32)
    gathered[...] = jnp.zeros(gathered.shape, f32)

    cells = 2 * lanes
    lane = lax.broadcasted_iota(jnp.int32, (pairs, cells), 1)
    row_image = lax.broadcasted_iota(jnp.int32, (pairs, cells), 0) // heads
    same = (lane % lanes) // rows == row_image
    spot_row = lax.broadcasted_iota(jnp.int32, (spots, cells), 0)
    spot_lane = lax.broadcasted_iota(jnp.int32, (spots, cells), 1)
    spot_at = spot_row - 1 - (spot_lane // lanes) * rows - spot_lane % rows

    order = sum(mine * packed for mine, packed in zip(here, ORDER, strict=True))
    first_step = 5 + GRAM_PARTS
    fold_rows = scaled.shape[0] // FOLD_PARTS

    def base_of(turn):
        code = (order >> (3 * turn)) % 8
        where, own = code // 2, code % 2
        return where * PLANE + 2 * (side * own + (1 - side) * (1 - own))

    def block_of(base):
        block = jnp.concatenate([slots[base], slots[base + 1]], axis=1)
        spot = jnp.where(spot_at == base * rows, 1.0, 0.0).astype(bf16)
        return jnp.concatenate([block, spot], axis=0)

    def front(base):
        block = block_of(base)
        image = jnp.dot(form[...], block, preferred_element_type=f32)
        norm = jnp.sum(
            image[top : top + padded] * block[:padded].astype(f32), axis=0, keepdims=True
        )
        tail = top + padded
        norm = norm + image[tail : tail + 1] + image[tail + 1 : tail + 2]
        rate = lax.rsqrt(norm * (1.0 / width) + epsilon)
        scores = image[:heads] + image[heads:top]
        kept[:heads, :] = scores * rate + constants[:, :1]
        kept[heads:, :] = jnp.broadcast_to(rate, (heads, cells))

    def back(base, scores, rate):
        block = block_of(base)
        scores = jnp.broadcast_to(scores[None], (images, heads, cells)).reshape(pairs, cells)
        scores = jnp.where(same, scores, LOWEST)
        before = peak[:, :1]
        now = jnp.maximum(before, jnp.max(scores, axis=1, keepdims=True))
        shrink = jnp.exp(before - now)
        chance = jnp.where(same, jnp.exp(scores - now), 0.0)
        peak[...] = jnp.broadcast_to(now, peak.shape)
        total[...] = total[...] * shrink + jnp.sum(chance, axis=1, keepdims=True)
        gathered[...] = gathered[...] * shrink + contract_last((chance * rate).astype(bf16), block)

    def fold(part_of):
        low = pl.multiple_of(part_of * fold_rows, TILE_ROWS)
        product = jnp.dot(
            scaled[pl.ds(low, fold_rows), :], value_w[...], preferred_element_type=f32
        )
        folded[pl.ds(low, fold_rows), :] = product.astype(bf16)
        ends[...] = product[fold_rows - ends.shape[0] :]

    def chip_step(turn, carry):
        for index in range(1, 2 * LINE):
            pl.when(turn == index)(functools.partial(events, first_step + 2 * index))
        base = base_of(turn)
        got_from_twin(base)
        scores = kept[:heads, :]
        rate = kept[heads : heads + 1, :]
        back(base_of(turn - 1), scores, rate)
        front(base)

        for index in range(1, 2 * LINE - 1):
            pl.when(turn == index)(functools.partial(events, first_step + 2 * index + 1))

        @pl.when(turn < FOLD_PARTS)
        def _():
            fold(turn)

        return carry

    events(first_step)
    got_from_twin(base_of(0))
    front(base_of(0))
    events(first_step + 1)
    fold(0)
    lax.fori_loop(1, 2 * LINE, chip_step, 0)
    back(base_of(2 * LINE - 1), kept[:heads, :], kept[heads : heads + 1, :])

    last = ends.shape[0]
    plain = ends[last - 3 : last - 2, :] + ends[last - 2 : last - 1, :]
    lead_value = ends[last - 1 :, :]
    values = jnp.dot(
        split_in_two(gathered[...]), folded[...], preferred_element_type=f32
    )
    share = 1.0 / total[:, :1]
    lead_chance = jnp.exp(first - peak[:, :1]) * share
    values = (values[:pairs] + values[pairs:]) * share
    values = values + plain + (lead_value - plain) * lead_chance
    pair_head = lax.broadcasted_iota(jnp.int32, (pairs, inner), 0) % heads
    pair_column = lax.broadcasted_iota(jnp.int32, (pairs, inner), 1)
    mine_only = (pair_column >= pair_head * head_dim) & (pair_column < (pair_head + 1) * head_dim)
    values = jnp.where(mine_only, values, 0.0)
    mixed = jnp.sum(values.reshape(images, heads, inner), axis=1).astype(bf16)
    loads[9].wait()
    hidden = leading + jnp.dot(mixed, out_w[...], preferred_element_type=f32)
    for index in (10, 11, 12, 13):
        loads[index].wait()
    center = hidden - jnp.mean(hidden, axis=-1, keepdims=True)
    shift = last_bias[...]
    shift_high = shift.astype(bf16)
    shift_low = (shift - shift_high.astype(f32)).astype(bf16)
    rows_in = jnp.concatenate(
        [
            center * last_gain[...],
            shift_high.astype(f32),
            shift_low.astype(f32),
            jnp.zeros((TILE_ROWS - images - 2, width), f32),
        ],
        axis=0,
    ).astype(bf16)
    spread_out = jnp.mean(center * center, axis=-1, keepdims=True)
    products = contract_last(rows_in, class_w[...])
    moved = products[images : images + 1] + products[images + 1 : images + 2] + class_bias[...]
    logits = products[:images] * lax.rsqrt(spread_out + epsilon) + moved
    lifted = logits - jnp.max(logits, axis=-1, keepdims=True)
    logp = lifted - jnp.log(jnp.sum(jnp.exp(lifted), axis=-1, keepdims=True))

    piece_width = part.shape[2]
    classes = out.shape[1]
    part[0] = logp[:, :piece_width]
    part[1] = jnp.concatenate(
        [logp[:, piece_width:], jnp.zeros((images, 2 * piece_width - classes), f32)], axis=1
    )
    swap = pltpu.make_async_remote_copy(
        src_ref=part.at[1 - core],
        dst_ref=from_pair,
        send_sem=tail_send.at[0],
        recv_sem=tail_recv.at[0],
        device_id={"sample": twin},
        device_id_type=MESH,
    )
    swap.start()
    swap.wait_recv()
    mine = part[core]
    theirs = from_pair[...]
    high = jnp.maximum(mine, theirs)
    ring[chip] = high + jnp.log(jnp.exp(mine - high) + jnp.exp(theirs - high))

    def pass_on(ref, target):
        return passing(ref, target, tail_send.at[2], tail_recv.at[2])

    for step in range(1, chips):
        other = step - 1 + jnp.minimum(step // jnp.maximum(chip + 1, 1), 1)
        pass_on(ring.at[chip], 2 * other + core).start()
    pass_on(ring.at[pl.ds(0, chips - 1)], twin).wait_recv()
    every = ring[...]
    high = jnp.max(every, axis=0)
    result[core] = high + jnp.log(jnp.sum(jnp.exp(every - high[None]), axis=0)) - math.log(count)
    share = pltpu.make_async_remote_copy(
        src_ref=result.at[core],
        dst_ref=result.at[core],
        send_sem=tail_send.at[1],
        recv_sem=tail_recv.at[1],
        device_id={"sample": twin},
        device_id_type=MESH,
    )
    share.start()

    for place in range(LINE):

        @pl.when(plane == place)
        def _(place=place):
            all_sent(place)

    swap.wait_send()
    pass_on(ring.at[pl.ds(0, chips - 1)], twin).wait_send()
    pltpu.make_async_remote_copy(
        src_ref=result.at[core],
        dst_ref=result.at[1 - core],
        send_sem=tail_send.at[1],
        recv_sem=tail_recv.at[1],
        device_id={"sample": twin},
        device_id_type=MESH,
    ).wait_recv()
    share.wait_send()
    out[:, :piece_width] = result[0]
    out[:, piece_width:] = result[1][:, : classes - piece_width]


def kernel_shards(
    patches,
    patch_weight,
    cls_token,
    pos_embed,
    ln1_gain,
    ln1_bias,
    w_query,
    w_key,
    w_value,
    w_out,
    lnf_gain,
    lnf_bias,
    head_w,
    head_bias,
):
    count = lax.axis_size("sample")
    images, rows, depth = patches.shape
    width = patch_weight.shape[2]
    inner = w_query.shape[2]
    heads = inner // HEAD_DIM
    pairs = heads * images
    chips = count // 2
    classes = head_w.shape[2]
    piece_width = pl.cdiv(classes, 256) * 128
    padded = pl.cdiv(depth, TILE_ROWS) * TILE_ROWS
    tall = FOLD_PARTS * TILE_ROWS
    features = pl.cdiv(padded + pos_embed.shape[1] + 3, tall) * tall
    far = pl.BlockSpec(memory_space=pl.ANY)
    dma = pltpu.SemaphoreType.DMA
    f32, bf16 = jnp.float32, jnp.bfloat16
    class_rows = jnp.swapaxes(head_w, 1, 2)
    given = (
        patches,
        cls_token,
        pos_embed,
        ln1_gain,
        ln1_bias,
        patch_weight,
        w_query,
        w_key,
        w_value,
        w_out,
        class_rows,
        lnf_gain,
        lnf_bias,
        head_bias,
    )
    held = [
        pltpu.VMEM(a.shape[1:] if place and a.ndim == 3 else a.shape, a.dtype)
        for place, a in enumerate(given)
    ]
    return pl.pallas_call(
        functools.partial(whole_kernel, count, heads),
        out_shape=jax.ShapeDtypeStruct((images, classes), f32),
        in_specs=[far] * len(given),
        out_specs=pl.BlockSpec(memory_space=pltpu.VMEM),
        scratch_shapes=[
            *held,
            pltpu.VMEM((count, padded, images * rows), bf16),
            pltpu.VMEM((2 * heads + features, width), bf16),
            pltpu.VMEM((features, width), bf16),
            pltpu.VMEM((padded + 2 * heads + TILE_ROWS, features), bf16),
            pltpu.VMEM((features, inner), bf16),
            pltpu.VMEM((TILE_ROWS, inner), f32),
            pltpu.VMEM((heads, 128), f32),
            pltpu.VMEM((2 * heads, 2 * images * rows), f32),
            pltpu.VMEM((pairs, features), f32),
            pltpu.VMEM((pairs, 128), f32),
            pltpu.VMEM((pairs, 128), f32),
            pltpu.VMEM((2, images, piece_width), f32),
            pltpu.VMEM((images, piece_width), f32),
            pltpu.VMEM((chips, images, piece_width), f32),
            pltpu.VMEM((2, images, piece_width), f32),
            dma((len(given),)),
            dma((chips, PIECES)),
            dma((chips,)),
            dma((2, PIECES)),
            pltpu.SemaphoreType.REGULAR((LINE,)),
            dma((3,)),
            dma((3,)),
        ],
        compiler_params=pltpu.CompilerParams(
            collective_id=0, has_side_effects=True, vmem_limit_bytes=60 << 20
        ),
    )(*given)


def takes_kernel(mesh, patches):
    count = mesh.shape["sample"]
    rows = patches.shape[1] // count
    images = patches.shape[0] // mesh.shape["group"]
    return count == PLANE * LINE and rows % TILE_ROWS == 0 and images * rows == 128


def solution(mesh):
    placed = (
        P("group", "sample", None),
        P("sample", None, None),
        P("sample", None),
        P("sample", None, None),
        P("sample", None),
        P("sample", None),
        P("sample", None, None),
        P("sample", None, None),
        P("sample", None, None),
        P("sample", None, None),
        P("sample", None),
        P("sample", None),
        P("sample", None, None),
        P("sample", None),
    )

    def run(*arrays):
        step = kernel_shards if takes_kernel(mesh, arrays[0]) else shards
        return jax.shard_map(
            step, mesh=mesh, in_specs=placed, out_specs=P("group", None), check_vma=False
        )(*arrays)

    return run
```

```python
import functools
import math

import jax
import jax.numpy as jnp
from jax import lax
from jax.experimental import pallas as pl
from jax.experimental.pallas import tpu as pltpu
from jax.sharding import PartitionSpec as P

HEAD_DIM = 80


epsilon = 1e-06


def combined_all(part, axis, combine):
    gathered = jax.tree.map(lambda a: lax.all_gather(a, axis), part)

    def take(source):
        return jax.tree.map(lambda a: lax.dynamic_index_in_dim(a, source, 0, False), gathered)

    return lax.fori_loop(
        1, lax.axis_size(axis), lambda source, state: combine(state, take(source)), take(0)
    )


def layer_norm(values, gain, shift):
    center = values - jnp.mean(values, axis=-1, keepdims=True)
    spread = jnp.mean(center * center, axis=-1, keepdims=True)
    return center * lax.rsqrt(spread + epsilon) * gain + shift


def shards(
    patches,
    patch_weight,
    cls_token,
    pos_embed,
    ln1_gain,
    ln1_bias,
    w_query,
    w_key,
    w_value,
    w_out,
    lnf_gain,
    lnf_bias,
    head_w,
    head_bias,
):
    embed_weight = patch_weight[0]
    position = pos_embed[0]
    gain_first = ln1_gain[0]
    bias_first = ln1_bias[0]
    query_weight = w_query[0]
    pair_weight = jnp.concatenate([w_key[0], w_value[0]], axis=1)
    out_weight = w_out[0]
    width = embed_weight.shape[1]
    inner = query_weight.shape[1]
    head_count = inner // HEAD_DIM
    leading = cls_token[0].astype(jnp.float32) + position[0].astype(jnp.float32)
    lead_norm = layer_norm(leading, gain_first, bias_first).astype(jnp.bfloat16)
    lead_pair = jnp.dot(lead_norm[None], pair_weight, preferred_element_type=jnp.float32).astype(
        jnp.bfloat16
    )
    query = jnp.dot(lead_norm[None], query_weight, preferred_element_type=jnp.float32).astype(
        jnp.bfloat16
    )
    query = query.reshape(head_count, HEAD_DIM)
    portion = lax.all_gather(patches, "sample", axis=1, tiled=True)
    image_count = portion.shape[0]
    row_count = portion.shape[1]
    flat = portion.reshape(-1, portion.shape[2])
    tokens = jnp.dot(flat, embed_weight, preferred_element_type=jnp.float32).reshape(
        image_count, row_count, width
    )
    placed = lax.dynamic_slice_in_dim(position, 1, row_count, 0)
    tokens = tokens + placed.astype(jnp.float32)[None]
    normed = layer_norm(tokens, gain_first, bias_first).astype(jnp.bfloat16)
    paired = jnp.dot(normed.reshape(-1, width), pair_weight, preferred_element_type=jnp.float32)
    key_values = paired.astype(jnp.bfloat16).reshape(image_count, row_count, 2 * inner)
    image_count = key_values.shape[0]
    lead_rows = jnp.broadcast_to(lead_pair[None], (image_count, 1, 2 * inner))
    full_rows = jnp.concatenate([lead_rows, key_values], axis=1)
    key_rows = full_rows[:, :, :inner].reshape(image_count, -1, head_count, HEAD_DIM)
    value_rows = full_rows[:, :, inner:].reshape(image_count, -1, head_count, HEAD_DIM)
    scores = jnp.einsum(
        "hd,ithd->iht", query, key_rows, preferred_element_type=jnp.float32
    ) / math.sqrt(HEAD_DIM)
    attention = jax.nn.softmax(scores, axis=-1).astype(jnp.bfloat16)
    mixed = jnp.einsum("iht,ithd->ihd", attention, value_rows, preferred_element_type=jnp.float32)
    mixed = mixed.astype(jnp.bfloat16).reshape(image_count, inner)
    hidden = leading[None] + jnp.dot(mixed, out_weight, preferred_element_type=jnp.float32)
    final = layer_norm(hidden, lnf_gain[0], lnf_bias[0]).astype(jnp.bfloat16)
    logits = jnp.dot(final, head_w[0], preferred_element_type=jnp.float32) + head_bias[0]
    logp = jax.nn.log_softmax(logits, axis=-1)
    count = lax.axis_size("sample")

    def combine(earlier, later):
        highest = jnp.maximum(earlier[0], later[0])
        summed = earlier[1] * jnp.exp(earlier[0] - highest) + later[1] * jnp.exp(later[0] - highest)
        return (highest, summed)

    peak, total = combined_all((logp, jnp.ones_like(logp)), "sample", combine)
    return peak + jnp.log(total) - math.log(count)


MESH = pl.DeviceIdType.MESH
PLANE = 4
LINE = 4
TILE_ROWS = 16
LOWEST = -1e30
GRAM_PARTS = 2
FOLD_PARTS = 3


def split_in_two(values):
    high = values.astype(jnp.bfloat16)
    low = (values - high.astype(jnp.float32)).astype(jnp.bfloat16)
    return jnp.concatenate([high, low], axis=0)


PIECES = 4
SENDS = (
    (
        (1,1,0,1,2), (1,1,0,1,1), (0,0,0,1,1), (0,0,0,1,3), (1,1,0,1,3), (1,1,0,1,0), (0,2,0,1,0),
        (0,2,0,1,1), (0,2,0,1,2), (0,2,0,1,3), (2,1,0,1,1), (2,1,0,1,0), (0,2,0,0,1), (0,0,1,1,1),
        (2,1,0,1,3), (0,2,1,1,1), (1,1,0,0,3), (3,1,0,0,3), (0,2,0,0,3), (0,0,0,1,0), (0,2,1,1,3),
        (0,0,1,1,2), (0,2,1,1,2), (0,0,1,1,0), (0,2,1,1,0), (0,0,0,1,2), (0,2,1,0,3), (0,2,1,0,1),
        (0,0,2,1,1), (0,2,2,1,1), (2,1,0,0,0), (3,1,0,0,0), (0,2,0,0,0), (0,0,2,1,0), (0,2,2,1,0),
        (0,2,1,0,2), (0,0,2,1,2), (0,2,2,1,2), (0,2,1,0,0), (0,0,2,1,3), (0,2,2,1,3), (3,1,0,0,2),
        (0,2,0,0,2), (0,2,2,0,1), (0,2,2,0,0), (0,2,3,1,0), (0,2,3,0,2), (0,2,2,0,2), (0,0,3,1,3),
        (0,2,3,1,3), (0,2,2,0,3), (0,2,3,1,1), (0,2,3,0,0), (0,2,3,1,2), (0,2,3,0,1), (0,2,3,0,3),
    ),
    (
        (0,1,1,1,1), (0,1,1,1,3), (1,0,1,1,3), (1,0,1,1,1), (2,1,1,1,0), (2,1,1,1,2), (2,1,1,1,1),
        (2,1,1,1,3), (0,1,1,1,2), (1,0,1,1,0), (0,1,1,1,0), (1,2,1,1,0), (1,2,1,1,1), (1,2,1,1,2),
        (1,2,1,1,3), (3,1,1,1,3), (1,0,1,1,2), (1,0,0,1,2), (2,1,0,1,2), (1,2,0,1,2), (0,1,1,0,3),
        (1,2,1,0,3), (1,0,0,1,1), (1,2,0,1,1), (1,2,1,0,1), (1,0,2,1,1), (0,1,2,1,1), (1,2,2,1,1),
        (1,2,0,1,3), (2,1,1,0,0), (1,2,1,0,0), (1,0,2,1,0), (0,1,2,1,0), (1,2,2,1,0), (1,0,0,1,0),
        (1,2,0,1,0), (1,0,2,1,2), (0,1,2,1,2), (1,2,2,1,2), (1,0,2,1,3), (0,1,2,1,3), (1,2,2,1,3),
        (1,2,1,0,2), (1,2,0,0,2), (1,2,0,0,3), (1,2,0,0,1), (0,1,3,1,0), (1,2,3,1,0), (1,2,2,0,1),
        (0,1,3,1,3), (1,0,3,1,3), (1,2,3,1,3), (1,2,2,0,0), (1,0,3,1,1), (0,1,3,1,1), (1,2,3,1,1),
        (1,2,0,0,0), (0,1,3,1,2), (1,2,3,1,2), (1,2,2,0,2), (1,2,2,0,3), (1,2,3,0,3), (1,2,3,0,2),
        (1,2,3,0,1), (1,2,3,0,0),
    ),
    (
        (1,1,2,1,1), (3,1,2,1,3), (1,1,2,1,0), (3,1,2,1,1), (1,1,2,1,2), (3,1,2,1,2), (2,0,2,1,3),
        (2,0,2,1,0), (3,1,2,1,0), (2,0,2,1,1), (1,1,2,1,3), (2,2,2,1,0), (2,2,2,1,1), (2,2,2,1,2),
        (2,2,2,1,3), (3,1,1,1,0), (2,2,1,1,0), (3,1,1,1,2), (2,0,1,1,2), (2,2,1,1,2), (2,2,2,0,3),
        (2,0,1,1,1), (3,1,1,1,1), (2,2,1,1,1), (2,0,3,1,1), (2,2,3,1,1), (2,2,2,0,0), (2,2,3,1,3),
        (2,2,2,0,1), (2,0,0,1,1), (3,1,0,1,1), (2,2,0,1,1), (2,0,3,1,0), (2,2,3,1,0), (3,1,0,1,0),
        (2,2,0,1,0), (2,0,2,1,2), (1,1,3,1,2), (2,2,3,1,2), (2,2,1,0,2), (2,0,1,1,3), (2,2,1,1,3),
        (3,1,0,1,3), (2,0,0,1,3), (2,2,0,1,3), (2,2,1,0,1), (2,2,3,0,1), (3,1,0,1,2), (2,0,0,1,2),
        (2,2,0,1,2), (2,2,3,0,3), (2,2,0,0,1), (2,2,1,0,0), (2,2,3,0,2), (2,2,3,0,0), (2,2,2,0,2),
        (2,2,0,0,0), (2,2,1,0,3), (2,2,0,0,3), (2,2,0,0,2),
    ),
    (
        (2,1,3,1,1), (3,0,3,1,3), (2,1,3,1,3), (2,1,3,1,0), (2,1,3,1,2), (3,0,3,1,2), (3,2,3,1,0),
        (3,2,3,1,1), (3,2,3,1,2), (3,2,3,1,3), (1,1,3,1,0), (1,1,3,1,3), (1,1,3,1,1), (3,0,2,1,3),
        (3,0,3,1,0), (3,2,2,1,3), (2,1,3,0,3), (3,2,3,0,3), (3,0,2,1,1), (3,2,2,1,1), (2,1,3,0,2),
        (0,1,3,0,2), (1,1,3,0,2), (3,2,3,0,2), (3,0,2,1,2), (3,2,2,1,2), (3,0,2,1,0), (3,2,2,1,0),
        (3,0,1,1,0), (3,2,1,1,0), (3,2,2,0,3), (1,1,3,0,0), (0,1,3,0,0), (3,2,3,0,0), (3,0,3,1,1),
        (3,2,2,0,1), (3,0,1,1,2), (3,2,1,1,2), (3,2,2,0,2), (3,0,1,1,3), (3,2,1,1,3), (3,2,0,0,3),
        (3,0,1,1,1), (3,2,1,1,1), (3,2,2,0,0), (3,0,0,1,1), (3,2,0,1,1), (3,2,1,0,0), (3,2,0,1,0),
        (0,1,3,0,1), (3,2,3,0,1), (3,2,1,0,2), (3,2,0,1,3), (3,2,0,0,0), (3,2,1,0,3), (3,2,0,1,2),
        (3,2,1,0,1), (3,2,0,0,1), (3,2,0,0,2),
    ),
)
EVENTS = (
    (
        ((-1,0,0,0,10),), (), (), ((-2,2,0,10,2),), (), (), ((-2,3,0,12,0),(0,0,1,12,1)),
        ((1,1,1,13,3),(0,0,3,16,3)), ((1,1,3,19,2),(1,1,2,21,2)), ((1,1,0,23,2),),
        ((1,0,3,25,2),(1,0,1,27,1)),
        ((2,1,1,28,2),(0,0,0,30,3),(2,1,0,33,2),(1,0,2,35,1),(2,1,2,36,2),(1,0,0,38,1)),
        ((2,1,3,39,2),(0,0,2,41,2)), ((2,0,1,43,1),), ((2,0,0,44,1),(3,1,0,45,1),(3,0,2,46,1),(2,0,2,47,1)),
        (), ((3,1,3,48,2),), ((2,0,3,50,1),), ((3,1,1,51,1),(3,0,0,52,1),(3,1,2,53,1)), (),
        ((3,0,1,54,1),(3,0,3,55,1)), (),
    ),
    (
        ((-1,0,0,0,15),), (), (), (), ((-2,3,0,15,1),), (), ((0,1,2,16,4),(1,0,3,20,2)),
        ((0,1,1,22,2),(1,0,1,24,1),(2,1,1,25,3),(0,1,3,28,1)), ((1,0,0,29,2),(2,1,0,31,3),(0,1,0,34,2)),
        ((2,1,2,36,3),), ((2,1,3,39,3),(1,0,2,42,1)), ((0,0,2,43,1),(0,0,3,44,1)),
        ((0,0,1,45,1),(3,1,0,46,2),(2,0,1,48,1),(3,1,3,49,3)), ((2,0,0,52,1),(3,1,1,53,3)),
        ((0,0,0,56,1),(3,1,2,57,2)), ((2,0,2,59,1),), ((2,0,3,60,1),(3,0,3,61,1),(3,0,2,62,1)), (),
        ((3,0,1,63,1),(3,0,0,64,1)), (), (), (),
    ),
    (
        ((-1,0,0,0,15),), ((-2,0,0,15,0),), (), (), (), ((1,1,0,15,2),), ((1,1,2,17,3),(2,0,3,20,1)),
        ((1,1,1,21,3),(3,1,1,24,2),(2,0,0,26,1)), ((3,1,3,27,1),(2,0,1,28,1),(0,1,1,29,3)),
        ((3,1,0,32,2),(0,1,0,34,2),(3,1,2,36,3)), ((1,0,2,39,1),(1,1,3,40,2),(0,1,3,42,3),(1,0,1,45,1)),
        ((3,0,1,46,1),(0,1,2,47,3)), ((3,0,3,50,1),(0,0,1,51,1),(1,0,0,52,1),(3,0,2,53,1),(3,0,0,54,1)),
        ((2,0,2,55,1),), ((0,0,0,56,1),(1,0,3,57,1)), (), ((0,0,3,58,1),(0,0,2,59,1)), (), (), (), (), (),
    ),
    (
        ((-1,0,0,0,10),), ((-2,1,0,10,3),(-2,0,0,13,0)), (), (), (), ((2,1,3,13,3),),
        ((3,0,3,16,2),(2,1,1,18,2)), ((3,0,2,20,4),(2,1,2,24,2)), ((2,1,0,26,2),),
        ((1,1,0,28,2),(2,0,3,30,1)), ((3,0,0,31,3),(2,0,1,34,2)),
        ((1,1,2,36,2),(2,0,2,38,1),(1,1,3,39,2),(0,0,3,41,1),(1,1,1,42,2)),
        ((2,0,0,44,1),(0,1,1,45,2),(1,0,0,47,1),(0,1,0,48,1)), ((3,0,1,49,2),),
        ((1,0,2,51,1),(0,1,3,52,1),(0,0,0,53,1),(1,0,3,54,1)), ((0,1,2,55,1),), ((1,0,1,56,1),), (),
        ((0,0,1,57,1),(0,0,2,58,1)), (), (), (),
    ),
)
ORDER = (14551705, 13862219, 680701, 583919)


def contract_last(left, right):
    return lax.dot_general(
        left, right, (((1,), (1,)), ((), ())), preferred_element_type=jnp.float32
    )


def whole_kernel(
    count,
    heads,
    patches,
    cls_token,
    pos_embed,
    ln1_gain,
    ln1_bias,
    patch_weight,
    w_query,
    w_key,
    w_value,
    w_out,
    head_w,
    lnf_gain,
    lnf_bias,
    head_bias,
    out,
    own_patches,
    cls_row,
    position,
    gain_row,
    bias_row,
    embed,
    query_w,
    key_w,
    value_w,
    out_w,
    class_w,
    last_gain,
    last_bias,
    class_bias,
    slots,
    basis,
    scaled,
    form,
    folded,
    ends,
    constants,
    kept,
    gathered,
    peak,
    total,
    part,
    from_pair,
    ring,
    result,
    load_sem,
    recv_sem,
    twin_sem,
    sent_sem,
    known_sem,
    tail_send,
    tail_recv,
):
    f32, bf16 = jnp.float32, jnp.bfloat16
    me = lax.axis_index("sample")
    core = me % 2
    side = (me // 2) % 2
    chip = me // 2
    chips = count // 2
    plane = me // PLANE
    images, rows, depth = own_patches.shape
    padded = slots.shape[1]
    lanes = slots.shape[2]
    tiles = padded // TILE_ROWS
    cuts = tuple(TILE_ROWS * (tiles * place // PIECES) for place in range(PIECES + 1))
    width = embed.shape[1]
    inner = query_w.shape[1]
    head_dim = inner // heads
    pairs = heads * images
    spots = basis.shape[0] - 2 * heads - padded
    held_rows = position.shape[0]

    loads = []
    for index, (source, target) in enumerate(
        (
            (patches, own_patches),
            (pos_embed.at[0], position),
            (cls_token, cls_row),
            (ln1_gain, gain_row),
            (ln1_bias, bias_row),
            (patch_weight.at[0], embed),
            (w_query.at[0], query_w),
            (w_key.at[0], key_w),
            (w_value.at[0], value_w),
            (w_out.at[0], out_w),
            (head_w.at[0], class_w),
            (lnf_gain, last_gain),
            (lnf_bias, last_bias),
            (head_bias, class_bias),
        )
    ):
        loads.append(pltpu.make_async_copy(source, target, load_sem.at[index]))
    for load in loads[:5]:
        load.start()

    twin = me + 1 - 2 * core
    beside = plane * PLANE + (1 - side) * 2 + core
    here = tuple(lax.convert_element_type(plane == place, jnp.int32) for place in range(LINE))
    line_of = tuple(
        (place * PLANE + (1 - side) * 2 + core, place * PLANE + side * 2 + core)
        for place in range(LINE)
    )

    barrier = pltpu.get_barrier_semaphore()

    def greet(target):
        pl.semaphore_signal(barrier, inc=1, device_id={"sample": target}, device_id_type=MESH)

    greet(twin)
    greet(beside)

    @pl.when(plane > 0)
    def _():
        greet(me - PLANE)

    @pl.when(plane < LINE - 1)
    def _():
        greet(me + PLANE)

    loads[0].wait()
    for load in loads[5:7]:
        load.start()
    eye = (
        lax.broadcasted_iota(jnp.int32, (padded, depth), 0)
        == lax.broadcasted_iota(jnp.int32, (padded, depth), 1)
    ).astype(bf16)
    flat = own_patches[...].reshape(images * rows, depth)
    slots[me] = contract_last(eye, flat).astype(bf16)
    pl.semaphore_wait(barrier, LINE - here[0] - here[LINE - 1])

    def passing(ref, target, sent_by, got_by):
        return pltpu.make_async_remote_copy(
            src_ref=ref,
            dst_ref=ref,
            send_sem=sent_by,
            recv_sem=got_by,
            device_id={"sample": target},
            device_id_type=MESH,
        )

    def rows_of(part_of):
        return pl.ds(cuts[part_of], cuts[part_of + 1] - cuts[part_of])

    def sent(place, slot):
        to, aside, origin, own, part_of = SENDS[place][slot]
        inside = aside // 2
        source = line_of[origin][own]
        got_by = twin_sem.at[source // 2] if inside else recv_sem.at[source // 2, part_of]
        target = twin if inside else line_of[to][aside]
        ref = slots.at[source, rows_of(part_of)]
        return passing(ref, target, sent_sem.at[inside, part_of], got_by)

    def got(source, part_of):
        ref = slots.at[source, rows_of(part_of)]
        passing(ref, twin, sent_sem.at[0, 0], recv_sem.at[source // 2, part_of]).wait_recv()

    def got_from_twin(base):
        ref = slots.at[base + 1 - core]
        passing(ref, twin, sent_sem.at[0, 0], twin_sem.at[base // 2]).wait_recv()

    def all_sent(place):
        for inside in range(2):
            for part_of in range(PIECES):
                number = sum(
                    1 for entry in SENDS[place] if (entry[1] // 2, entry[4]) == (inside, part_of)
                )
                ref = slots.at[pl.ds(0, number), rows_of(part_of)]
                passing(ref, twin, sent_sem.at[inside, part_of], twin_sem.at[0]).wait_send()

    def tell(target, entered):
        pl.semaphore_signal(
            known_sem.at[entered], inc=1, device_id={"sample": target}, device_id_type=MESH
        )

    def learn(place, entered):
        pl.semaphore_wait(known_sem.at[entered], 1)
        if place == 1 and entered == 3:
            tell(me - PLANE, 3)
        if place == 2 and entered == 0:
            tell(me + PLANE, 0)

    for place in (1, 2):

        @pl.when(plane == place)
        def _(place=place):
            tell(me - PLANE, place + 1)
            tell(me + PLANE, place - 1)

    def events(group):
        for place in range(LINE):
            entries = EVENTS[place][group]
            if entries:

                @pl.when(plane == place)
                def _(place=place, entries=entries):
                    for origin, own, part_of, low, number in entries:
                        if origin == -2:
                            learn(place, own)
                        if origin >= 0:
                            got(line_of[origin][own], part_of)
                        for slot in range(low, low + number):
                            sent(place, slot).start()

    events(0)
    for load in loads[7:]:
        load.start()

    for index in (1, 2, 3, 4):
        loads[index].wait()
    events(1)
    gain = gain_row[...]
    bias = bias_row[...]
    leading = cls_row[...].astype(f32) + position[0:1, :].astype(f32)
    lead = jnp.broadcast_to(layer_norm(leading, gain, bias), (TILE_ROWS, width)).astype(bf16)
    lead_row = lead[:1].astype(f32)

    events(2)
    placed = position[...].astype(f32)
    placed = placed - jnp.mean(placed, axis=1, keepdims=True)
    blank = jnp.zeros((spots - held_rows, width), f32)
    top = 2 * heads
    placed = jnp.concatenate([placed, blank], axis=0)
    basis[top + padded :, :] = placed.astype(bf16)
    bias_high = bias.astype(bf16).astype(f32)
    ending = jnp.concatenate([blank[3:], bias_high, bias - bias_high, lead_row], axis=0)
    ending = jnp.concatenate([jnp.zeros((held_rows, width), f32), ending], axis=0)
    scaled[padded:, :] = (placed * gain + ending).astype(bf16)
    weight = jnp.broadcast_to(jnp.sum(placed * placed, axis=1, keepdims=True), (spots, 128))
    weight = jnp.concatenate([weight, jnp.zeros((-spots % 128, 128), f32)], axis=0)
    weight = jnp.transpose(weight)[:1, :spots]

    loads[5].wait()
    table = embed[...].astype(f32)
    table = table - jnp.mean(table, axis=1, keepdims=True)
    table = jnp.concatenate([table, jnp.zeros((padded - depth, width), f32)], axis=0)
    basis[top : top + padded, :] = table.astype(bf16)
    scaled[:padded, :] = (table * gain).astype(bf16)

    events(3)
    loads[6].wait()
    query = jnp.dot(lead, query_w[...], preferred_element_type=f32)[:1]
    head_row = lax.broadcasted_iota(jnp.int32, (TILE_ROWS, inner), 0)
    column = lax.broadcasted_iota(jnp.int32, (TILE_ROWS, inner), 1)
    own_head = (column >= head_row * head_dim) & (column < (head_row + 1) * head_dim)
    spread = jnp.where(own_head, jnp.broadcast_to(query, (TILE_ROWS, inner)), 0.0).astype(bf16)
    events(4)
    loads[7].wait()
    turned = contract_last(spread, key_w[...])[:heads] * (1.0 / math.sqrt(head_dim))
    first = jnp.sum(turned * lead_row, axis=1, keepdims=True)
    level = jnp.sum(turned * bias, axis=1, keepdims=True)
    constants[...] = jnp.broadcast_to(level, constants.shape)
    basis[:top, :] = split_in_two(turned * gain)

    features = padded + spots
    for part_of in range(GRAM_PARTS):
        events(5 + part_of)
        low = 256 * (pl.cdiv(features, 256) * part_of // GRAM_PARTS)
        high = min(features, 256 * (pl.cdiv(features, 256) * (part_of + 1) // GRAM_PARTS))
        square = contract_last(basis[: top + padded, :], basis[top + low : top + high, :])
        place = low + lax.broadcasted_iota(jnp.int32, (padded, high - low), 1)
        form[top : top + padded, low:high] = jnp.where(
            place < padded, square[top:], 2.0 * square[top:]
        ).astype(bf16)
        form[:top, low:high] = split_in_two(square[:heads] + square[heads:top])
    sizes = jnp.concatenate([jnp.zeros((1, padded), f32), weight], axis=1)
    sizes_high = sizes.astype(bf16).astype(f32)
    sizes = jnp.concatenate(
        [sizes_high, sizes - sizes_high, jnp.zeros((TILE_ROWS - 2, padded + spots), f32)], axis=0
    )
    form[top + padded :, :] = sizes.astype(bf16)

    loads[8].wait()
    first = jnp.broadcast_to(first[None], (images, heads, 1)).reshape(pairs, 1)
    peak[...] = jnp.broadcast_to(first, peak.shape)
    total[...] = jnp.ones(total.shape, f32)
    gathered[...] = jnp.zeros(gathered.shape, f32)

    cells = 2 * lanes
    lane = lax.broadcasted_iota(jnp.int32, (pairs, cells), 1)
    row_image = lax.broadcasted_iota(jnp.int32, (pairs, cells), 0) // heads
    same = (lane % lanes) // rows == row_image
    spot_row = lax.broadcasted_iota(jnp.int32, (spots, cells), 0)
    spot_lane = lax.broadcasted_iota(jnp.int32, (spots, cells), 1)
    spot_at = spot_row - 1 - (spot_lane // lanes) * rows - spot_lane % rows

    order = sum(mine * packed for mine, packed in zip(here, ORDER, strict=True))
    first_step = 5 + GRAM_PARTS
    fold_rows = scaled.shape[0] // FOLD_PARTS

    def base_of(turn):
        code = (order >> (3 * turn)) % 8
        where, own = code // 2, code % 2
        return where * PLANE + 2 * (side * own + (1 - side) * (1 - own))

    def block_of(base):
        block = jnp.concatenate([slots[base], slots[base + 1]], axis=1)
        spot = jnp.where(spot_at == base * rows, 1.0, 0.0).astype(bf16)
        return jnp.concatenate([block, spot], axis=0)

    def front(base):
        block = block_of(base)
        image = jnp.dot(form[...], block, preferred_element_type=f32)
        norm = jnp.sum(
            image[top : top + padded] * block[:padded].astype(f32), axis=0, keepdims=True
        )
        tail = top + padded
        norm = norm + image[tail : tail + 1] + image[tail + 1 : tail + 2]
        rate = lax.rsqrt(norm * (1.0 / width) + epsilon)
        scores = image[:heads] + image[heads:top]
        kept[:heads, :] = scores * rate + constants[:, :1]
        kept[heads:, :] = jnp.broadcast_to(rate, (heads, cells))

    def back(base, scores, rate):
        block = block_of(base)
        scores = jnp.broadcast_to(scores[None], (images, heads, cells)).reshape(pairs, cells)
        scores = jnp.where(same, scores, LOWEST)
        before = peak[:, :1]
        now = jnp.maximum(before, jnp.max(scores, axis=1, keepdims=True))
        shrink = jnp.exp(before - now)
        chance = jnp.where(same, jnp.exp(scores - now), 0.0)
        peak[...] = jnp.broadcast_to(now, peak.shape)
        total[...] = total[...] * shrink + jnp.sum(chance, axis=1, keepdims=True)
        gathered[...] = gathered[...] * shrink + contract_last((chance * rate).astype(bf16), block)

    def fold(part_of):
        low = pl.multiple_of(part_of * fold_rows, TILE_ROWS)
        product = jnp.dot(
            scaled[pl.ds(low, fold_rows), :], value_w[...], preferred_element_type=f32
        )
        folded[pl.ds(low, fold_rows), :] = product.astype(bf16)
        ends[...] = product[fold_rows - ends.shape[0] :]

    def chip_step(turn, carry):
        for index in range(1, 2 * LINE):
            pl.when(turn == index)(functools.partial(events, first_step + 2 * index))
        base = base_of(turn)
        got_from_twin(base)
        scores = kept[:heads, :]
        rate = kept[heads : heads + 1, :]
        back(base_of(turn - 1), scores, rate)
        front(base)

        for index in range(1, 2 * LINE - 1):
            pl.when(turn == index)(functools.partial(events, first_step + 2 * index + 1))

        @pl.when(turn < FOLD_PARTS)
        def _():
            fold(turn)

        return carry

    events(first_step)
    got_from_twin(base_of(0))
    front(base_of(0))
    events(first_step + 1)
    fold(0)
    lax.fori_loop(1, 2 * LINE, chip_step, 0)
    back(base_of(2 * LINE - 1), kept[:heads, :], kept[heads : heads + 1, :])

    last = ends.shape[0]
    plain = ends[last - 3 : last - 2, :] + ends[last - 2 : last - 1, :]
    lead_value = ends[last - 1 :, :]
    values = jnp.dot(
        split_in_two(gathered[...]), folded[...], preferred_element_type=f32
    )
    share = 1.0 / total[:, :1]
    lead_chance = jnp.exp(first - peak[:, :1]) * share
    values = (values[:pairs] + values[pairs:]) * share
    values = values + plain + (lead_value - plain) * lead_chance
    pair_head = lax.broadcasted_iota(jnp.int32, (pairs, inner), 0) % heads
    pair_column = lax.broadcasted_iota(jnp.int32, (pairs, inner), 1)
    mine_only = (pair_column >= pair_head * head_dim) & (pair_column < (pair_head + 1) * head_dim)
    values = jnp.where(mine_only, values, 0.0)
    mixed = jnp.sum(values.reshape(images, heads, inner), axis=1).astype(bf16)
    loads[9].wait()
    hidden = leading + jnp.dot(mixed, out_w[...], preferred_element_type=f32)
    for index in (10, 11, 12, 13):
        loads[index].wait()
    center = hidden - jnp.mean(hidden, axis=-1, keepdims=True)
    shift = last_bias[...]
    shift_high = shift.astype(bf16)
    shift_low = (shift - shift_high.astype(f32)).astype(bf16)
    rows_in = jnp.concatenate(
        [
            center * last_gain[...],
            shift_high.astype(f32),
            shift_low.astype(f32),
            jnp.zeros((TILE_ROWS - images - 2, width), f32),
        ],
        axis=0,
    ).astype(bf16)
    spread_out = jnp.mean(center * center, axis=-1, keepdims=True)
    products = contract_last(rows_in, class_w[...])
    moved = products[images : images + 1] + products[images + 1 : images + 2] + class_bias[...]
    logits = products[:images] * lax.rsqrt(spread_out + epsilon) + moved
    lifted = logits - jnp.max(logits, axis=-1, keepdims=True)
    logp = lifted - jnp.log(jnp.sum(jnp.exp(lifted), axis=-1, keepdims=True))

    piece_width = part.shape[2]
    classes = out.shape[1]
    part[0] = logp[:, :piece_width]
    part[1] = jnp.concatenate(
        [logp[:, piece_width:], jnp.zeros((images, 2 * piece_width - classes), f32)], axis=1
    )
    swap = pltpu.make_async_remote_copy(
        src_ref=part.at[1 - core],
        dst_ref=from_pair,
        send_sem=tail_send.at[0],
        recv_sem=tail_recv.at[0],
        device_id={"sample": twin},
        device_id_type=MESH,
    )
    swap.start()
    swap.wait_recv()
    mine = part[core]
    theirs = from_pair[...]
    high = jnp.maximum(mine, theirs)
    ring[chip] = high + jnp.log(jnp.exp(mine - high) + jnp.exp(theirs - high))

    def pass_on(ref, target):
        return passing(ref, target, tail_send.at[2], tail_recv.at[2])

    for step in range(1, chips):
        other = step - 1 + jnp.minimum(step // jnp.maximum(chip + 1, 1), 1)
        pass_on(ring.at[chip], 2 * other + core).start()
    pass_on(ring.at[pl.ds(0, chips - 1)], twin).wait_recv()
    every = ring[...]
    high = jnp.max(every, axis=0)
    result[core] = high + jnp.log(jnp.sum(jnp.exp(every - high[None]), axis=0)) - math.log(count)
    share = pltpu.make_async_remote_copy(
        src_ref=result.at[core],
        dst_ref=result.at[core],
        send_sem=tail_send.at[1],
        recv_sem=tail_recv.at[1],
        device_id={"sample": twin},
        device_id_type=MESH,
    )
    share.start()

    for place in range(LINE):

        @pl.when(plane == place)
        def _(place=place):
            all_sent(place)

    swap.wait_send()
    pass_on(ring.at[pl.ds(0, chips - 1)], twin).wait_send()
    pltpu.make_async_remote_copy(
        src_ref=result.at[core],
        dst_ref=result.at[1 - core],
        send_sem=tail_send.at[1],
        recv_sem=tail_recv.at[1],
        device_id={"sample": twin},
        device_id_type=MESH,
    ).wait_recv()
    share.wait_send()
    out[:, :piece_width] = result[0]
    out[:, piece_width:] = result[1][:, : classes - piece_width]


def kernel_shards(
    patches,
    patch_weight,
    cls_token,
    pos_embed,
    ln1_gain,
    ln1_bias,
    w_query,
    w_key,
    w_value,
    w_out,
    lnf_gain,
    lnf_bias,
    head_w,
    head_bias,
):
    count = lax.axis_size("sample")
    images, rows, depth = patches.shape
    width = patch_weight.shape[2]
    inner = w_query.shape[2]
    heads = inner // HEAD_DIM
    pairs = heads * images
    chips = count // 2
    classes = head_w.shape[2]
    piece_width = pl.cdiv(classes, 256) * 128
    padded = pl.cdiv(depth, TILE_ROWS) * TILE_ROWS
    tall = FOLD_PARTS * TILE_ROWS
    features = pl.cdiv(padded + pos_embed.shape[1] + 3, tall) * tall
    far = pl.BlockSpec(memory_space=pl.ANY)
    dma = pltpu.SemaphoreType.DMA
    f32, bf16 = jnp.float32, jnp.bfloat16
    class_rows = jnp.swapaxes(head_w, 1, 2)
    given = (
        patches,
        cls_token,
        pos_embed,
        ln1_gain,
        ln1_bias,
        patch_weight,
        w_query,
        w_key,
        w_value,
        w_out,
        class_rows,
        lnf_gain,
        lnf_bias,
        head_bias,
    )
    held = [
        pltpu.VMEM(a.shape[1:] if place and a.ndim == 3 else a.shape, a.dtype)
        for place, a in enumerate(given)
    ]
    return pl.pallas_call(
        functools.partial(whole_kernel, count, heads),
        out_shape=pltpu.VMEM((images, classes), f32),
        in_specs=[far] * len(given),
        out_specs=pl.BlockSpec(memory_space=pltpu.VMEM),
        scratch_shapes=[
            *held,
            pltpu.VMEM((count, padded, images * rows), bf16),
            pltpu.VMEM((2 * heads + features, width), bf16),
            pltpu.VMEM((features, width), bf16),
            pltpu.VMEM((padded + 2 * heads + TILE_ROWS, features), bf16),
            pltpu.VMEM((features, inner), bf16),
            pltpu.VMEM((TILE_ROWS, inner), f32),
            pltpu.VMEM((heads, 128), f32),
            pltpu.VMEM((2 * heads, 2 * images * rows), f32),
            pltpu.VMEM((pairs, features), f32),
            pltpu.VMEM((pairs, 128), f32),
            pltpu.VMEM((pairs, 128), f32),
            pltpu.VMEM((2, images, piece_width), f32),
            pltpu.VMEM((images, piece_width), f32),
            pltpu.VMEM((chips, images, piece_width), f32),
            pltpu.VMEM((2, images, piece_width), f32),
            dma((len(given),)),
            dma((chips, PIECES)),
            dma((chips,)),
            dma((2, PIECES)),
            pltpu.SemaphoreType.REGULAR((LINE,)),
            dma((3,)),
            dma((3,)),
        ],
        compiler_params=pltpu.CompilerParams(
            collective_id=0, has_side_effects=True, vmem_limit_bytes=60 << 20
        ),
    )(*given)


def takes_kernel(mesh, patches):
    count = mesh.shape["sample"]
    rows = patches.shape[1] // count
    images = patches.shape[0] // mesh.shape["group"]
    return count == PLANE * LINE and rows % TILE_ROWS == 0 and images * rows == 128


def solution(mesh):
    placed = (
        P("group", "sample", None),
        P("sample", None, None),
        P("sample", None),
        P("sample", None, None),
        P("sample", None),
        P("sample", None),
        P("sample", None, None),
        P("sample", None, None),
        P("sample", None, None),
        P("sample", None, None),
        P("sample", None),
        P("sample", None),
        P("sample", None, None),
        P("sample", None),
    )

    def run(*arrays):
        step = kernel_shards if takes_kernel(mesh, arrays[0]) else shards
        return jax.shard_map(
            step, mesh=mesh, in_specs=placed, out_specs=P("group", None), check_vma=False
        )(*arrays)

    return run
```

```python
import functools
import math

import jax
import jax.numpy as jnp
from jax import lax
from jax.experimental import pallas as pl
from jax.experimental.pallas import tpu as pltpu
from jax.sharding import PartitionSpec as P

HEAD_DIM = 80


epsilon = 1e-06


def combined_all(part, axis, combine):
    gathered = jax.tree.map(lambda a: lax.all_gather(a, axis), part)

    def take(source):
        return jax.tree.map(lambda a: lax.dynamic_index_in_dim(a, source, 0, False), gathered)

    return lax.fori_loop(
        1, lax.axis_size(axis), lambda source, state: combine(state, take(source)), take(0)
    )


def layer_norm(values, gain, shift):
    center = values - jnp.mean(values, axis=-1, keepdims=True)
    spread = jnp.mean(center * center, axis=-1, keepdims=True)
    return center * lax.rsqrt(spread + epsilon) * gain + shift


def shards(
    patches,
    patch_weight,
    cls_token,
    pos_embed,
    ln1_gain,
    ln1_bias,
    w_query,
    w_key,
    w_value,
    w_out,
    lnf_gain,
    lnf_bias,
    head_w,
    head_bias,
):
    embed_weight = patch_weight[0]
    position = pos_embed[0]
    gain_first = ln1_gain[0]
    bias_first = ln1_bias[0]
    query_weight = w_query[0]
    pair_weight = jnp.concatenate([w_key[0], w_value[0]], axis=1)
    out_weight = w_out[0]
    width = embed_weight.shape[1]
    inner = query_weight.shape[1]
    head_count = inner // HEAD_DIM
    leading = cls_token[0].astype(jnp.float32) + position[0].astype(jnp.float32)
    lead_norm = layer_norm(leading, gain_first, bias_first).astype(jnp.bfloat16)
    lead_pair = jnp.dot(lead_norm[None], pair_weight, preferred_element_type=jnp.float32).astype(
        jnp.bfloat16
    )
    query = jnp.dot(lead_norm[None], query_weight, preferred_element_type=jnp.float32).astype(
        jnp.bfloat16
    )
    query = query.reshape(head_count, HEAD_DIM)
    portion = lax.all_gather(patches, "sample", axis=1, tiled=True)
    image_count = portion.shape[0]
    row_count = portion.shape[1]
    flat = portion.reshape(-1, portion.shape[2])
    tokens = jnp.dot(flat, embed_weight, preferred_element_type=jnp.float32).reshape(
        image_count, row_count, width
    )
    placed = lax.dynamic_slice_in_dim(position, 1, row_count, 0)
    tokens = tokens + placed.astype(jnp.float32)[None]
    normed = layer_norm(tokens, gain_first, bias_first).astype(jnp.bfloat16)
    paired = jnp.dot(normed.reshape(-1, width), pair_weight, preferred_element_type=jnp.float32)
    key_values = paired.astype(jnp.bfloat16).reshape(image_count, row_count, 2 * inner)
    image_count = key_values.shape[0]
    lead_rows = jnp.broadcast_to(lead_pair[None], (image_count, 1, 2 * inner))
    full_rows = jnp.concatenate([lead_rows, key_values], axis=1)
    key_rows = full_rows[:, :, :inner].reshape(image_count, -1, head_count, HEAD_DIM)
    value_rows = full_rows[:, :, inner:].reshape(image_count, -1, head_count, HEAD_DIM)
    scores = jnp.einsum(
        "hd,ithd->iht", query, key_rows, preferred_element_type=jnp.float32
    ) / math.sqrt(HEAD_DIM)
    attention = jax.nn.softmax(scores, axis=-1).astype(jnp.bfloat16)
    mixed = jnp.einsum("iht,ithd->ihd", attention, value_rows, preferred_element_type=jnp.float32)
    mixed = mixed.astype(jnp.bfloat16).reshape(image_count, inner)
    hidden = leading[None] + jnp.dot(mixed, out_weight, preferred_element_type=jnp.float32)
    final = layer_norm(hidden, lnf_gain[0], lnf_bias[0]).astype(jnp.bfloat16)
    logits = jnp.dot(final, head_w[0], preferred_element_type=jnp.float32) + head_bias[0]
    logp = jax.nn.log_softmax(logits, axis=-1)
    count = lax.axis_size("sample")

    def combine(earlier, later):
        highest = jnp.maximum(earlier[0], later[0])
        summed = earlier[1] * jnp.exp(earlier[0] - highest) + later[1] * jnp.exp(later[0] - highest)
        return (highest, summed)

    peak, total = combined_all((logp, jnp.ones_like(logp)), "sample", combine)
    return peak + jnp.log(total) - math.log(count)


MESH = pl.DeviceIdType.MESH
PLANE = 4
LINE = 4
TILE_ROWS = 16
LOWEST = -1e30
GRAM_PARTS = 2
FOLD_PARTS = 3


def split_in_two(values):
    high = values.astype(jnp.bfloat16)
    low = (values - high.astype(jnp.float32)).astype(jnp.bfloat16)
    return jnp.concatenate([high, low], axis=0)


PIECES = 4
SENDS = (
    (
        (0,0,0,1,3), (1,1,0,1,1), (1,1,0,1,0), (1,1,0,1,2), (1,1,0,1,3), (0,0,0,1,0), (0,2,0,1,0),
        (0,2,0,1,1), (0,2,0,1,2), (0,2,0,1,3), (3,1,0,1,0), (1,1,0,0,3), (0,0,0,1,1), (2,1,0,0,3),
        (0,2,0,0,3), (0,0,1,1,2), (0,2,1,1,2), (3,1,0,1,3), (1,1,0,0,0), (0,2,0,0,0), (0,2,1,1,0),
        (0,0,0,1,2), (0,2,1,1,3), (0,0,1,1,1), (0,2,1,1,1), (3,1,0,0,1), (0,2,0,0,1), (0,2,1,0,2),
        (2,1,0,1,0), (0,2,1,0,3), (2,1,0,0,2), (3,1,0,0,2), (0,2,0,0,2), (0,0,2,1,0), (0,2,2,1,0),
        (0,2,1,0,1), (0,0,2,1,2), (0,2,2,1,2), (0,2,3,0,3), (0,0,2,1,3), (0,2,2,1,3), (0,0,2,1,1),
        (0,2,2,1,1), (0,2,3,0,0), (0,2,1,0,0), (0,2,2,0,0), (0,2,3,0,1), (0,2,2,0,2), (0,2,3,1,3),
        (0,2,3,0,2), (0,2,2,0,3), (0,2,3,1,1), (0,2,2,0,1), (0,2,3,1,0), (0,2,3,1,2),
    ),
    (
        (2,1,1,1,0), (2,1,1,1,3), (2,1,1,1,1), (0,1,1,1,2), (1,0,1,1,3), (2,1,1,1,2), (0,1,1,1,0),
        (0,1,1,1,3), (0,1,1,1,1), (1,0,1,1,2), (1,2,1,1,0), (1,2,1,1,1), (1,2,1,1,2), (1,2,1,1,3),
        (1,0,1,1,0), (2,1,0,1,1), (1,0,0,1,1), (1,2,0,1,1), (0,1,1,0,3), (1,2,1,0,3), (1,2,0,1,0),
        (1,2,1,0,2), (1,0,2,1,0), (0,1,2,1,0), (1,2,2,1,0), (1,0,0,1,2), (2,1,0,1,2), (1,2,0,1,2),
        (1,0,1,1,1), (1,0,2,1,3), (0,1,2,1,3), (1,2,2,1,3), (2,1,0,1,3), (1,2,0,1,3), (0,1,2,1,1),
        (1,0,2,1,1), (1,2,2,1,1), (1,0,2,1,2), (1,2,2,1,2), (0,1,1,0,0), (1,2,1,0,0), (1,2,0,0,3),
        (1,2,0,0,1), (1,2,2,0,0), (0,1,3,1,3), (1,0,3,1,3), (1,2,3,1,3), (1,2,0,0,2), (1,2,0,0,0),
        (1,0,3,1,1), (0,1,3,1,1), (1,2,3,1,1), (1,2,1,0,1), (1,2,2,0,3), (0,1,3,1,0), (1,0,3,1,0),
        (1,2,3,1,0), (1,2,2,0,1), (0,1,3,1,2), (1,2,3,1,2), (1,2,2,0,2), (1,2,3,0,3), (1,2,3,0,1),
        (1,2,3,0,2), (1,2,3,0,0),
    ),
    (
        (1,1,2,1,0), (1,1,2,1,3), (1,1,2,1,1), (2,0,2,1,3), (3,1,2,1,0), (2,0,2,1,0), (2,0,2,1,1),
        (3,1,2,1,2), (3,1,2,1,3), (3,1,2,1,1), (1,1,2,1,2), (2,0,2,1,2), (2,2,2,1,0), (2,2,2,1,1),
        (2,2,2,1,2), (2,2,2,1,3), (0,1,2,1,2), (3,1,1,1,0), (2,0,1,1,0), (2,2,1,1,0), (2,0,1,1,3),
        (3,1,1,1,3), (2,2,1,1,3), (2,2,2,0,3), (3,1,1,1,1), (2,0,1,1,1), (2,2,1,1,1), (1,1,3,1,1),
        (2,0,3,1,1), (2,2,3,1,1), (2,2,2,0,0), (1,1,3,1,0), (2,2,3,1,0), (2,2,2,0,1), (2,0,1,1,2),
        (3,1,1,1,2), (2,2,1,1,2), (2,0,3,1,2), (1,1,3,1,2), (2,2,3,1,2), (2,2,2,0,2), (2,2,3,1,3),
        (2,2,1,0,0), (2,2,1,0,3), (2,2,0,0,3), (2,0,0,1,1), (3,1,0,1,1), (2,2,0,1,1), (2,2,1,0,1),
        (3,1,0,1,2), (2,2,0,1,2), (2,2,3,0,3), (2,2,3,0,1), (2,2,0,1,3), (2,2,3,0,0), (2,2,1,0,2),
        (2,2,3,0,2), (2,0,0,1,0), (2,2,0,1,0), (2,2,0,0,1), (2,2,0,0,2), (2,2,0,0,0),
    ),
    (
        (2,1,3,1,1), (2,1,3,1,0), (3,0,3,1,3), (3,0,3,1,0), (2,1,3,1,2), (2,1,3,1,3), (3,2,3,1,0),
        (3,2,3,1,1), (3,2,3,1,2), (3,2,3,1,3), (1,1,3,1,3), (3,0,2,1,0), (3,2,2,1,0), (0,1,3,0,3),
        (2,1,3,0,3), (3,0,3,1,1), (3,2,3,0,3), (3,0,2,1,2), (3,2,2,1,2), (2,1,3,0,0), (0,1,3,0,0),
        (3,2,3,0,0), (3,0,3,1,2), (3,0,2,1,3), (3,2,2,1,3), (3,0,2,1,1), (3,2,2,1,1), (3,0,0,1,0),
        (3,2,0,1,0), (3,2,2,0,0), (0,1,3,0,1), (3,2,3,0,1), (3,0,1,1,0), (3,2,1,1,0), (3,2,2,0,2),
        (3,0,1,1,3), (3,2,1,1,3), (3,0,0,1,3), (3,2,0,1,3), (0,1,3,0,2), (1,1,3,0,2), (3,2,3,0,2),
        (3,0,1,1,1), (3,2,1,1,1), (3,2,2,0,3), (3,0,1,1,2), (3,2,1,1,2), (3,2,0,0,1), (3,2,2,0,1),
        (3,2,0,0,0), (3,2,0,1,1), (3,2,1,0,0), (3,2,0,1,2), (3,2,0,0,2), (3,2,1,0,3), (3,2,0,0,3),
        (3,2,1,0,1), (3,2,1,0,2),
    ),
)
EVENTS = (
    (
        ((-1,0,0,0,10),), (), (), ((-2,2,0,10,0),), (), (), ((-2,3,0,10,1),(0,0,3,11,4)),
        ((1,1,2,15,2),(0,0,0,17,3)), ((1,1,0,20,1),(1,1,3,21,2)), ((1,1,1,23,2),),
        ((0,0,1,25,2),(1,0,2,27,1),(1,0,3,28,2)), ((0,0,2,30,3),),
        ((2,1,0,33,2),(1,0,1,35,1),(2,1,2,36,2),(3,0,3,38,1),(2,1,3,39,2)), ((2,1,1,41,2),),
        ((3,0,0,43,1),(1,0,0,44,1)), (), ((2,0,0,45,1),(3,0,1,46,1),(2,0,2,47,1),(3,1,3,48,1),(3,0,2,49,1)),
        ((2,0,3,50,1),(3,1,1,51,1)), ((2,0,1,52,1),(3,1,0,53,1),(3,1,2,54,1)), (), (), (),
    ),
    (
        ((-1,0,0,0,14),), (), (), (), ((-2,3,0,14,0),), (), ((0,1,1,14,4),(1,0,3,18,2)),
        ((0,1,0,20,1),(1,0,2,21,1),(2,1,0,22,3),(0,1,2,25,3)), ((2,1,3,28,4),(0,1,3,32,2)), ((2,1,1,34,3),),
        ((2,1,2,37,2),(1,0,0,39,2),(0,0,3,41,1)), ((0,0,1,42,1),), ((2,0,0,43,1),(3,1,3,44,3),(0,0,2,47,1)),
        ((0,0,0,48,1),(3,1,1,49,3),(1,0,1,52,1)), ((2,0,3,53,1),(3,1,0,54,3),(2,0,1,57,1),(3,1,2,58,2)),
        ((2,0,2,60,1),), ((3,0,3,61,1),), (), ((3,0,1,62,1),), (), (), ((3,0,2,63,1),(3,0,0,64,1)),
    ),
    (
        ((-1,0,0,0,16),), ((-2,0,0,16,1),), (), (), (), ((1,1,0,17,3),), ((1,1,3,20,3),(2,0,3,23,1)),
        ((1,1,1,24,3),(3,1,1,27,3),(2,0,0,30,1)), ((3,1,0,31,2),(2,0,1,33,1),(1,1,2,34,3)),
        ((3,1,2,37,3),(2,0,2,40,1),(3,1,3,41,1),(1,0,0,42,1)), ((1,0,3,43,1),(0,0,3,44,1)),
        ((0,1,1,45,3),(1,0,1,48,1)),
        ((0,1,2,49,2),(3,0,3,51,1),(3,0,1,52,1),(0,1,3,53,1),(3,0,0,54,1),(1,0,2,55,1)), ((3,0,2,56,1),),
        ((0,1,0,57,2),), (), ((0,0,1,59,1),(0,0,2,60,1)), (), (), (), (), ((0,0,0,61,1),),
    ),
    (
        ((-1,0,0,0,10),), ((-2,1,0,10,1),(-2,0,0,11,0)), (), (), (), ((2,1,0,11,2),),
        ((3,0,3,13,4),(2,1,2,17,2)), ((3,0,0,19,3),), ((2,1,3,22,3),),
        ((2,1,1,25,2),(0,1,0,27,2),(2,0,0,29,1)),
        ((3,0,1,30,2),(1,1,0,32,2),(2,0,2,34,1),(1,1,3,35,2),(0,1,3,37,2)), ((3,0,2,39,3),),
        ((1,1,1,42,2),(2,0,3,44,1),(1,1,2,45,2),(0,0,1,47,1),(2,0,1,48,1)),
        ((0,0,0,49,1),(0,1,1,50,1),(1,0,0,51,1)), ((0,1,2,52,1),(0,0,2,53,1),(1,0,3,54,1)), (),
        ((0,0,3,55,1),), (), ((1,0,1,56,1),(1,0,2,57,1)), (), (), (),
    ),
)
ORDER = (15936025, 13869387, 470813, 4245423)


def contract_last(left, right):
    return lax.dot_general(
        left, right, (((1,), (1,)), ((), ())), preferred_element_type=jnp.float32
    )


def whole_kernel(
    count,
    heads,
    patches,
    cls_token,
    pos_embed,
    ln1_gain,
    ln1_bias,
    patch_weight,
    w_query,
    w_key,
    w_value,
    w_out,
    head_w,
    lnf_gain,
    lnf_bias,
    head_bias,
    out,
    own_patches,
    cls_row,
    position,
    gain_row,
    bias_row,
    embed,
    query_w,
    key_w,
    value_w,
    out_w,
    class_w,
    last_gain,
    last_bias,
    class_bias,
    slots,
    basis,
    scaled,
    form,
    folded,
    ends,
    constants,
    kept,
    gathered,
    peak,
    total,
    part,
    from_pair,
    ring,
    result,
    load_sem,
    recv_sem,
    twin_sem,
    sent_sem,
    known_sem,
    tail_send,
    tail_recv,
):
    f32, bf16 = jnp.float32, jnp.bfloat16
    me = lax.axis_index("sample")
    core = me % 2
    side = (me // 2) % 2
    chip = me // 2
    chips = count // 2
    plane = me // PLANE
    images, rows, depth = own_patches.shape
    padded = slots.shape[1]
    lanes = slots.shape[2]
    tiles = padded // TILE_ROWS
    cuts = tuple(TILE_ROWS * (tiles * place // PIECES) for place in range(PIECES + 1))
    width = embed.shape[1]
    inner = query_w.shape[1]
    head_dim = inner // heads
    pairs = heads * images
    spots = basis.shape[0] - 2 * heads - padded
    held_rows = position.shape[0]

    loads = []
    for index, (source, target) in enumerate(
        (
            (patches, own_patches),
            (pos_embed.at[0], position),
            (cls_token, cls_row),
            (ln1_gain, gain_row),
            (ln1_bias, bias_row),
            (patch_weight.at[0], embed),
            (w_query.at[0], query_w),
            (w_key.at[0], key_w),
            (w_value.at[0], value_w),
            (w_out.at[0], out_w),
            (head_w.at[0], class_w),
            (lnf_gain, last_gain),
            (lnf_bias, last_bias),
            (head_bias, class_bias),
        )
    ):
        loads.append(pltpu.make_async_copy(source, target, load_sem.at[index]))
    for load in loads[:5]:
        load.start()

    twin = me + 1 - 2 * core
    beside = plane * PLANE + (1 - side) * 2 + core
    here = tuple(lax.convert_element_type(plane == place, jnp.int32) for place in range(LINE))
    line_of = tuple(
        (place * PLANE + (1 - side) * 2 + core, place * PLANE + side * 2 + core)
        for place in range(LINE)
    )

    barrier = pltpu.get_barrier_semaphore()

    def greet(target):
        pl.semaphore_signal(barrier, inc=1, device_id={"sample": target}, device_id_type=MESH)

    greet(twin)
    greet(beside)

    @pl.when(plane > 0)
    def _():
        greet(me - PLANE)

    @pl.when(plane < LINE - 1)
    def _():
        greet(me + PLANE)

    loads[0].wait()
    for load in loads[5:7]:
        load.start()
    eye = (
        lax.broadcasted_iota(jnp.int32, (padded, depth), 0)
        == lax.broadcasted_iota(jnp.int32, (padded, depth), 1)
    ).astype(bf16)
    flat = own_patches[...].reshape(images * rows, depth)
    slots[me] = contract_last(eye, flat).astype(bf16)
    pl.semaphore_wait(barrier, LINE - here[0] - here[LINE - 1])

    def passing(ref, target, sent_by, got_by):
        return pltpu.make_async_remote_copy(
            src_ref=ref,
            dst_ref=ref,
            send_sem=sent_by,
            recv_sem=got_by,
            device_id={"sample": target},
            device_id_type=MESH,
        )

    def rows_of(part_of):
        return pl.ds(cuts[part_of], cuts[part_of + 1] - cuts[part_of])

    def sent(place, slot):
        to, aside, origin, own, part_of = SENDS[place][slot]
        inside = aside // 2
        source = line_of[origin][own]
        got_by = twin_sem.at[source // 2] if inside else recv_sem.at[source // 2, part_of]
        target = twin if inside else line_of[to][aside]
        ref = slots.at[source, rows_of(part_of)]
        return passing(ref, target, sent_sem.at[PIECES if inside else part_of], got_by)

    def got(source, part_of):
        ref = slots.at[source, rows_of(part_of)]
        passing(ref, twin, sent_sem.at[0], recv_sem.at[source // 2, part_of]).wait_recv()

    def got_from_twin(base):
        ref = slots.at[base + 1 - core]
        passing(ref, twin, sent_sem.at[0], twin_sem.at[base // 2]).wait_recv()

    def all_sent(place):
        for part_of in range(PIECES):
            number = sum(1 for entry in SENDS[place] if entry[1] < 2 and entry[4] == part_of)
            ref = slots.at[pl.ds(0, number), rows_of(part_of)]
            passing(ref, twin, sent_sem.at[part_of], twin_sem.at[0]).wait_send()
        ref = slots.at[pl.ds(0, chips)]
        passing(ref, twin, sent_sem.at[PIECES], twin_sem.at[0]).wait_send()

    def tell(target, far):
        pl.semaphore_signal(
            known_sem.at[far], inc=1, device_id={"sample": target}, device_id_type=MESH
        )

    def learn(place, entered):
        pl.semaphore_wait(known_sem.at[abs(entered - place) - 2], 1)
        if place == 1 and entered == 3:
            tell(me - PLANE, 1)
        if place == 2 and entered == 0:
            tell(me + PLANE, 1)

    for place in (1, 2):

        @pl.when(plane == place)
        def _(place=place):
            tell(me - PLANE, 0)
            tell(me + PLANE, 0)

    def events(group):
        for place in range(LINE):
            entries = EVENTS[place][group]
            if entries:

                @pl.when(plane == place)
                def _(place=place, entries=entries):
                    for origin, own, part_of, low, number in entries:
                        if origin == -2:
                            learn(place, own)
                        if origin >= 0:
                            got(line_of[origin][own], part_of)
                        for slot in range(low, low + number):
                            sent(place, slot).start()

    events(0)
    for load in loads[7:]:
        load.start()

    for index in (1, 2, 3, 4):
        loads[index].wait()
    events(1)
    gain = gain_row[...]
    bias = bias_row[...]
    leading = cls_row[...].astype(f32) + position[0:1, :].astype(f32)
    lead = jnp.broadcast_to(layer_norm(leading, gain, bias), (TILE_ROWS, width)).astype(bf16)
    lead_row = lead[:1].astype(f32)

    events(2)
    placed = position[...].astype(f32)
    placed = placed - jnp.mean(placed, axis=1, keepdims=True)
    blank = jnp.zeros((spots - held_rows, width), f32)
    top = 2 * heads
    placed = jnp.concatenate([placed, blank], axis=0)
    basis[top + padded :, :] = placed.astype(bf16)
    bias_high = bias.astype(bf16).astype(f32)
    ending = jnp.concatenate([blank[3:], bias_high, bias - bias_high, lead_row], axis=0)
    ending = jnp.concatenate([jnp.zeros((held_rows, width), f32), ending], axis=0)
    scaled[padded:, :] = (placed * gain + ending).astype(bf16)
    weight = jnp.broadcast_to(jnp.sum(placed * placed, axis=1, keepdims=True), (spots, 128))
    weight = jnp.concatenate([weight, jnp.zeros((-spots % 128, 128), f32)], axis=0)
    weight = jnp.transpose(weight)[:1, :spots]

    loads[5].wait()
    table = embed[...].astype(f32)
    table = table - jnp.mean(table, axis=1, keepdims=True)
    table = jnp.concatenate([table, jnp.zeros((padded - depth, width), f32)], axis=0)
    basis[top : top + padded, :] = table.astype(bf16)
    scaled[:padded, :] = (table * gain).astype(bf16)

    events(3)
    loads[6].wait()
    query = jnp.dot(lead, query_w[...], preferred_element_type=f32)[:1]
    head_row = lax.broadcasted_iota(jnp.int32, (TILE_ROWS, inner), 0)
    column = lax.broadcasted_iota(jnp.int32, (TILE_ROWS, inner), 1)
    own_head = (column >= head_row * head_dim) & (column < (head_row + 1) * head_dim)
    spread = jnp.where(own_head, jnp.broadcast_to(query, (TILE_ROWS, inner)), 0.0).astype(bf16)
    events(4)
    loads[7].wait()
    turned = contract_last(spread, key_w[...])[:heads] * (1.0 / math.sqrt(head_dim))
    first = jnp.sum(turned * lead_row, axis=1, keepdims=True)
    level = jnp.sum(turned * bias, axis=1, keepdims=True)
    constants[...] = jnp.broadcast_to(level, constants.shape)
    basis[:top, :] = split_in_two(turned * gain)

    features = padded + spots
    for part_of in range(GRAM_PARTS):
        events(5 + part_of)
        low = 256 * (pl.cdiv(features, 256) * part_of // GRAM_PARTS)
        high = min(features, 256 * (pl.cdiv(features, 256) * (part_of + 1) // GRAM_PARTS))
        square = contract_last(basis[: top + padded, :], basis[top + low : top + high, :])
        place = low + lax.broadcasted_iota(jnp.int32, (padded, high - low), 1)
        form[top : top + padded, low:high] = jnp.where(
            place < padded, square[top:], 2.0 * square[top:]
        ).astype(bf16)
        form[:top, low:high] = split_in_two(square[:heads] + square[heads:top])
    sizes = jnp.concatenate([jnp.zeros((1, padded), f32), weight], axis=1)
    sizes_high = sizes.astype(bf16).astype(f32)
    sizes = jnp.concatenate(
        [sizes_high, sizes - sizes_high, jnp.zeros((TILE_ROWS - 2, padded + spots), f32)], axis=0
    )
    form[top + padded :, :] = sizes.astype(bf16)

    loads[8].wait()
    first = jnp.broadcast_to(first[None], (images, heads, 1)).reshape(pairs, 1)
    peak[...] = jnp.broadcast_to(first, peak.shape)
    total[...] = jnp.ones(total.shape, f32)
    gathered[...] = jnp.zeros(gathered.shape, f32)

    cells = 2 * lanes
    lane = lax.broadcasted_iota(jnp.int32, (pairs, cells), 1)
    row_image = lax.broadcasted_iota(jnp.int32, (pairs, cells), 0) // heads
    same = (lane % lanes) // rows == row_image
    spot_row = lax.broadcasted_iota(jnp.int32, (spots, cells), 0)
    spot_lane = lax.broadcasted_iota(jnp.int32, (spots, cells), 1)
    spot_at = spot_row - 1 - (spot_lane // lanes) * rows - spot_lane % rows

    order = sum(mine * packed for mine, packed in zip(here, ORDER, strict=True))
    first_step = 5 + GRAM_PARTS
    fold_rows = scaled.shape[0] // FOLD_PARTS

    def base_of(turn):
        code = (order >> (3 * turn)) % 8
        where, own = code // 2, code % 2
        return where * PLANE + 2 * (side * own + (1 - side) * (1 - own))

    def block_of(base):
        block = jnp.concatenate([slots[base], slots[base + 1]], axis=1)
        spot = jnp.where(spot_at == base * rows, 1.0, 0.0).astype(bf16)
        return jnp.concatenate([block, spot], axis=0)

    def front(base):
        block = block_of(base)
        image = jnp.dot(form[...], block, preferred_element_type=f32)
        norm = jnp.sum(
            image[top : top + padded] * block[:padded].astype(f32), axis=0, keepdims=True
        )
        tail = top + padded
        norm = norm + image[tail : tail + 1] + image[tail + 1 : tail + 2]
        rate = lax.rsqrt(norm * (1.0 / width) + epsilon)
        scores = image[:heads] + image[heads:top]
        kept[:heads, :] = scores * rate + constants[:, :1]
        kept[heads:, :] = jnp.broadcast_to(rate, (heads, cells))

    def back(base, scores, rate):
        block = block_of(base)
        scores = jnp.broadcast_to(scores[None], (images, heads, cells)).reshape(pairs, cells)
        scores = jnp.where(same, scores, LOWEST)
        before = peak[:, :1]
        now = jnp.maximum(before, jnp.max(scores, axis=1, keepdims=True))
        shrink = jnp.exp(before - now)
        chance = jnp.where(same, jnp.exp(scores - now), 0.0)
        peak[...] = jnp.broadcast_to(now, peak.shape)
        total[...] = total[...] * shrink + jnp.sum(chance, axis=1, keepdims=True)
        gathered[...] = gathered[...] * shrink + contract_last((chance * rate).astype(bf16), block)

    def fold(part_of):
        low = pl.multiple_of(part_of * fold_rows, TILE_ROWS)
        product = jnp.dot(
            scaled[pl.ds(low, fold_rows), :], value_w[...], preferred_element_type=f32
        )
        folded[pl.ds(low, fold_rows), :] = product.astype(bf16)
        ends[...] = product[fold_rows - ends.shape[0] :]

    def chip_step(turn, carry):
        for index in range(1, 2 * LINE):
            pl.when(turn == index)(functools.partial(events, first_step + 2 * index))
        base = base_of(turn)
        got_from_twin(base)
        scores = kept[:heads, :]
        rate = kept[heads : heads + 1, :]
        back(base_of(turn - 1), scores, rate)
        front(base)

        for index in range(1, 2 * LINE - 1):
            pl.when(turn == index)(functools.partial(events, first_step + 2 * index + 1))

        @pl.when(turn < FOLD_PARTS)
        def _():
            fold(turn)

        return carry

    events(first_step)
    got_from_twin(base_of(0))
    front(base_of(0))
    events(first_step + 1)
    fold(0)
    lax.fori_loop(1, 2 * LINE, chip_step, 0)
    back(base_of(2 * LINE - 1), kept[:heads, :], kept[heads : heads + 1, :])

    last = ends.shape[0]
    plain = ends[last - 3 : last - 2, :] + ends[last - 2 : last - 1, :]
    lead_value = ends[last - 1 :, :]
    values = jnp.dot(
        split_in_two(gathered[...]), folded[...], preferred_element_type=f32
    )
    share = 1.0 / total[:, :1]
    lead_chance = jnp.exp(first - peak[:, :1]) * share
    values = (values[:pairs] + values[pairs:]) * share
    values = values + plain + (lead_value - plain) * lead_chance
    pair_head = lax.broadcasted_iota(jnp.int32, (pairs, inner), 0) % heads
    pair_column = lax.broadcasted_iota(jnp.int32, (pairs, inner), 1)
    mine_only = (pair_column >= pair_head * head_dim) & (pair_column < (pair_head + 1) * head_dim)
    values = jnp.where(mine_only, values, 0.0)
    mixed = jnp.sum(values.reshape(images, heads, inner), axis=1).astype(bf16)
    loads[9].wait()
    hidden = leading + jnp.dot(mixed, out_w[...], preferred_element_type=f32)
    for index in (10, 11, 12, 13):
        loads[index].wait()
    center = hidden - jnp.mean(hidden, axis=-1, keepdims=True)
    shift = last_bias[...]
    shift_high = shift.astype(bf16)
    shift_low = (shift - shift_high.astype(f32)).astype(bf16)
    rows_in = jnp.concatenate(
        [
            center * last_gain[...],
            shift_high.astype(f32),
            shift_low.astype(f32),
            jnp.zeros((TILE_ROWS - images - 2, width), f32),
        ],
        axis=0,
    ).astype(bf16)
    spread_out = jnp.mean(center * center, axis=-1, keepdims=True)
    products = contract_last(rows_in, class_w[...])
    moved = products[images : images + 1] + products[images + 1 : images + 2] + class_bias[...]
    logits = products[:images] * lax.rsqrt(spread_out + epsilon) + moved
    lifted = logits - jnp.max(logits, axis=-1, keepdims=True)
    logp = lifted - jnp.log(jnp.sum(jnp.exp(lifted), axis=-1, keepdims=True))

    piece_width = part.shape[2]
    classes = out.shape[1]
    part[0] = logp[:, :piece_width]
    part[1] = jnp.concatenate(
        [logp[:, piece_width:], jnp.zeros((images, 2 * piece_width - classes), f32)], axis=1
    )
    swap = pltpu.make_async_remote_copy(
        src_ref=part.at[1 - core],
        dst_ref=from_pair,
        send_sem=tail_send.at[0],
        recv_sem=tail_recv.at[0],
        device_id={"sample": twin},
        device_id_type=MESH,
    )
    swap.start()
    swap.wait_recv()
    mine = part[core]
    theirs = from_pair[...]
    high = jnp.maximum(mine, theirs)
    ring[chip] = high + jnp.log(jnp.exp(mine - high) + jnp.exp(theirs - high))

    def pass_on(ref, target):
        return passing(ref, target, tail_send.at[2], tail_recv.at[2])

    for step in range(1, chips):
        other = step - 1 + jnp.minimum(step // jnp.maximum(chip + 1, 1), 1)
        pass_on(ring.at[chip], 2 * other + core).start()
    pass_on(ring.at[pl.ds(0, chips - 1)], twin).wait_recv()
    every = ring[...]
    high = jnp.max(every, axis=0)
    result[core] = high + jnp.log(jnp.sum(jnp.exp(every - high[None]), axis=0)) - math.log(count)
    share = pltpu.make_async_remote_copy(
        src_ref=result.at[core],
        dst_ref=result.at[core],
        send_sem=tail_send.at[1],
        recv_sem=tail_recv.at[1],
        device_id={"sample": twin},
        device_id_type=MESH,
    )
    share.start()

    for place in range(LINE):

        @pl.when(plane == place)
        def _(place=place):
            all_sent(place)

    swap.wait_send()
    pass_on(ring.at[pl.ds(0, chips - 1)], twin).wait_send()
    pltpu.make_async_remote_copy(
        src_ref=result.at[core],
        dst_ref=result.at[1 - core],
        send_sem=tail_send.at[1],
        recv_sem=tail_recv.at[1],
        device_id={"sample": twin},
        device_id_type=MESH,
    ).wait_recv()
    share.wait_send()
    out[:, :piece_width] = result[0]
    out[:, piece_width:] = result[1][:, : classes - piece_width]


def kernel_shards(
    patches,
    patch_weight,
    cls_token,
    pos_embed,
    ln1_gain,
    ln1_bias,
    w_query,
    w_key,
    w_value,
    w_out,
    lnf_gain,
    lnf_bias,
    head_w,
    head_bias,
):
    count = lax.axis_size("sample")
    images, rows, depth = patches.shape
    width = patch_weight.shape[2]
    inner = w_query.shape[2]
    heads = inner // HEAD_DIM
    pairs = heads * images
    chips = count // 2
    classes = head_w.shape[2]
    piece_width = pl.cdiv(classes, 256) * 128
    padded = pl.cdiv(depth, TILE_ROWS) * TILE_ROWS
    tall = FOLD_PARTS * TILE_ROWS
    features = pl.cdiv(padded + pos_embed.shape[1] + 3, tall) * tall
    far = pl.BlockSpec(memory_space=pl.ANY)
    dma = pltpu.SemaphoreType.DMA
    f32, bf16 = jnp.float32, jnp.bfloat16
    class_rows = jnp.swapaxes(head_w, 1, 2)
    given = (
        patches,
        cls_token,
        pos_embed,
        ln1_gain,
        ln1_bias,
        patch_weight,
        w_query,
        w_key,
        w_value,
        w_out,
        class_rows,
        lnf_gain,
        lnf_bias,
        head_bias,
    )
    held = [
        pltpu.VMEM(a.shape[1:] if place and a.ndim == 3 else a.shape, a.dtype)
        for place, a in enumerate(given)
    ]
    return pl.pallas_call(
        functools.partial(whole_kernel, count, heads),
        out_shape=pltpu.VMEM((images, classes), f32),
        in_specs=[far] * len(given),
        out_specs=pl.BlockSpec(memory_space=pltpu.VMEM),
        scratch_shapes=[
            *held,
            pltpu.VMEM((count, padded, images * rows), bf16),
            pltpu.VMEM((2 * heads + features, width), bf16),
            pltpu.VMEM((features, width), bf16),
            pltpu.VMEM((padded + 2 * heads + TILE_ROWS, features), bf16),
            pltpu.VMEM((features, inner), bf16),
            pltpu.VMEM((TILE_ROWS, inner), f32),
            pltpu.VMEM((heads, 128), f32),
            pltpu.VMEM((2 * heads, 2 * images * rows), f32),
            pltpu.VMEM((pairs, features), f32),
            pltpu.VMEM((pairs, 128), f32),
            pltpu.VMEM((pairs, 128), f32),
            pltpu.VMEM((2, images, piece_width), f32),
            pltpu.VMEM((images, piece_width), f32),
            pltpu.VMEM((chips, images, piece_width), f32),
            pltpu.VMEM((2, images, piece_width), f32),
            dma((len(given),)),
            dma((chips, PIECES)),
            dma((chips,)),
            dma((PIECES + 1,)),
            pltpu.SemaphoreType.REGULAR((LINE - 2,)),
            dma((3,)),
            dma((3,)),
        ],
        compiler_params=pltpu.CompilerParams(
            collective_id=0, has_side_effects=True, vmem_limit_bytes=60 << 20
        ),
    )(*given)


def takes_kernel(mesh, patches):
    count = mesh.shape["sample"]
    rows = patches.shape[1] // count
    images = patches.shape[0] // mesh.shape["group"]
    return count == PLANE * LINE and rows % TILE_ROWS == 0 and images * rows == 128


def solution(mesh):
    placed = (
        P("group", "sample", None),
        P("sample", None, None),
        P("sample", None),
        P("sample", None, None),
        P("sample", None),
        P("sample", None),
        P("sample", None, None),
        P("sample", None, None),
        P("sample", None, None),
        P("sample", None, None),
        P("sample", None),
        P("sample", None),
        P("sample", None, None),
        P("sample", None),
    )

    def run(*arrays):
        step = kernel_shards if takes_kernel(mesh, arrays[0]) else shards
        return jax.shard_map(
            step, mesh=mesh, in_specs=placed, out_specs=P("group", None), check_vma=False
        )(*arrays)

    return run
```

```python
import functools
import math

import jax
import jax.numpy as jnp
from jax import lax
from jax.experimental import pallas as pl
from jax.experimental.pallas import tpu as pltpu
from jax.sharding import PartitionSpec as P

HEAD_DIM = 80


epsilon = 1e-06


def combined_all(part, axis, combine):
    gathered = jax.tree.map(lambda a: lax.all_gather(a, axis), part)

    def take(source):
        return jax.tree.map(lambda a: lax.dynamic_index_in_dim(a, source, 0, False), gathered)

    return lax.fori_loop(
        1, lax.axis_size(axis), lambda source, state: combine(state, take(source)), take(0)
    )


def layer_norm(values, gain, shift):
    center = values - jnp.mean(values, axis=-1, keepdims=True)
    spread = jnp.mean(center * center, axis=-1, keepdims=True)
    return center * lax.rsqrt(spread + epsilon) * gain + shift


def shards(
    patches,
    patch_weight,
    cls_token,
    pos_embed,
    ln1_gain,
    ln1_bias,
    w_query,
    w_key,
    w_value,
    w_out,
    lnf_gain,
    lnf_bias,
    head_w,
    head_bias,
):
    embed_weight = patch_weight[0]
    position = pos_embed[0]
    gain_first = ln1_gain[0]
    bias_first = ln1_bias[0]
    query_weight = w_query[0]
    pair_weight = jnp.concatenate([w_key[0], w_value[0]], axis=1)
    out_weight = w_out[0]
    width = embed_weight.shape[1]
    inner = query_weight.shape[1]
    head_count = inner // HEAD_DIM
    leading = cls_token[0].astype(jnp.float32) + position[0].astype(jnp.float32)
    lead_norm = layer_norm(leading, gain_first, bias_first).astype(jnp.bfloat16)
    lead_pair = jnp.dot(lead_norm[None], pair_weight, preferred_element_type=jnp.float32).astype(
        jnp.bfloat16
    )
    query = jnp.dot(lead_norm[None], query_weight, preferred_element_type=jnp.float32).astype(
        jnp.bfloat16
    )
    query = query.reshape(head_count, HEAD_DIM)
    portion = lax.all_gather(patches, "sample", axis=1, tiled=True)
    image_count = portion.shape[0]
    row_count = portion.shape[1]
    flat = portion.reshape(-1, portion.shape[2])
    tokens = jnp.dot(flat, embed_weight, preferred_element_type=jnp.float32).reshape(
        image_count, row_count, width
    )
    placed = lax.dynamic_slice_in_dim(position, 1, row_count, 0)
    tokens = tokens + placed.astype(jnp.float32)[None]
    normed = layer_norm(tokens, gain_first, bias_first).astype(jnp.bfloat16)
    paired = jnp.dot(normed.reshape(-1, width), pair_weight, preferred_element_type=jnp.float32)
    key_values = paired.astype(jnp.bfloat16).reshape(image_count, row_count, 2 * inner)
    image_count = key_values.shape[0]
    lead_rows = jnp.broadcast_to(lead_pair[None], (image_count, 1, 2 * inner))
    full_rows = jnp.concatenate([lead_rows, key_values], axis=1)
    key_rows = full_rows[:, :, :inner].reshape(image_count, -1, head_count, HEAD_DIM)
    value_rows = full_rows[:, :, inner:].reshape(image_count, -1, head_count, HEAD_DIM)
    scores = jnp.einsum(
        "hd,ithd->iht", query, key_rows, preferred_element_type=jnp.float32
    ) / math.sqrt(HEAD_DIM)
    attention = jax.nn.softmax(scores, axis=-1).astype(jnp.bfloat16)
    mixed = jnp.einsum("iht,ithd->ihd", attention, value_rows, preferred_element_type=jnp.float32)
    mixed = mixed.astype(jnp.bfloat16).reshape(image_count, inner)
    hidden = leading[None] + jnp.dot(mixed, out_weight, preferred_element_type=jnp.float32)
    final = layer_norm(hidden, lnf_gain[0], lnf_bias[0]).astype(jnp.bfloat16)
    logits = jnp.dot(final, head_w[0], preferred_element_type=jnp.float32) + head_bias[0]
    logp = jax.nn.log_softmax(logits, axis=-1)
    count = lax.axis_size("sample")

    def combine(earlier, later):
        highest = jnp.maximum(earlier[0], later[0])
        summed = earlier[1] * jnp.exp(earlier[0] - highest) + later[1] * jnp.exp(later[0] - highest)
        return (highest, summed)

    peak, total = combined_all((logp, jnp.ones_like(logp)), "sample", combine)
    return peak + jnp.log(total) - math.log(count)


MESH = pl.DeviceIdType.MESH
PLANE = 4
LINE = 4
TILE_ROWS = 16
LOWEST = -1e30
GRAM_PARTS = 2
FOLD_PARTS = 3


def split_in_two(values):
    high = values.astype(jnp.bfloat16)
    low = (values - high.astype(jnp.float32)).astype(jnp.bfloat16)
    return jnp.concatenate([high, low], axis=0)


PIECES = 4
SENDS = (
    (
        (1,1,0,1,3), (0,0,0,1,3), (1,1,0,1,1), (0,0,0,1,0), (0,0,0,1,2), (1,1,0,1,2), (0,2,0,1,0),
        (0,2,0,1,1), (0,2,0,1,2), (0,2,0,1,3), (2,1,0,1,1), (2,1,0,1,0), (2,1,0,1,2), (0,2,0,0,3),
        (0,0,1,1,0), (0,2,1,1,0), (0,2,0,0,0), (0,0,1,1,2), (0,2,1,1,2), (1,1,0,1,0), (1,1,0,0,2),
        (0,2,0,0,2), (0,0,1,1,3), (0,2,1,1,3), (0,2,1,1,1), (0,0,0,1,1), (0,2,1,0,0), (0,0,2,1,0),
        (0,2,2,1,0), (0,2,1,0,2), (0,2,1,0,3), (0,2,2,1,1), (0,0,2,1,2), (0,2,2,1,2), (0,0,3,1,3),
        (0,2,3,1,3), (0,0,2,1,3), (0,2,2,1,3), (3,1,0,0,1), (0,2,0,0,1), (0,2,1,0,1), (0,2,2,0,0),
        (0,0,3,1,1), (0,2,3,1,1), (0,0,3,1,0), (0,2,3,1,0), (0,2,2,0,2), (0,2,2,0,1), (0,0,3,1,2),
        (0,2,3,1,2), (0,2,3,0,3), (0,2,2,0,3), (0,2,3,0,1), (0,2,3,0,0), (0,2,3,0,2),
    ),
    (
        (1,0,1,1,3), (0,1,1,1,0), (1,0,1,1,0), (2,1,1,1,2), (1,0,1,1,2), (2,1,1,1,0), (0,1,1,1,2),
        (1,0,1,1,1), (0,1,1,1,3), (0,1,1,1,1), (1,2,1,1,0), (1,2,1,1,1), (1,2,1,1,2), (1,2,1,1,3),
        (3,1,1,1,1), (3,1,1,1,3), (1,0,0,1,3), (2,1,0,1,3), (1,2,0,1,3), (2,1,1,0,3), (1,2,1,0,3),
        (2,1,1,1,3), (1,0,0,1,1), (1,2,0,1,1), (1,2,1,0,0), (1,0,2,1,0), (0,1,2,1,0), (2,1,1,1,1),
        (1,2,2,1,0), (1,2,0,1,2), (1,2,1,0,2), (0,1,2,1,2), (1,0,2,1,2), (1,2,2,1,2), (0,1,1,0,1),
        (2,1,1,0,1), (1,2,1,0,1), (1,0,2,1,1), (1,2,2,1,1), (1,2,0,0,3), (1,0,3,1,1), (0,1,3,1,1),
        (1,2,3,1,1), (1,2,0,0,1), (1,0,0,1,0), (1,2,0,1,0), (1,0,3,1,0), (0,1,3,1,0), (1,2,3,1,0),
        (1,2,2,0,0), (1,2,0,0,2), (1,0,3,1,2), (0,1,3,1,2), (1,2,3,1,2), (1,2,2,0,2), (1,2,2,0,1),
        (1,2,2,0,3), (1,2,3,0,1), (1,0,3,1,3), (1,2,3,1,3), (1,2,0,0,0), (1,2,2,1,3), (1,2,3,0,0),
        (1,2,3,0,2), (1,2,3,0,3),
    ),
    (
        (2,0,2,1,2), (2,0,2,1,3), (2,0,2,1,0), (3,1,2,1,2), (1,1,2,1,0), (3,1,2,1,0), (1,1,2,1,2),
        (1,1,2,1,1), (2,0,2,1,1), (3,1,2,1,3), (3,1,2,1,1), (2,2,2,1,0), (2,2,2,1,1), (2,2,2,1,2),
        (2,2,2,1,3), (0,1,2,1,1), (0,1,2,1,3), (3,1,1,1,2), (2,0,1,1,2), (2,2,1,1,2), (3,1,1,1,0),
        (2,0,1,1,0), (2,2,1,1,0), (2,2,2,0,2), (2,0,3,1,1), (2,2,3,1,1), (1,1,2,0,3), (2,2,2,0,3),
        (2,0,0,1,1), (3,1,0,1,1), (2,2,0,1,1), (2,0,3,1,3), (1,1,3,1,3), (2,2,3,1,3), (2,2,2,0,0),
        (2,0,0,1,0), (3,1,0,1,0), (2,2,0,1,0), (1,1,2,1,3), (2,2,3,1,2), (0,1,2,0,1), (2,2,2,0,1),
        (3,1,0,1,2), (2,0,0,1,2), (2,2,0,1,2), (2,2,1,0,2), (2,2,1,0,0), (2,2,3,0,1), (2,0,0,1,3),
        (3,1,0,1,3), (2,2,0,1,3), (2,2,1,0,3), (2,2,0,0,1), (2,2,1,1,3), (2,2,3,0,3), (2,0,3,1,0),
        (2,2,3,1,0), (2,2,1,1,1), (2,2,0,0,0), (2,2,3,0,2), (2,2,1,0,1), (2,2,0,0,2), (2,2,0,0,3),
        (2,2,3,0,0),
    ),
    (
        (3,0,3,1,1), (2,1,3,1,1), (3,0,3,1,0), (2,1,3,1,3), (3,0,3,1,2), (2,1,3,1,2), (3,0,3,1,3),
        (3,2,3,1,0), (3,2,3,1,1), (3,2,3,1,2), (3,2,3,1,3), (1,1,3,1,1), (1,1,3,1,0), (1,1,3,1,2),
        (0,1,3,1,3), (3,0,2,1,2), (3,2,2,1,2), (3,2,3,0,1), (3,0,2,1,0), (3,2,2,1,0), (3,2,3,0,0),
        (3,0,2,1,3), (3,2,2,1,3), (2,1,3,1,0), (2,1,3,0,2), (3,2,3,0,2), (3,0,2,1,1), (3,2,2,1,1),
        (3,2,3,0,3), (3,0,1,1,1), (3,2,1,1,1), (3,2,2,0,2), (3,0,1,1,3), (3,2,1,1,3), (3,2,2,0,0),
        (3,0,1,1,2), (3,2,1,1,2), (3,0,1,1,0), (3,2,1,1,0), (3,2,2,0,3), (3,2,0,1,1), (3,2,2,0,1),
        (3,0,0,1,0), (3,2,0,1,0), (3,2,1,0,1), (3,0,0,1,2), (3,2,0,1,2), (3,2,1,0,3), (3,0,0,1,3),
        (3,2,0,1,3), (3,2,1,0,2), (3,2,1,0,0), (3,2,0,0,0), (3,2,0,0,2), (3,2,0,0,3), (3,2,0,0,1),
    ),
)
EVENTS = (
    (
        ((-1,0,0,0,10),), (), (), ((-2,2,0,10,3),), (), (), ((-2,3,0,13,0),(0,0,3,13,1)),
        ((1,1,0,14,2),(0,0,0,16,1)), ((1,1,2,17,2),(0,0,2,19,3),(1,1,3,22,2)), ((1,1,1,24,1),),
        ((1,0,0,25,2),),
        ((2,1,0,27,2),(1,0,2,29,1),(1,0,3,30,1),(2,1,1,31,1),(2,1,2,32,2),(3,1,3,34,2),(2,1,3,36,2)),
        ((0,0,1,38,2),(1,0,1,40,1),(2,0,0,41,1),(3,1,1,42,2)), ((3,1,0,44,2),),
        ((2,0,2,46,1),(2,0,1,47,1),(3,1,2,48,2),(3,0,3,50,1)), (), ((2,0,3,51,1),), (), ((3,0,1,52,1),), (),
        ((3,0,0,53,1),), ((3,0,2,54,1),),
    ),
    (
        ((-1,0,0,0,14),), (), (), (), ((-2,3,0,14,2),), (), ((0,1,3,16,3),(1,0,3,19,2)),
        ((0,1,1,21,3),(1,0,0,24,1),(2,1,0,25,4),(0,1,2,29,1)), ((1,0,2,30,1),(2,1,2,31,3)),
        ((1,0,1,34,3),(2,1,1,37,2)), ((0,0,3,39,1),(3,1,1,40,3),(0,0,1,43,1)),
        ((0,1,0,44,2),(3,1,0,46,3),(2,0,0,49,1),(0,0,2,50,1)), ((3,1,2,51,3),(2,0,2,54,1),(2,0,1,55,1)),
        ((2,0,3,56,1),(3,0,1,57,1),(3,1,3,58,2)), ((0,0,0,60,1),(2,1,3,61,1),(3,0,0,62,1)), (),
        ((3,0,2,63,1),), (), ((3,0,3,64,1),), (), (), (),
    ),
    (
        ((-1,0,0,0,15),), ((-2,0,0,15,2),), (), (), (), ((1,1,2,17,3),), ((1,1,0,20,3),(2,0,2,23,1)),
        ((3,1,1,24,2),(2,0,3,26,2)), ((0,1,1,28,3),(3,1,3,31,3),(2,0,0,34,1),(0,1,0,35,3)),
        ((3,1,2,38,2),(2,0,1,40,2),(0,1,2,42,3),(1,0,2,45,1)), ((1,0,0,46,1),(3,0,1,47,1),(0,1,3,48,3)),
        ((1,0,3,51,1),(0,0,1,52,1)), ((1,1,3,53,1),(3,0,3,54,1),(3,1,0,55,2)),
        ((1,1,1,57,1),(0,0,0,58,1),(3,0,2,59,1),(1,0,1,60,1),(0,0,2,61,1)), ((0,0,3,62,1),), (), (), (),
        ((3,0,0,63,1),), (), (), (),
    ),
    (
        ((-1,0,0,0,11),), ((-2,1,0,11,3),(-2,0,0,14,1)), (), (), (), ((2,1,2,15,2),),
        ((3,0,1,17,1),(2,1,0,18,2)), ((3,0,0,20,1),(2,1,3,21,2)), ((3,0,2,23,3),(2,1,1,26,2)),
        ((3,0,3,28,1),(1,1,1,29,2),(2,0,2,31,1)), ((1,1,3,32,2),(2,0,0,34,1),(1,1,2,35,2)),
        ((1,1,0,37,2),(2,0,3,39,1)), ((0,1,1,40,1),(2,0,1,41,1),(0,1,0,42,2)), ((1,0,1,44,1),(0,1,2,45,2)),
        ((1,0,3,47,1),(0,1,3,48,2)), (), ((1,0,2,50,1),(1,0,0,51,1)), (), ((0,0,0,52,1),), (),
        ((0,0,2,53,1),), ((0,0,3,54,1),(0,0,1,55,1)),
    ),
)
ORDER = (13869401, 13924435, 12664421, 575407)


def contract_last(left, right):
    return lax.dot_general(
        left, right, (((1,), (1,)), ((), ())), preferred_element_type=jnp.float32
    )


def whole_kernel(
    count,
    heads,
    patches,
    cls_token,
    pos_embed,
    ln1_gain,
    ln1_bias,
    patch_weight,
    w_query,
    w_key,
    w_value,
    w_out,
    head_w,
    lnf_gain,
    lnf_bias,
    head_bias,
    out,
    own_patches,
    cls_row,
    position,
    gain_row,
    bias_row,
    embed,
    query_w,
    key_w,
    value_w,
    out_w,
    class_w,
    last_gain,
    last_bias,
    class_bias,
    slots,
    basis,
    scaled,
    form,
    folded,
    ends,
    constants,
    kept,
    gathered,
    peak,
    total,
    part,
    from_pair,
    ring,
    result,
    load_sem,
    recv_sem,
    twin_sem,
    sent_sem,
    known_sem,
    tail_send,
    tail_recv,
):
    f32, bf16 = jnp.float32, jnp.bfloat16
    me = lax.axis_index("sample")
    core = me % 2
    side = (me // 2) % 2
    chip = me // 2
    chips = count // 2
    plane = me // PLANE
    images, rows, depth = own_patches.shape
    padded = slots.shape[1]
    lanes = slots.shape[2]
    tiles = padded // TILE_ROWS
    cuts = tuple(TILE_ROWS * (tiles * place // PIECES) for place in range(PIECES + 1))
    width = embed.shape[1]
    inner = query_w.shape[1]
    head_dim = inner // heads
    pairs = heads * images
    spots = basis.shape[0] - 2 * heads - padded
    held_rows = position.shape[0]

    loads = []
    for index, (source, target) in enumerate(
        (
            (patches, own_patches),
            (pos_embed.at[0], position),
            (cls_token, cls_row),
            (ln1_gain, gain_row),
            (ln1_bias, bias_row),
            (patch_weight.at[0], embed),
            (w_query.at[0], query_w),
            (w_key.at[0], key_w),
            (w_value.at[0], value_w),
            (w_out.at[0], out_w),
            (head_w.at[0], class_w),
            (lnf_gain, last_gain),
            (lnf_bias, last_bias),
            (head_bias, class_bias),
        )
    ):
        loads.append(pltpu.make_async_copy(source, target, load_sem.at[index]))
    for load in loads[:5]:
        load.start()

    twin = me + 1 - 2 * core
    beside = plane * PLANE + (1 - side) * 2 + core
    here = tuple(lax.convert_element_type(plane == place, jnp.int32) for place in range(LINE))
    line_of = tuple(
        (place * PLANE + (1 - side) * 2 + core, place * PLANE + side * 2 + core)
        for place in range(LINE)
    )

    barrier = pltpu.get_barrier_semaphore()

    def greet(target):
        pl.semaphore_signal(barrier, inc=1, device_id={"sample": target}, device_id_type=MESH)

    greet(twin)
    greet(beside)

    @pl.when(plane > 0)
    def _():
        greet(me - PLANE)

    @pl.when(plane < LINE - 1)
    def _():
        greet(me + PLANE)

    loads[0].wait()
    for load in loads[5:7]:
        load.start()
    eye = (
        lax.broadcasted_iota(jnp.int32, (padded, depth), 0)
        == lax.broadcasted_iota(jnp.int32, (padded, depth), 1)
    ).astype(bf16)
    flat = own_patches[...].reshape(images * rows, depth)
    slots[me] = contract_last(eye, flat).astype(bf16)
    pl.semaphore_wait(barrier, LINE - here[0] - here[LINE - 1])

    def passing(ref, target, sent_by, got_by):
        return pltpu.make_async_remote_copy(
            src_ref=ref,
            dst_ref=ref,
            send_sem=sent_by,
            recv_sem=got_by,
            device_id={"sample": target},
            device_id_type=MESH,
        )

    def rows_of(part_of):
        return pl.ds(cuts[part_of], cuts[part_of + 1] - cuts[part_of])

    def sent(place, slot):
        to, aside, origin, own, part_of = SENDS[place][slot]
        inside = aside // 2
        source = line_of[origin][own]
        got_by = twin_sem.at[source // 2] if inside else recv_sem.at[source // 2, part_of]
        target = twin if inside else line_of[to][aside]
        ref = slots.at[source, rows_of(part_of)]
        return passing(ref, target, sent_sem.at[PIECES if inside else part_of], got_by)

    def got(source, part_of):
        ref = slots.at[source, rows_of(part_of)]
        passing(ref, twin, sent_sem.at[0], recv_sem.at[source // 2, part_of]).wait_recv()

    def got_from_twin(base):
        ref = slots.at[base + 1 - core]
        passing(ref, twin, sent_sem.at[0], twin_sem.at[base // 2]).wait_recv()

    def all_sent(place):
        for part_of in range(PIECES):
            number = sum(1 for entry in SENDS[place] if entry[1] < 2 and entry[4] == part_of)
            ref = slots.at[pl.ds(0, number), rows_of(part_of)]
            passing(ref, twin, sent_sem.at[part_of], twin_sem.at[0]).wait_send()
        ref = slots.at[pl.ds(0, chips)]
        passing(ref, twin, sent_sem.at[PIECES], twin_sem.at[0]).wait_send()

    def tell(target, far):
        pl.semaphore_signal(
            known_sem.at[far], inc=1, device_id={"sample": target}, device_id_type=MESH
        )

    def learn(place, entered):
        pl.semaphore_wait(known_sem.at[abs(entered - place) - 2], 1)
        if place == 1 and entered == 3:
            tell(me - PLANE, 1)
        if place == 2 and entered == 0:
            tell(me + PLANE, 1)

    for place in (1, 2):

        @pl.when(plane == place)
        def _(place=place):
            tell(me - PLANE, 0)
            tell(me + PLANE, 0)

    def events(group):
        for place in range(LINE):
            entries = EVENTS[place][group]
            if entries:

                @pl.when(plane == place)
                def _(place=place, entries=entries):
                    for origin, own, part_of, low, number in entries:
                        if origin == -2:
                            learn(place, own)
                        if origin >= 0:
                            got(line_of[origin][own], part_of)
                        for slot in range(low, low + number):
                            sent(place, slot).start()

    events(0)
    for load in loads[7:]:
        load.start()

    for index in (1, 2, 3, 4):
        loads[index].wait()
    events(1)
    gain = gain_row[...]
    bias = bias_row[...]
    leading = cls_row[...].astype(f32) + position[0:1, :].astype(f32)
    lead = jnp.broadcast_to(layer_norm(leading, gain, bias), (TILE_ROWS, width)).astype(bf16)
    lead_row = lead[:1].astype(f32)

    events(2)
    placed = position[...].astype(f32)
    placed = placed - jnp.mean(placed, axis=1, keepdims=True)
    blank = jnp.zeros((spots - held_rows, width), f32)
    top = 2 * heads
    placed = jnp.concatenate([placed, blank], axis=0)
    basis[top + padded :, :] = placed.astype(bf16)
    bias_high = bias.astype(bf16).astype(f32)
    ending = jnp.concatenate([blank[3:], bias_high, bias - bias_high, lead_row], axis=0)
    ending = jnp.concatenate([jnp.zeros((held_rows, width), f32), ending], axis=0)
    scaled[padded:, :] = (placed * gain + ending).astype(bf16)
    weight = jnp.broadcast_to(jnp.sum(placed * placed, axis=1, keepdims=True), (spots, 128))
    weight = jnp.concatenate([weight, jnp.zeros((-spots % 128, 128), f32)], axis=0)
    weight = jnp.transpose(weight)[:1, :spots]

    loads[5].wait()
    table = embed[...].astype(f32)
    table = table - jnp.mean(table, axis=1, keepdims=True)
    table = jnp.concatenate([table, jnp.zeros((padded - depth, width), f32)], axis=0)
    basis[top : top + padded, :] = table.astype(bf16)
    scaled[:padded, :] = (table * gain).astype(bf16)

    events(3)
    loads[6].wait()
    query = jnp.dot(lead, query_w[...], preferred_element_type=f32)[:1]
    head_row = lax.broadcasted_iota(jnp.int32, (TILE_ROWS, inner), 0)
    column = lax.broadcasted_iota(jnp.int32, (TILE_ROWS, inner), 1)
    own_head = (column >= head_row * head_dim) & (column < (head_row + 1) * head_dim)
    spread = jnp.where(own_head, jnp.broadcast_to(query, (TILE_ROWS, inner)), 0.0).astype(bf16)
    events(4)
    loads[7].wait()
    turned = contract_last(spread, key_w[...])[:heads] * (1.0 / math.sqrt(head_dim))
    first = jnp.sum(turned * lead_row, axis=1, keepdims=True)
    level = jnp.sum(turned * bias, axis=1, keepdims=True)
    constants[...] = jnp.broadcast_to(level, constants.shape)
    basis[:top, :] = split_in_two(turned * gain)

    features = padded + spots
    for part_of in range(GRAM_PARTS):
        events(5 + part_of)
        low = 256 * (pl.cdiv(features, 256) * part_of // GRAM_PARTS)
        high = min(features, 256 * (pl.cdiv(features, 256) * (part_of + 1) // GRAM_PARTS))
        square = contract_last(basis[: top + padded, :], basis[top + low : top + high, :])
        place = low + lax.broadcasted_iota(jnp.int32, (padded, high - low), 1)
        form[top : top + padded, low:high] = jnp.where(
            place < padded, square[top:], 2.0 * square[top:]
        ).astype(bf16)
        form[:top, low:high] = split_in_two(square[:heads] + square[heads:top])
    sizes = jnp.concatenate([jnp.zeros((1, padded), f32), weight], axis=1)
    sizes_high = sizes.astype(bf16).astype(f32)
    sizes = jnp.concatenate(
        [sizes_high, sizes - sizes_high, jnp.zeros((TILE_ROWS - 2, padded + spots), f32)], axis=0
    )
    form[top + padded :, :] = sizes.astype(bf16)

    loads[8].wait()
    first = jnp.broadcast_to(first[None], (images, heads, 1)).reshape(pairs, 1)
    peak[...] = jnp.broadcast_to(first, peak.shape)
    total[...] = jnp.ones(total.shape, f32)
    gathered[...] = jnp.zeros(gathered.shape, f32)

    cells = 2 * lanes
    lane = lax.broadcasted_iota(jnp.int32, (pairs, cells), 1)
    row_image = lax.broadcasted_iota(jnp.int32, (pairs, cells), 0) // heads
    same = (lane % lanes) // rows == row_image
    spot_row = lax.broadcasted_iota(jnp.int32, (spots, cells), 0)
    spot_lane = lax.broadcasted_iota(jnp.int32, (spots, cells), 1)
    spot_at = spot_row - 1 - (spot_lane // lanes) * rows - spot_lane % rows

    order = sum(mine * packed for mine, packed in zip(here, ORDER, strict=True))
    first_step = 5 + GRAM_PARTS
    fold_rows = scaled.shape[0] // FOLD_PARTS

    def base_of(turn):
        code = (order >> (3 * turn)) % 8
        where, own = code // 2, code % 2
        return where * PLANE + 2 * (side * own + (1 - side) * (1 - own))

    def block_of(base):
        block = jnp.concatenate([slots[base], slots[base + 1]], axis=1)
        spot = jnp.where(spot_at == base * rows, 1.0, 0.0).astype(bf16)
        return jnp.concatenate([block, spot], axis=0)

    def front(base):
        block = block_of(base)
        image = jnp.dot(form[...], block, preferred_element_type=f32)
        norm = jnp.sum(
            image[top : top + padded] * block[:padded].astype(f32), axis=0, keepdims=True
        )
        tail = top + padded
        norm = norm + image[tail : tail + 1] + image[tail + 1 : tail + 2]
        rate = lax.rsqrt(norm * (1.0 / width) + epsilon)
        scores = image[:heads] + image[heads:top]
        kept[:heads, :] = scores * rate + constants[:, :1]
        kept[heads:, :] = jnp.broadcast_to(rate, (heads, cells))

    def back(base, scores, rate):
        block = block_of(base)
        scores = jnp.broadcast_to(scores[None], (images, heads, cells)).reshape(pairs, cells)
        scores = jnp.where(same, scores, LOWEST)
        before = peak[:, :1]
        now = jnp.maximum(before, jnp.max(scores, axis=1, keepdims=True))
        shrink = jnp.exp(before - now)
        chance = jnp.where(same, jnp.exp(scores - now), 0.0)
        peak[...] = jnp.broadcast_to(now, peak.shape)
        total[...] = total[...] * shrink + jnp.sum(chance, axis=1, keepdims=True)
        gathered[...] = gathered[...] * shrink + contract_last((chance * rate).astype(bf16), block)

    def fold(part_of):
        low = pl.multiple_of(part_of * fold_rows, TILE_ROWS)
        product = jnp.dot(
            scaled[pl.ds(low, fold_rows), :], value_w[...], preferred_element_type=f32
        )
        folded[pl.ds(low, fold_rows), :] = product.astype(bf16)
        ends[...] = product[fold_rows - ends.shape[0] :]

    def chip_step(turn, carry):
        for index in range(1, 2 * LINE):
            pl.when(turn == index)(functools.partial(events, first_step + 2 * index))
        base = base_of(turn)
        got_from_twin(base)
        scores = kept[:heads, :]
        rate = kept[heads : heads + 1, :]
        back(base_of(turn - 1), scores, rate)
        front(base)

        for index in range(1, 2 * LINE - 1):
            pl.when(turn == index)(functools.partial(events, first_step + 2 * index + 1))

        @pl.when(turn < FOLD_PARTS)
        def _():
            fold(turn)

        return carry

    events(first_step)
    got_from_twin(base_of(0))
    front(base_of(0))
    events(first_step + 1)
    fold(0)
    lax.fori_loop(1, 2 * LINE, chip_step, 0)
    back(base_of(2 * LINE - 1), kept[:heads, :], kept[heads : heads + 1, :])

    last = ends.shape[0]
    plain = ends[last - 3 : last - 2, :] + ends[last - 2 : last - 1, :]
    lead_value = ends[last - 1 :, :]
    values = jnp.dot(
        split_in_two(gathered[...]), folded[...], preferred_element_type=f32
    )
    share = 1.0 / total[:, :1]
    lead_chance = jnp.exp(first - peak[:, :1]) * share
    values = (values[:pairs] + values[pairs:]) * share
    values = values + plain + (lead_value - plain) * lead_chance
    pair_head = lax.broadcasted_iota(jnp.int32, (pairs, inner), 0) % heads
    pair_column = lax.broadcasted_iota(jnp.int32, (pairs, inner), 1)
    mine_only = (pair_column >= pair_head * head_dim) & (pair_column < (pair_head + 1) * head_dim)
    values = jnp.where(mine_only, values, 0.0)
    mixed = jnp.sum(values.reshape(images, heads, inner), axis=1).astype(bf16)
    loads[9].wait()
    hidden = leading + jnp.dot(mixed, out_w[...], preferred_element_type=f32)
    for index in (10, 11, 12, 13):
        loads[index].wait()
    center = hidden - jnp.mean(hidden, axis=-1, keepdims=True)
    shift = last_bias[...]
    shift_high = shift.astype(bf16)
    shift_low = (shift - shift_high.astype(f32)).astype(bf16)
    rows_in = jnp.concatenate(
        [
            center * last_gain[...],
            shift_high.astype(f32),
            shift_low.astype(f32),
            jnp.zeros((TILE_ROWS - images - 2, width), f32),
        ],
        axis=0,
    ).astype(bf16)
    spread_out = jnp.mean(center * center, axis=-1, keepdims=True)
    products = contract_last(rows_in, class_w[...])
    moved = products[images : images + 1] + products[images + 1 : images + 2] + class_bias[...]
    logits = products[:images] * lax.rsqrt(spread_out + epsilon) + moved
    lifted = logits - jnp.max(logits, axis=-1, keepdims=True)
    logp = lifted - jnp.log(jnp.sum(jnp.exp(lifted), axis=-1, keepdims=True))

    piece_width = part.shape[2]
    classes = out.shape[1]
    part[0] = logp[:, :piece_width]
    part[1] = jnp.concatenate(
        [logp[:, piece_width:], jnp.zeros((images, 2 * piece_width - classes), f32)], axis=1
    )
    swap = pltpu.make_async_remote_copy(
        src_ref=part.at[1 - core],
        dst_ref=from_pair,
        send_sem=tail_send.at[0],
        recv_sem=tail_recv.at[0],
        device_id={"sample": twin},
        device_id_type=MESH,
    )
    swap.start()
    swap.wait_recv()
    mine = part[core]
    theirs = from_pair[...]
    high = jnp.maximum(mine, theirs)
    ring[chip] = high + jnp.log(jnp.exp(mine - high) + jnp.exp(theirs - high))

    def pass_on(ref, target):
        return passing(ref, target, tail_send.at[2], tail_recv.at[2])

    for step in range(1, chips):
        other = step - 1 + jnp.minimum(step // jnp.maximum(chip + 1, 1), 1)
        pass_on(ring.at[chip], 2 * other + core).start()
    pass_on(ring.at[pl.ds(0, chips - 1)], twin).wait_recv()
    every = ring[...]
    high = jnp.max(every, axis=0)
    result[core] = high + jnp.log(jnp.sum(jnp.exp(every - high[None]), axis=0)) - math.log(count)
    share = pltpu.make_async_remote_copy(
        src_ref=result.at[core],
        dst_ref=result.at[core],
        send_sem=tail_send.at[1],
        recv_sem=tail_recv.at[1],
        device_id={"sample": twin},
        device_id_type=MESH,
    )
    share.start()

    for place in range(LINE):

        @pl.when(plane == place)
        def _(place=place):
            all_sent(place)

    swap.wait_send()
    pass_on(ring.at[pl.ds(0, chips - 1)], twin).wait_send()
    pltpu.make_async_remote_copy(
        src_ref=result.at[core],
        dst_ref=result.at[1 - core],
        send_sem=tail_send.at[1],
        recv_sem=tail_recv.at[1],
        device_id={"sample": twin},
        device_id_type=MESH,
    ).wait_recv()
    share.wait_send()
    out[:, :piece_width] = result[0]
    out[:, piece_width:] = result[1][:, : classes - piece_width]


def kernel_shards(
    patches,
    patch_weight,
    cls_token,
    pos_embed,
    ln1_gain,
    ln1_bias,
    w_query,
    w_key,
    w_value,
    w_out,
    lnf_gain,
    lnf_bias,
    head_w,
    head_bias,
):
    count = lax.axis_size("sample")
    images, rows, depth = patches.shape
    width = patch_weight.shape[2]
    inner = w_query.shape[2]
    heads = inner // HEAD_DIM
    pairs = heads * images
    chips = count // 2
    classes = head_w.shape[2]
    piece_width = pl.cdiv(classes, 256) * 128
    padded = pl.cdiv(depth, TILE_ROWS) * TILE_ROWS
    tall = FOLD_PARTS * TILE_ROWS
    features = pl.cdiv(padded + pos_embed.shape[1] + 3, tall) * tall
    far = pl.BlockSpec(memory_space=pl.ANY)
    dma = pltpu.SemaphoreType.DMA
    f32, bf16 = jnp.float32, jnp.bfloat16
    class_rows = jnp.swapaxes(head_w, 1, 2)
    given = (
        patches,
        cls_token,
        pos_embed,
        ln1_gain,
        ln1_bias,
        patch_weight,
        w_query,
        w_key,
        w_value,
        w_out,
        class_rows,
        lnf_gain,
        lnf_bias,
        head_bias,
    )
    held = [
        pltpu.VMEM(a.shape[1:] if place and a.ndim == 3 else a.shape, a.dtype)
        for place, a in enumerate(given)
    ]
    return pl.pallas_call(
        functools.partial(whole_kernel, count, heads),
        out_shape=pltpu.VMEM((images, classes), f32),
        in_specs=[far] * len(given),
        out_specs=pl.BlockSpec(memory_space=pltpu.VMEM),
        scratch_shapes=[
            *held,
            pltpu.VMEM((count, padded, images * rows), bf16),
            pltpu.VMEM((2 * heads + features, width), bf16),
            pltpu.VMEM((features, width), bf16),
            pltpu.VMEM((padded + 2 * heads + TILE_ROWS, features), bf16),
            pltpu.VMEM((features, inner), bf16),
            pltpu.VMEM((TILE_ROWS, inner), f32),
            pltpu.VMEM((heads, 128), f32),
            pltpu.VMEM((2 * heads, 2 * images * rows), f32),
            pltpu.VMEM((pairs, features), f32),
            pltpu.VMEM((pairs, 128), f32),
            pltpu.VMEM((pairs, 128), f32),
            pltpu.VMEM((2, images, piece_width), f32),
            pltpu.VMEM((images, piece_width), f32),
            pltpu.VMEM((chips, images, piece_width), f32),
            pltpu.VMEM((2, images, piece_width), f32),
            dma((len(given),)),
            dma((chips, PIECES)),
            dma((chips,)),
            dma((PIECES + 1,)),
            pltpu.SemaphoreType.REGULAR((LINE - 2,)),
            dma((3,)),
            dma((3,)),
        ],
        compiler_params=pltpu.CompilerParams(
            collective_id=0, has_side_effects=True, vmem_limit_bytes=60 << 20
        ),
    )(*given)


def takes_kernel(mesh, patches):
    count = mesh.shape["sample"]
    rows = patches.shape[1] // count
    images = patches.shape[0] // mesh.shape["group"]
    return count == PLANE * LINE and rows % TILE_ROWS == 0 and images * rows == 128


def solution(mesh):
    placed = (
        P("group", "sample", None),
        P("sample", None, None),
        P("sample", None),
        P("sample", None, None),
        P("sample", None),
        P("sample", None),
        P("sample", None, None),
        P("sample", None, None),
        P("sample", None, None),
        P("sample", None, None),
        P("sample", None),
        P("sample", None),
        P("sample", None, None),
        P("sample", None),
    )

    def run(*arrays):
        step = kernel_shards if takes_kernel(mesh, arrays[0]) else shards
        return jax.shard_map(
            step, mesh=mesh, in_specs=placed, out_specs=P("group", None), check_vma=False
        )(*arrays)

    return run
```

```python
import functools
import math

import jax
import jax.numpy as jnp
from jax import lax
from jax.experimental import pallas as pl
from jax.experimental.pallas import tpu as pltpu
from jax.sharding import PartitionSpec as P

HEAD_DIM = 80


epsilon = 1e-06


def combined_all(part, axis, combine):
    gathered = jax.tree.map(lambda a: lax.all_gather(a, axis), part)

    def take(source):
        return jax.tree.map(lambda a: lax.dynamic_index_in_dim(a, source, 0, False), gathered)

    return lax.fori_loop(
        1, lax.axis_size(axis), lambda source, state: combine(state, take(source)), take(0)
    )


def layer_norm(values, gain, shift):
    center = values - jnp.mean(values, axis=-1, keepdims=True)
    spread = jnp.mean(center * center, axis=-1, keepdims=True)
    return center * lax.rsqrt(spread + epsilon) * gain + shift


def shards(
    patches,
    patch_weight,
    cls_token,
    pos_embed,
    ln1_gain,
    ln1_bias,
    w_query,
    w_key,
    w_value,
    w_out,
    lnf_gain,
    lnf_bias,
    head_w,
    head_bias,
):
    embed_weight = patch_weight[0]
    position = pos_embed[0]
    gain_first = ln1_gain[0]
    bias_first = ln1_bias[0]
    query_weight = w_query[0]
    pair_weight = jnp.concatenate([w_key[0], w_value[0]], axis=1)
    out_weight = w_out[0]
    width = embed_weight.shape[1]
    inner = query_weight.shape[1]
    head_count = inner // HEAD_DIM
    leading = cls_token[0].astype(jnp.float32) + position[0].astype(jnp.float32)
    lead_norm = layer_norm(leading, gain_first, bias_first).astype(jnp.bfloat16)
    lead_pair = jnp.dot(lead_norm[None], pair_weight, preferred_element_type=jnp.float32).astype(
        jnp.bfloat16
    )
    query = jnp.dot(lead_norm[None], query_weight, preferred_element_type=jnp.float32).astype(
        jnp.bfloat16
    )
    query = query.reshape(head_count, HEAD_DIM)
    portion = lax.all_gather(patches, "sample", axis=1, tiled=True)
    image_count = portion.shape[0]
    row_count = portion.shape[1]
    flat = portion.reshape(-1, portion.shape[2])
    tokens = jnp.dot(flat, embed_weight, preferred_element_type=jnp.float32).reshape(
        image_count, row_count, width
    )
    placed = lax.dynamic_slice_in_dim(position, 1, row_count, 0)
    tokens = tokens + placed.astype(jnp.float32)[None]
    normed = layer_norm(tokens, gain_first, bias_first).astype(jnp.bfloat16)
    paired = jnp.dot(normed.reshape(-1, width), pair_weight, preferred_element_type=jnp.float32)
    key_values = paired.astype(jnp.bfloat16).reshape(image_count, row_count, 2 * inner)
    image_count = key_values.shape[0]
    lead_rows = jnp.broadcast_to(lead_pair[None], (image_count, 1, 2 * inner))
    full_rows = jnp.concatenate([lead_rows, key_values], axis=1)
    key_rows = full_rows[:, :, :inner].reshape(image_count, -1, head_count, HEAD_DIM)
    value_rows = full_rows[:, :, inner:].reshape(image_count, -1, head_count, HEAD_DIM)
    scores = jnp.einsum(
        "hd,ithd->iht", query, key_rows, preferred_element_type=jnp.float32
    ) / math.sqrt(HEAD_DIM)
    attention = jax.nn.softmax(scores, axis=-1).astype(jnp.bfloat16)
    mixed = jnp.einsum("iht,ithd->ihd", attention, value_rows, preferred_element_type=jnp.float32)
    mixed = mixed.astype(jnp.bfloat16).reshape(image_count, inner)
    hidden = leading[None] + jnp.dot(mixed, out_weight, preferred_element_type=jnp.float32)
    final = layer_norm(hidden, lnf_gain[0], lnf_bias[0]).astype(jnp.bfloat16)
    logits = jnp.dot(final, head_w[0], preferred_element_type=jnp.float32) + head_bias[0]
    logp = jax.nn.log_softmax(logits, axis=-1)
    count = lax.axis_size("sample")

    def combine(earlier, later):
        highest = jnp.maximum(earlier[0], later[0])
        summed = earlier[1] * jnp.exp(earlier[0] - highest) + later[1] * jnp.exp(later[0] - highest)
        return (highest, summed)

    peak, total = combined_all((logp, jnp.ones_like(logp)), "sample", combine)
    return peak + jnp.log(total) - math.log(count)


MESH = pl.DeviceIdType.MESH
PLANE = 4
LINE = 4
TILE_ROWS = 16
LOWEST = -1e30
GRAM_PARTS = 2
FOLD_PARTS = 3


def split_in_two(values):
    high = values.astype(jnp.bfloat16)
    low = (values - high.astype(jnp.float32)).astype(jnp.bfloat16)
    return jnp.concatenate([high, low], axis=0)


PIECES = 4
SENDS = (
    (
        (1,1,0,1,3), (0,0,0,1,3), (1,1,0,1,1), (0,0,0,1,0), (0,0,0,1,2), (1,1,0,1,2), (0,2,0,1,0),
        (0,2,0,1,1), (0,2,0,1,2), (0,2,0,1,3), (2,1,0,1,1), (2,1,0,1,0), (2,1,0,1,2), (0,2,0,0,3),
        (0,0,1,1,0), (0,2,1,1,0), (0,2,0,0,0), (0,0,1,1,2), (0,2,1,1,2), (1,1,0,1,0), (1,1,0,0,2),
        (0,2,0,0,2), (0,0,1,1,3), (0,2,1,1,3), (0,2,1,1,1), (0,0,0,1,1), (0,2,1,0,0), (0,0,2,1,0),
        (0,2,2,1,0), (0,2,1,0,2), (0,2,1,0,3), (0,2,2,1,1), (0,0,2,1,2), (0,2,2,1,2), (0,0,3,1,3),
        (0,2,3,1,3), (0,0,2,1,3), (0,2,2,1,3), (3,1,0,0,1), (0,2,0,0,1), (0,2,1,0,1), (0,2,2,0,0),
        (0,0,3,1,1), (0,2,3,1,1), (0,0,3,1,0), (0,2,3,1,0), (0,2,2,0,2), (0,2,2,0,1), (0,0,3,1,2),
        (0,2,3,1,2), (0,2,3,0,3), (0,2,2,0,3), (0,2,3,0,1), (0,2,3,0,0), (0,2,3,0,2),
    ),
    (
        (1,0,1,1,3), (0,1,1,1,0), (1,0,1,1,0), (2,1,1,1,2), (1,0,1,1,2), (2,1,1,1,0), (0,1,1,1,2),
        (1,0,1,1,1), (0,1,1,1,3), (0,1,1,1,1), (1,2,1,1,0), (1,2,1,1,1), (1,2,1,1,2), (1,2,1,1,3),
        (3,1,1,1,1), (3,1,1,1,3), (1,0,0,1,3), (2,1,0,1,3), (1,2,0,1,3), (2,1,1,0,3), (1,2,1,0,3),
        (2,1,1,1,3), (1,0,0,1,1), (1,2,0,1,1), (1,2,1,0,0), (1,0,2,1,0), (0,1,2,1,0), (2,1,1,1,1),
        (1,2,2,1,0), (1,2,0,1,2), (1,2,1,0,2), (0,1,2,1,2), (1,0,2,1,2), (1,2,2,1,2), (0,1,1,0,1),
        (2,1,1,0,1), (1,2,1,0,1), (1,0,2,1,1), (1,2,2,1,1), (1,2,0,0,3), (1,0,3,1,1), (0,1,3,1,1),
        (1,2,3,1,1), (1,2,0,0,1), (1,0,0,1,0), (1,2,0,1,0), (1,0,3,1,0), (0,1,3,1,0), (1,2,3,1,0),
        (1,2,2,0,0), (1,2,0,0,2), (1,0,3,1,2), (0,1,3,1,2), (1,2,3,1,2), (1,2,2,0,2), (1,2,2,0,1),
        (1,2,2,0,3), (1,2,3,0,1), (1,0,3,1,3), (1,2,3,1,3), (1,2,0,0,0), (1,2,2,1,3), (1,2,3,0,0),
        (1,2,3,0,2), (1,2,3,0,3),
    ),
    (
        (2,0,2,1,2), (2,0,2,1,3), (2,0,2,1,0), (3,1,2,1,2), (1,1,2,1,0), (3,1,2,1,0), (1,1,2,1,2),
        (1,1,2,1,1), (2,0,2,1,1), (3,1,2,1,3), (3,1,2,1,1), (2,2,2,1,0), (2,2,2,1,1), (2,2,2,1,2),
        (2,2,2,1,3), (0,1,2,1,1), (0,1,2,1,3), (3,1,1,1,2), (2,0,1,1,2), (2,2,1,1,2), (3,1,1,1,0),
        (2,0,1,1,0), (2,2,1,1,0), (2,2,2,0,2), (2,0,3,1,1), (2,2,3,1,1), (1,1,2,0,3), (2,2,2,0,3),
        (2,0,0,1,1), (3,1,0,1,1), (2,2,0,1,1), (2,0,3,1,3), (1,1,3,1,3), (2,2,3,1,3), (2,2,2,0,0),
        (2,0,0,1,0), (3,1,0,1,0), (2,2,0,1,0), (1,1,2,1,3), (2,2,3,1,2), (0,1,2,0,1), (2,2,2,0,1),
        (3,1,0,1,2), (2,0,0,1,2), (2,2,0,1,2), (2,2,1,0,2), (2,2,1,0,0), (2,2,3,0,1), (2,0,0,1,3),
        (3,1,0,1,3), (2,2,0,1,3), (2,2,1,0,3), (2,2,0,0,1), (2,2,1,1,3), (2,2,3,0,3), (2,0,3,1,0),
        (2,2,3,1,0), (2,2,1,1,1), (2,2,0,0,0), (2,2,3,0,2), (2,2,1,0,1), (2,2,0,0,2), (2,2,0,0,3),
        (2,2,3,0,0),
    ),
    (
        (3,0,3,1,1), (2,1,3,1,1), (3,0,3,1,0), (2,1,3,1,3), (3,0,3,1,2), (2,1,3,1,2), (3,0,3,1,3),
        (3,2,3,1,0), (3,2,3,1,1), (3,2,3,1,2), (3,2,3,1,3), (1,1,3,1,1), (1,1,3,1,0), (1,1,3,1,2),
        (0,1,3,1,3), (3,0,2,1,2), (3,2,2,1,2), (3,2,3,0,1), (3,0,2,1,0), (3,2,2,1,0), (3,2,3,0,0),
        (3,0,2,1,3), (3,2,2,1,3), (2,1,3,1,0), (2,1,3,0,2), (3,2,3,0,2), (3,0,2,1,1), (3,2,2,1,1),
        (3,2,3,0,3), (3,0,1,1,1), (3,2,1,1,1), (3,2,2,0,2), (3,0,1,1,3), (3,2,1,1,3), (3,2,2,0,0),
        (3,0,1,1,2), (3,2,1,1,2), (3,0,1,1,0), (3,2,1,1,0), (3,2,2,0,3), (3,2,0,1,1), (3,2,2,0,1),
        (3,0,0,1,0), (3,2,0,1,0), (3,2,1,0,1), (3,0,0,1,2), (3,2,0,1,2), (3,2,1,0,3), (3,0,0,1,3),
        (3,2,0,1,3), (3,2,1,0,2), (3,2,1,0,0), (3,2,0,0,0), (3,2,0,0,2), (3,2,0,0,3), (3,2,0,0,1),
    ),
)
EVENTS = (
    (
        ((-1,0,0,0,10),), (), (), ((-2,2,0,10,3),), (), (), ((-2,3,0,13,0),(0,0,3,13,1)),
        ((1,1,0,14,2),(0,0,0,16,1)), ((1,1,2,17,2),(0,0,2,19,3),(1,1,3,22,2)), ((1,1,1,24,1),),
        ((1,0,0,25,2),),
        ((2,1,0,27,2),(1,0,2,29,1),(1,0,3,30,1),(2,1,1,31,1),(2,1,2,32,2),(3,1,3,34,2),(2,1,3,36,2)),
        ((0,0,1,38,2),(1,0,1,40,1),(2,0,0,41,1),(3,1,1,42,2)), ((3,1,0,44,2),),
        ((2,0,2,46,1),(2,0,1,47,1),(3,1,2,48,2),(3,0,3,50,1)), (), ((2,0,3,51,1),), (), ((3,0,1,52,1),), (),
        ((3,0,0,53,1),), ((3,0,2,54,1),),
    ),
    (
        ((-1,0,0,0,14),), (), (), (), ((-2,3,0,14,2),), (), ((0,1,3,16,3),(1,0,3,19,2)),
        ((0,1,1,21,3),(1,0,0,24,1),(2,1,0,25,4),(0,1,2,29,1)), ((1,0,2,30,1),(2,1,2,31,3)),
        ((1,0,1,34,3),(2,1,1,37,2)), ((0,0,3,39,1),(3,1,1,40,3),(0,0,1,43,1)),
        ((0,1,0,44,2),(3,1,0,46,3),(2,0,0,49,1),(0,0,2,50,1)), ((3,1,2,51,3),(2,0,2,54,1),(2,0,1,55,1)),
        ((2,0,3,56,1),(3,0,1,57,1),(3,1,3,58,2)), ((0,0,0,60,1),(2,1,3,61,1),(3,0,0,62,1)), (),
        ((3,0,2,63,1),), (), ((3,0,3,64,1),), (), (), (),
    ),
    (
        ((-1,0,0,0,15),), ((-2,0,0,15,2),), (), (), (), ((1,1,2,17,3),), ((1,1,0,20,3),(2,0,2,23,1)),
        ((3,1,1,24,2),(2,0,3,26,2)), ((0,1,1,28,3),(3,1,3,31,3),(2,0,0,34,1),(0,1,0,35,3)),
        ((3,1,2,38,2),(2,0,1,40,2),(0,1,2,42,3),(1,0,2,45,1)), ((1,0,0,46,1),(3,0,1,47,1),(0,1,3,48,3)),
        ((1,0,3,51,1),(0,0,1,52,1)), ((1,1,3,53,1),(3,0,3,54,1),(3,1,0,55,2)),
        ((1,1,1,57,1),(0,0,0,58,1),(3,0,2,59,1),(1,0,1,60,1),(0,0,2,61,1)), ((0,0,3,62,1),), (), (), (),
        ((3,0,0,63,1),), (), (), (),
    ),
    (
        ((-1,0,0,0,11),), ((-2,1,0,11,3),(-2,0,0,14,1)), (), (), (), ((2,1,2,15,2),),
        ((3,0,1,17,1),(2,1,0,18,2)), ((3,0,0,20,1),(2,1,3,21,2)), ((3,0,2,23,3),(2,1,1,26,2)),
        ((3,0,3,28,1),(1,1,1,29,2),(2,0,2,31,1)), ((1,1,3,32,2),(2,0,0,34,1),(1,1,2,35,2)),
        ((1,1,0,37,2),(2,0,3,39,1)), ((0,1,1,40,1),(2,0,1,41,1),(0,1,0,42,2)), ((1,0,1,44,1),(0,1,2,45,2)),
        ((1,0,3,47,1),(0,1,3,48,2)), (), ((1,0,2,50,1),(1,0,0,51,1)), (), ((0,0,0,52,1),), (),
        ((0,0,2,53,1),), ((0,0,3,54,1),(0,0,1,55,1)),
    ),
)
ORDER = (13869401, 13924435, 12664421, 575407)


def contract_last(left, right):
    return lax.dot_general(
        left, right, (((1,), (1,)), ((), ())), preferred_element_type=jnp.float32
    )


def whole_kernel(
    count,
    heads,
    patches,
    cls_token,
    pos_embed,
    ln1_gain,
    ln1_bias,
    patch_weight,
    w_query,
    w_key,
    w_value,
    w_out,
    head_w,
    lnf_gain,
    lnf_bias,
    head_bias,
    out,
    own_patches,
    cls_row,
    position,
    gain_row,
    bias_row,
    embed,
    query_w,
    key_w,
    value_w,
    out_w,
    class_w,
    last_gain,
    last_bias,
    class_bias,
    slots,
    basis,
    scaled,
    form,
    folded,
    ends,
    constants,
    kept,
    gathered,
    peak,
    total,
    part,
    from_pair,
    ring,
    result,
    load_sem,
    recv_sem,
    twin_sem,
    sent_sem,
    known_sem,
    tail_send,
    tail_recv,
):
    f32, bf16 = jnp.float32, jnp.bfloat16
    me = lax.axis_index("sample")
    core = me % 2
    side = (me // 2) % 2
    chip = me // 2
    chips = count // 2
    plane = me // PLANE
    images, rows, depth = own_patches.shape
    padded = slots.shape[1]
    lanes = slots.shape[2]
    tiles = padded // TILE_ROWS
    cuts = tuple(TILE_ROWS * (tiles * place // PIECES) for place in range(PIECES + 1))
    width = embed.shape[1]
    inner = query_w.shape[1]
    head_dim = inner // heads
    pairs = heads * images
    spots = basis.shape[0] - 2 * heads - padded
    held_rows = position.shape[0]

    loads = []
    for index, (source, target) in enumerate(
        (
            (patches, own_patches),
            (pos_embed.at[0], position),
            (cls_token, cls_row),
            (ln1_gain, gain_row),
            (ln1_bias, bias_row),
            (patch_weight.at[0], embed),
            (w_query.at[0], query_w),
            (w_key.at[0], key_w),
            (w_value.at[0], value_w),
            (w_out.at[0], out_w),
            (head_w.at[0], class_w),
            (lnf_gain, last_gain),
            (lnf_bias, last_bias),
            (head_bias, class_bias),
        )
    ):
        loads.append(pltpu.make_async_copy(source, target, load_sem.at[index]))
    for load in loads[:5]:
        load.start()

    twin = me + 1 - 2 * core
    beside = plane * PLANE + (1 - side) * 2 + core
    here = tuple(lax.convert_element_type(plane == place, jnp.int32) for place in range(LINE))
    line_of = tuple(
        (place * PLANE + (1 - side) * 2 + core, place * PLANE + side * 2 + core)
        for place in range(LINE)
    )

    barrier = pltpu.get_barrier_semaphore()

    def greet(target):
        pl.semaphore_signal(barrier, inc=1, device_id={"sample": target}, device_id_type=MESH)

    greet(twin)
    greet(beside)

    @pl.when(plane > 0)
    def _():
        greet(me - PLANE)

    @pl.when(plane < LINE - 1)
    def _():
        greet(me + PLANE)

    loads[0].wait()
    for load in loads[5:7]:
        load.start()
    eye = (
        lax.broadcasted_iota(jnp.int32, (padded, depth), 0)
        == lax.broadcasted_iota(jnp.int32, (padded, depth), 1)
    ).astype(bf16)
    flat = own_patches[...].reshape(images * rows, depth)
    slots[me] = contract_last(eye, flat).astype(bf16)
    pl.semaphore_wait(barrier, LINE - here[0] - here[LINE - 1])

    def passing(ref, target, sent_by, got_by):
        return pltpu.make_async_remote_copy(
            src_ref=ref,
            dst_ref=ref,
            send_sem=sent_by,
            recv_sem=got_by,
            device_id={"sample": target},
            device_id_type=MESH,
        )

    def rows_of(part_of):
        return pl.ds(cuts[part_of], cuts[part_of + 1] - cuts[part_of])

    def sent(place, slot):
        to, aside, origin, own, part_of = SENDS[place][slot]
        inside = aside // 2
        source = line_of[origin][own]
        got_by = twin_sem.at[source // 2] if inside else recv_sem.at[source // 2, part_of]
        target = twin if inside else line_of[to][aside]
        ref = slots.at[source, rows_of(part_of)]
        return passing(ref, target, sent_sem.at[PIECES if inside else part_of], got_by)

    def got(source, part_of):
        ref = slots.at[source, rows_of(part_of)]
        passing(ref, twin, sent_sem.at[0], recv_sem.at[source // 2, part_of]).wait_recv()

    def got_from_twin(base):
        ref = slots.at[base + 1 - core]
        passing(ref, twin, sent_sem.at[0], twin_sem.at[base // 2]).wait_recv()

    def all_sent(place):
        for part_of in range(PIECES):
            number = sum(1 for entry in SENDS[place] if entry[1] < 2 and entry[4] == part_of)
            ref = slots.at[pl.ds(0, number), rows_of(part_of)]
            passing(ref, twin, sent_sem.at[part_of], twin_sem.at[0]).wait_send()
        ref = slots.at[pl.ds(0, chips)]
        passing(ref, twin, sent_sem.at[PIECES], twin_sem.at[0]).wait_send()

    def tell(target, far):
        pl.semaphore_signal(
            known_sem.at[far], inc=1, device_id={"sample": target}, device_id_type=MESH
        )

    def learn(place, entered):
        pl.semaphore_wait(known_sem.at[abs(entered - place) - 2], 1)
        if place == 1 and entered == 3:
            tell(me - PLANE, 1)
        if place == 2 and entered == 0:
            tell(me + PLANE, 1)

    for place in (1, 2):

        @pl.when(plane == place)
        def _(place=place):
            tell(me - PLANE, 0)
            tell(me + PLANE, 0)

    def events_at(place, group):
        for origin, own, part_of, low, number in EVENTS[place][group]:
            if origin == -2:
                learn(place, own)
            if origin >= 0:
                got(line_of[origin][own], part_of)
            for slot in range(low, low + number):
                sent(place, slot).start()

    def narrowed(value, low, high, act, busy):
        live = [place for place in range(low, high) if busy(place)]
        if not live:
            return
        if high - low == 1:
            act(low)
            return
        middle = (low + high) // 2
        pl.when(value < middle)(lambda: narrowed(value, low, middle, act, busy))
        pl.when(value >= middle)(lambda: narrowed(value, middle, high, act, busy))

    def events(group):
        narrowed(
            plane,
            0,
            LINE,
            lambda place: events_at(place, group),
            lambda place: bool(EVENTS[place][group]),
        )

    events(0)
    for load in loads[7:]:
        load.start()

    for index in (1, 2, 3, 4):
        loads[index].wait()
    events(1)
    gain = gain_row[...]
    bias = bias_row[...]
    leading = cls_row[...].astype(f32) + position[0:1, :].astype(f32)
    lead = jnp.broadcast_to(layer_norm(leading, gain, bias), (TILE_ROWS, width)).astype(bf16)
    lead_row = lead[:1].astype(f32)

    events(2)
    placed = position[...].astype(f32)
    placed = placed - jnp.mean(placed, axis=1, keepdims=True)
    blank = jnp.zeros((spots - held_rows, width), f32)
    top = 2 * heads
    placed = jnp.concatenate([placed, blank], axis=0)
    basis[top + padded :, :] = placed.astype(bf16)
    bias_high = bias.astype(bf16).astype(f32)
    ending = jnp.concatenate([blank[3:], bias_high, bias - bias_high, lead_row], axis=0)
    ending = jnp.concatenate([jnp.zeros((held_rows, width), f32), ending], axis=0)
    scaled[padded:, :] = (placed * gain + ending).astype(bf16)
    weight = jnp.broadcast_to(jnp.sum(placed * placed, axis=1, keepdims=True), (spots, 128))
    weight = jnp.concatenate([weight, jnp.zeros((-spots % 128, 128), f32)], axis=0)
    weight = jnp.transpose(weight)[:1, :spots]

    loads[5].wait()
    table = embed[...].astype(f32)
    table = table - jnp.mean(table, axis=1, keepdims=True)
    table = jnp.concatenate([table, jnp.zeros((padded - depth, width), f32)], axis=0)
    basis[top : top + padded, :] = table.astype(bf16)
    scaled[:padded, :] = (table * gain).astype(bf16)

    events(3)
    loads[6].wait()
    query = jnp.dot(lead, query_w[...], preferred_element_type=f32)[:1]
    head_row = lax.broadcasted_iota(jnp.int32, (TILE_ROWS, inner), 0)
    column = lax.broadcasted_iota(jnp.int32, (TILE_ROWS, inner), 1)
    own_head = (column >= head_row * head_dim) & (column < (head_row + 1) * head_dim)
    spread = jnp.where(own_head, jnp.broadcast_to(query, (TILE_ROWS, inner)), 0.0).astype(bf16)
    events(4)
    loads[7].wait()
    turned = contract_last(spread, key_w[...])[:heads] * (1.0 / math.sqrt(head_dim))
    first = jnp.sum(turned * lead_row, axis=1, keepdims=True)
    level = jnp.sum(turned * bias, axis=1, keepdims=True)
    constants[...] = jnp.broadcast_to(level, constants.shape)
    basis[:top, :] = split_in_two(turned * gain)

    features = padded + spots
    for part_of in range(GRAM_PARTS):
        events(5 + part_of)
        low = 256 * (pl.cdiv(features, 256) * part_of // GRAM_PARTS)
        high = min(features, 256 * (pl.cdiv(features, 256) * (part_of + 1) // GRAM_PARTS))
        square = contract_last(basis[: top + padded, :], basis[top + low : top + high, :])
        place = low + lax.broadcasted_iota(jnp.int32, (padded, high - low), 1)
        form[top : top + padded, low:high] = jnp.where(
            place < padded, square[top:], 2.0 * square[top:]
        ).astype(bf16)
        form[:top, low:high] = split_in_two(square[:heads] + square[heads:top])
    sizes = jnp.concatenate([jnp.zeros((1, padded), f32), weight], axis=1)
    sizes_high = sizes.astype(bf16).astype(f32)
    sizes = jnp.concatenate(
        [sizes_high, sizes - sizes_high, jnp.zeros((TILE_ROWS - 2, padded + spots), f32)], axis=0
    )
    form[top + padded :, :] = sizes.astype(bf16)

    loads[8].wait()
    first = jnp.broadcast_to(first[None], (images, heads, 1)).reshape(pairs, 1)
    peak[...] = jnp.broadcast_to(first, peak.shape)
    total[...] = jnp.ones(total.shape, f32)
    gathered[...] = jnp.zeros(gathered.shape, f32)

    cells = 2 * lanes
    lane = lax.broadcasted_iota(jnp.int32, (pairs, cells), 1)
    row_image = lax.broadcasted_iota(jnp.int32, (pairs, cells), 0) // heads
    same = (lane % lanes) // rows == row_image
    spot_row = lax.broadcasted_iota(jnp.int32, (spots, cells), 0)
    spot_lane = lax.broadcasted_iota(jnp.int32, (spots, cells), 1)
    spot_at = spot_row - 1 - (spot_lane // lanes) * rows - spot_lane % rows

    order = sum(mine * packed for mine, packed in zip(here, ORDER, strict=True))
    first_step = 5 + GRAM_PARTS
    fold_rows = scaled.shape[0] // FOLD_PARTS

    def base_of(turn):
        code = (order >> (3 * turn)) % 8
        where, own = code // 2, code % 2
        return where * PLANE + 2 * (side * own + (1 - side) * (1 - own))

    def block_of(base):
        block = jnp.concatenate([slots[base], slots[base + 1]], axis=1)
        spot = jnp.where(spot_at == base * rows, 1.0, 0.0).astype(bf16)
        return jnp.concatenate([block, spot], axis=0)

    def front(base):
        block = block_of(base)
        image = jnp.dot(form[...], block, preferred_element_type=f32)
        norm = jnp.sum(
            image[top : top + padded] * block[:padded].astype(f32), axis=0, keepdims=True
        )
        tail = top + padded
        norm = norm + image[tail : tail + 1] + image[tail + 1 : tail + 2]
        rate = lax.rsqrt(norm * (1.0 / width) + epsilon)
        scores = image[:heads] + image[heads:top]
        kept[:heads, :] = scores * rate + constants[:, :1]
        kept[heads:, :] = jnp.broadcast_to(rate, (heads, cells))

    def back(base, scores, rate):
        block = block_of(base)
        scores = jnp.broadcast_to(scores[None], (images, heads, cells)).reshape(pairs, cells)
        scores = jnp.where(same, scores, LOWEST)
        before = peak[:, :1]
        now = jnp.maximum(before, jnp.max(scores, axis=1, keepdims=True))
        shrink = jnp.exp(before - now)
        chance = jnp.where(same, jnp.exp(scores - now), 0.0)
        peak[...] = jnp.broadcast_to(now, peak.shape)
        total[...] = total[...] * shrink + jnp.sum(chance, axis=1, keepdims=True)
        gathered[...] = gathered[...] * shrink + contract_last((chance * rate).astype(bf16), block)

    def fold(part_of):
        low = pl.multiple_of(part_of * fold_rows, TILE_ROWS)
        product = jnp.dot(
            scaled[pl.ds(low, fold_rows), :], value_w[...], preferred_element_type=f32
        )
        folded[pl.ds(low, fold_rows), :] = product.astype(bf16)
        ends[...] = product[fold_rows - ends.shape[0] :]

    def chip_step(turn, carry):
        narrowed(turn, 1, 2 * LINE, lambda index: events(first_step + 2 * index), lambda index: True)
        base = base_of(turn)
        got_from_twin(base)
        scores = kept[:heads, :]
        rate = kept[heads : heads + 1, :]
        back(base_of(turn - 1), scores, rate)
        front(base)

        narrowed(
            turn,
            1,
            2 * LINE,
            lambda index: events(first_step + 2 * index + 1),
            lambda index: index < 2 * LINE - 1,
        )

        @pl.when(turn < FOLD_PARTS)
        def _():
            fold(turn)

        return carry

    events(first_step)
    got_from_twin(base_of(0))
    front(base_of(0))
    events(first_step + 1)
    fold(0)
    lax.fori_loop(1, 2 * LINE, chip_step, 0)
    back(base_of(2 * LINE - 1), kept[:heads, :], kept[heads : heads + 1, :])

    last = ends.shape[0]
    plain = ends[last - 3 : last - 2, :] + ends[last - 2 : last - 1, :]
    lead_value = ends[last - 1 :, :]
    values = jnp.dot(
        split_in_two(gathered[...]), folded[...], preferred_element_type=f32
    )
    share = 1.0 / total[:, :1]
    lead_chance = jnp.exp(first - peak[:, :1]) * share
    values = (values[:pairs] + values[pairs:]) * share
    values = values + plain + (lead_value - plain) * lead_chance
    pair_head = lax.broadcasted_iota(jnp.int32, (pairs, inner), 0) % heads
    pair_column = lax.broadcasted_iota(jnp.int32, (pairs, inner), 1)
    mine_only = (pair_column >= pair_head * head_dim) & (pair_column < (pair_head + 1) * head_dim)
    values = jnp.where(mine_only, values, 0.0)
    mixed = jnp.sum(values.reshape(images, heads, inner), axis=1).astype(bf16)
    loads[9].wait()
    hidden = leading + jnp.dot(mixed, out_w[...], preferred_element_type=f32)
    for index in (10, 11, 12, 13):
        loads[index].wait()
    center = hidden - jnp.mean(hidden, axis=-1, keepdims=True)
    shift = last_bias[...]
    shift_high = shift.astype(bf16)
    shift_low = (shift - shift_high.astype(f32)).astype(bf16)
    rows_in = jnp.concatenate(
        [
            center * last_gain[...],
            shift_high.astype(f32),
            shift_low.astype(f32),
            jnp.zeros((TILE_ROWS - images - 2, width), f32),
        ],
        axis=0,
    ).astype(bf16)
    spread_out = jnp.mean(center * center, axis=-1, keepdims=True)
    products = contract_last(rows_in, class_w[...])
    moved = products[images : images + 1] + products[images + 1 : images + 2] + class_bias[...]
    logits = products[:images] * lax.rsqrt(spread_out + epsilon) + moved
    lifted = logits - jnp.max(logits, axis=-1, keepdims=True)
    logp = lifted - jnp.log(jnp.sum(jnp.exp(lifted), axis=-1, keepdims=True))

    piece_width = part.shape[2]
    classes = out.shape[1]
    part[0] = logp[:, :piece_width]
    part[1] = jnp.concatenate(
        [logp[:, piece_width:], jnp.zeros((images, 2 * piece_width - classes), f32)], axis=1
    )
    swap = pltpu.make_async_remote_copy(
        src_ref=part.at[1 - core],
        dst_ref=from_pair,
        send_sem=tail_send.at[0],
        recv_sem=tail_recv.at[0],
        device_id={"sample": twin},
        device_id_type=MESH,
    )
    swap.start()
    swap.wait_recv()
    mine = part[core]
    theirs = from_pair[...]
    high = jnp.maximum(mine, theirs)
    ring[chip] = high + jnp.log(jnp.exp(mine - high) + jnp.exp(theirs - high))

    def pass_on(ref, target):
        return passing(ref, target, tail_send.at[2], tail_recv.at[2])

    for step in range(1, chips):
        other = step - 1 + jnp.minimum(step // jnp.maximum(chip + 1, 1), 1)
        pass_on(ring.at[chip], 2 * other + core).start()
    pass_on(ring.at[pl.ds(0, chips - 1)], twin).wait_recv()
    every = ring[...]
    high = jnp.max(every, axis=0)
    result[core] = high + jnp.log(jnp.sum(jnp.exp(every - high[None]), axis=0)) - math.log(count)
    share = pltpu.make_async_remote_copy(
        src_ref=result.at[core],
        dst_ref=result.at[core],
        send_sem=tail_send.at[1],
        recv_sem=tail_recv.at[1],
        device_id={"sample": twin},
        device_id_type=MESH,
    )
    share.start()

    for place in range(LINE):

        @pl.when(plane == place)
        def _(place=place):
            all_sent(place)

    swap.wait_send()
    pass_on(ring.at[pl.ds(0, chips - 1)], twin).wait_send()
    pltpu.make_async_remote_copy(
        src_ref=result.at[core],
        dst_ref=result.at[1 - core],
        send_sem=tail_send.at[1],
        recv_sem=tail_recv.at[1],
        device_id={"sample": twin},
        device_id_type=MESH,
    ).wait_recv()
    share.wait_send()
    out[:, :piece_width] = result[0]
    out[:, piece_width:] = result[1][:, : classes - piece_width]


def kernel_shards(
    patches,
    patch_weight,
    cls_token,
    pos_embed,
    ln1_gain,
    ln1_bias,
    w_query,
    w_key,
    w_value,
    w_out,
    lnf_gain,
    lnf_bias,
    head_w,
    head_bias,
):
    count = lax.axis_size("sample")
    images, rows, depth = patches.shape
    width = patch_weight.shape[2]
    inner = w_query.shape[2]
    heads = inner // HEAD_DIM
    pairs = heads * images
    chips = count // 2
    classes = head_w.shape[2]
    piece_width = pl.cdiv(classes, 256) * 128
    padded = pl.cdiv(depth, TILE_ROWS) * TILE_ROWS
    tall = FOLD_PARTS * TILE_ROWS
    features = pl.cdiv(padded + pos_embed.shape[1] + 3, tall) * tall
    far = pl.BlockSpec(memory_space=pl.ANY)
    dma = pltpu.SemaphoreType.DMA
    f32, bf16 = jnp.float32, jnp.bfloat16
    class_rows = jnp.swapaxes(head_w, 1, 2)
    given = (
        patches,
        cls_token,
        pos_embed,
        ln1_gain,
        ln1_bias,
        patch_weight,
        w_query,
        w_key,
        w_value,
        w_out,
        class_rows,
        lnf_gain,
        lnf_bias,
        head_bias,
    )
    held = [
        pltpu.VMEM(a.shape[1:] if place and a.ndim == 3 else a.shape, a.dtype)
        for place, a in enumerate(given)
    ]
    return pl.pallas_call(
        functools.partial(whole_kernel, count, heads),
        out_shape=pltpu.VMEM((images, classes), f32),
        in_specs=[far] * len(given),
        out_specs=pl.BlockSpec(memory_space=pltpu.VMEM),
        scratch_shapes=[
            *held,
            pltpu.VMEM((count, padded, images * rows), bf16),
            pltpu.VMEM((2 * heads + features, width), bf16),
            pltpu.VMEM((features, width), bf16),
            pltpu.VMEM((padded + 2 * heads + TILE_ROWS, features), bf16),
            pltpu.VMEM((features, inner), bf16),
            pltpu.VMEM((TILE_ROWS, inner), f32),
            pltpu.VMEM((heads, 128), f32),
            pltpu.VMEM((2 * heads, 2 * images * rows), f32),
            pltpu.VMEM((pairs, features), f32),
            pltpu.VMEM((pairs, 128), f32),
            pltpu.VMEM((pairs, 128), f32),
            pltpu.VMEM((2, images, piece_width), f32),
            pltpu.VMEM((images, piece_width), f32),
            pltpu.VMEM((chips, images, piece_width), f32),
            pltpu.VMEM((2, images, piece_width), f32),
            dma((len(given),)),
            dma((chips, PIECES)),
            dma((chips,)),
            dma((PIECES + 1,)),
            pltpu.SemaphoreType.REGULAR((LINE - 2,)),
            dma((3,)),
            dma((3,)),
        ],
        compiler_params=pltpu.CompilerParams(
            collective_id=0, has_side_effects=True, vmem_limit_bytes=60 << 20
        ),
    )(*given)


def takes_kernel(mesh, patches):
    count = mesh.shape["sample"]
    rows = patches.shape[1] // count
    images = patches.shape[0] // mesh.shape["group"]
    return count == PLANE * LINE and rows % TILE_ROWS == 0 and images * rows == 128


def solution(mesh):
    placed = (
        P("group", "sample", None),
        P("sample", None, None),
        P("sample", None),
        P("sample", None, None),
        P("sample", None),
        P("sample", None),
        P("sample", None, None),
        P("sample", None, None),
        P("sample", None, None),
        P("sample", None, None),
        P("sample", None),
        P("sample", None),
        P("sample", None, None),
        P("sample", None),
    )

    def run(*arrays):
        step = kernel_shards if takes_kernel(mesh, arrays[0]) else shards
        return jax.shard_map(
            step, mesh=mesh, in_specs=placed, out_specs=P("group", None), check_vma=False
        )(*arrays)

    return run
```

```python
import functools
import math

import jax
import jax.numpy as jnp
from jax import lax
from jax.experimental import pallas as pl
from jax.experimental.pallas import tpu as pltpu
from jax.sharding import PartitionSpec as P

HEAD_DIM = 80


epsilon = 1e-06


def combined_all(part, axis, combine):
    gathered = jax.tree.map(lambda a: lax.all_gather(a, axis), part)

    def take(source):
        return jax.tree.map(lambda a: lax.dynamic_index_in_dim(a, source, 0, False), gathered)

    return lax.fori_loop(
        1, lax.axis_size(axis), lambda source, state: combine(state, take(source)), take(0)
    )


def layer_norm(values, gain, shift):
    center = values - jnp.mean(values, axis=-1, keepdims=True)
    spread = jnp.mean(center * center, axis=-1, keepdims=True)
    return center * lax.rsqrt(spread + epsilon) * gain + shift


def shards(
    patches,
    patch_weight,
    cls_token,
    pos_embed,
    ln1_gain,
    ln1_bias,
    w_query,
    w_key,
    w_value,
    w_out,
    lnf_gain,
    lnf_bias,
    head_w,
    head_bias,
):
    embed_weight = patch_weight[0]
    position = pos_embed[0]
    gain_first = ln1_gain[0]
    bias_first = ln1_bias[0]
    query_weight = w_query[0]
    pair_weight = jnp.concatenate([w_key[0], w_value[0]], axis=1)
    out_weight = w_out[0]
    width = embed_weight.shape[1]
    inner = query_weight.shape[1]
    head_count = inner // HEAD_DIM
    leading = cls_token[0].astype(jnp.float32) + position[0].astype(jnp.float32)
    lead_norm = layer_norm(leading, gain_first, bias_first).astype(jnp.bfloat16)
    lead_pair = jnp.dot(lead_norm[None], pair_weight, preferred_element_type=jnp.float32).astype(
        jnp.bfloat16
    )
    query = jnp.dot(lead_norm[None], query_weight, preferred_element_type=jnp.float32).astype(
        jnp.bfloat16
    )
    query = query.reshape(head_count, HEAD_DIM)
    portion = lax.all_gather(patches, "sample", axis=1, tiled=True)
    image_count = portion.shape[0]
    row_count = portion.shape[1]
    flat = portion.reshape(-1, portion.shape[2])
    tokens = jnp.dot(flat, embed_weight, preferred_element_type=jnp.float32).reshape(
        image_count, row_count, width
    )
    placed = lax.dynamic_slice_in_dim(position, 1, row_count, 0)
    tokens = tokens + placed.astype(jnp.float32)[None]
    normed = layer_norm(tokens, gain_first, bias_first).astype(jnp.bfloat16)
    paired = jnp.dot(normed.reshape(-1, width), pair_weight, preferred_element_type=jnp.float32)
    key_values = paired.astype(jnp.bfloat16).reshape(image_count, row_count, 2 * inner)
    image_count = key_values.shape[0]
    lead_rows = jnp.broadcast_to(lead_pair[None], (image_count, 1, 2 * inner))
    full_rows = jnp.concatenate([lead_rows, key_values], axis=1)
    key_rows = full_rows[:, :, :inner].reshape(image_count, -1, head_count, HEAD_DIM)
    value_rows = full_rows[:, :, inner:].reshape(image_count, -1, head_count, HEAD_DIM)
    scores = jnp.einsum(
        "hd,ithd->iht", query, key_rows, preferred_element_type=jnp.float32
    ) / math.sqrt(HEAD_DIM)
    attention = jax.nn.softmax(scores, axis=-1).astype(jnp.bfloat16)
    mixed = jnp.einsum("iht,ithd->ihd", attention, value_rows, preferred_element_type=jnp.float32)
    mixed = mixed.astype(jnp.bfloat16).reshape(image_count, inner)
    hidden = leading[None] + jnp.dot(mixed, out_weight, preferred_element_type=jnp.float32)
    final = layer_norm(hidden, lnf_gain[0], lnf_bias[0]).astype(jnp.bfloat16)
    logits = jnp.dot(final, head_w[0], preferred_element_type=jnp.float32) + head_bias[0]
    logp = jax.nn.log_softmax(logits, axis=-1)
    count = lax.axis_size("sample")

    def combine(earlier, later):
        highest = jnp.maximum(earlier[0], later[0])
        summed = earlier[1] * jnp.exp(earlier[0] - highest) + later[1] * jnp.exp(later[0] - highest)
        return (highest, summed)

    peak, total = combined_all((logp, jnp.ones_like(logp)), "sample", combine)
    return peak + jnp.log(total) - math.log(count)


MESH = pl.DeviceIdType.MESH
PLANE = 4
LINE = 4
TILE_ROWS = 16
LOWEST = -1e30
GRAM_PARTS = 2
FOLD_PARTS = 3


def split_in_two(values):
    high = values.astype(jnp.bfloat16)
    low = (values - high.astype(jnp.float32)).astype(jnp.bfloat16)
    return jnp.concatenate([high, low], axis=0)


PIECES = 4
SENDS = (
    (
        (1,1,0,1,3), (0,0,0,1,3), (1,1,0,1,1), (0,0,0,1,0), (0,0,0,1,2), (1,1,0,1,2), (0,2,0,1,0),
        (0,2,0,1,1), (0,2,0,1,2), (0,2,0,1,3), (2,1,0,1,1), (2,1,0,1,0), (2,1,0,1,2), (0,2,0,0,3),
        (0,0,1,1,0), (0,2,1,1,0), (0,2,0,0,0), (0,0,1,1,2), (0,2,1,1,2), (1,1,0,1,0), (1,1,0,0,2),
        (0,2,0,0,2), (0,0,1,1,3), (0,2,1,1,3), (0,2,1,1,1), (0,0,0,1,1), (0,2,1,0,0), (0,0,2,1,0),
        (0,2,2,1,0), (0,2,1,0,2), (0,2,1,0,3), (0,2,2,1,1), (0,0,2,1,2), (0,2,2,1,2), (0,0,3,1,3),
        (0,2,3,1,3), (0,0,2,1,3), (0,2,2,1,3), (3,1,0,0,1), (0,2,0,0,1), (0,2,1,0,1), (0,2,2,0,0),
        (0,0,3,1,1), (0,2,3,1,1), (0,0,3,1,0), (0,2,3,1,0), (0,2,2,0,2), (0,2,2,0,1), (0,0,3,1,2),
        (0,2,3,1,2), (0,2,3,0,3), (0,2,2,0,3), (0,2,3,0,1), (0,2,3,0,0), (0,2,3,0,2),
    ),
    (
        (1,0,1,1,3), (0,1,1,1,0), (1,0,1,1,0), (2,1,1,1,2), (1,0,1,1,2), (2,1,1,1,0), (0,1,1,1,2),
        (1,0,1,1,1), (0,1,1,1,3), (0,1,1,1,1), (1,2,1,1,0), (1,2,1,1,1), (1,2,1,1,2), (1,2,1,1,3),
        (3,1,1,1,1), (3,1,1,1,3), (1,0,0,1,3), (2,1,0,1,3), (1,2,0,1,3), (2,1,1,0,3), (1,2,1,0,3),
        (2,1,1,1,3), (1,0,0,1,1), (1,2,0,1,1), (1,2,1,0,0), (1,0,2,1,0), (0,1,2,1,0), (2,1,1,1,1),
        (1,2,2,1,0), (1,2,0,1,2), (1,2,1,0,2), (0,1,2,1,2), (1,0,2,1,2), (1,2,2,1,2), (0,1,1,0,1),
        (2,1,1,0,1), (1,2,1,0,1), (1,0,2,1,1), (1,2,2,1,1), (1,2,0,0,3), (1,0,3,1,1), (0,1,3,1,1),
        (1,2,3,1,1), (1,2,0,0,1), (1,0,0,1,0), (1,2,0,1,0), (1,0,3,1,0), (0,1,3,1,0), (1,2,3,1,0),
        (1,2,2,0,0), (1,2,0,0,2), (1,0,3,1,2), (0,1,3,1,2), (1,2,3,1,2), (1,2,2,0,2), (1,2,2,0,1),
        (1,2,2,0,3), (1,2,3,0,1), (1,0,3,1,3), (1,2,3,1,3), (1,2,0,0,0), (1,2,2,1,3), (1,2,3,0,0),
        (1,2,3,0,2), (1,2,3,0,3),
    ),
    (
        (2,0,2,1,2), (2,0,2,1,3), (2,0,2,1,0), (3,1,2,1,2), (1,1,2,1,0), (3,1,2,1,0), (1,1,2,1,2),
        (1,1,2,1,1), (2,0,2,1,1), (3,1,2,1,3), (3,1,2,1,1), (2,2,2,1,0), (2,2,2,1,1), (2,2,2,1,2),
        (2,2,2,1,3), (0,1,2,1,1), (0,1,2,1,3), (3,1,1,1,2), (2,0,1,1,2), (2,2,1,1,2), (3,1,1,1,0),
        (2,0,1,1,0), (2,2,1,1,0), (2,2,2,0,2), (2,0,3,1,1), (2,2,3,1,1), (1,1,2,0,3), (2,2,2,0,3),
        (2,0,0,1,1), (3,1,0,1,1), (2,2,0,1,1), (2,0,3,1,3), (1,1,3,1,3), (2,2,3,1,3), (2,2,2,0,0),
        (2,0,0,1,0), (3,1,0,1,0), (2,2,0,1,0), (1,1,2,1,3), (2,2,3,1,2), (0,1,2,0,1), (2,2,2,0,1),
        (3,1,0,1,2), (2,0,0,1,2), (2,2,0,1,2), (2,2,1,0,2), (2,2,1,0,0), (2,2,3,0,1), (2,0,0,1,3),
        (3,1,0,1,3), (2,2,0,1,3), (2,2,1,0,3), (2,2,0,0,1), (2,2,1,1,3), (2,2,3,0,3), (2,0,3,1,0),
        (2,2,3,1,0), (2,2,1,1,1), (2,2,0,0,0), (2,2,3,0,2), (2,2,1,0,1), (2,2,0,0,2), (2,2,0,0,3),
        (2,2,3,0,0),
    ),
    (
        (3,0,3,1,1), (2,1,3,1,1), (3,0,3,1,0), (2,1,3,1,3), (3,0,3,1,2), (2,1,3,1,2), (3,0,3,1,3),
        (3,2,3,1,0), (3,2,3,1,1), (3,2,3,1,2), (3,2,3,1,3), (1,1,3,1,1), (1,1,3,1,0), (1,1,3,1,2),
        (0,1,3,1,3), (3,0,2,1,2), (3,2,2,1,2), (3,2,3,0,1), (3,0,2,1,0), (3,2,2,1,0), (3,2,3,0,0),
        (3,0,2,1,3), (3,2,2,1,3), (2,1,3,1,0), (2,1,3,0,2), (3,2,3,0,2), (3,0,2,1,1), (3,2,2,1,1),
        (3,2,3,0,3), (3,0,1,1,1), (3,2,1,1,1), (3,2,2,0,2), (3,0,1,1,3), (3,2,1,1,3), (3,2,2,0,0),
        (3,0,1,1,2), (3,2,1,1,2), (3,0,1,1,0), (3,2,1,1,0), (3,2,2,0,3), (3,2,0,1,1), (3,2,2,0,1),
        (3,0,0,1,0), (3,2,0,1,0), (3,2,1,0,1), (3,0,0,1,2), (3,2,0,1,2), (3,2,1,0,3), (3,0,0,1,3),
        (3,2,0,1,3), (3,2,1,0,2), (3,2,1,0,0), (3,2,0,0,0), (3,2,0,0,2), (3,2,0,0,3), (3,2,0,0,1),
    ),
)
EVENTS = (
    (
        ((-1,0,0,0,10),), (), (), ((-2,2,0,10,3),), (), (), ((-2,3,0,13,0),(0,0,3,13,1)),
        ((1,1,0,14,2),(0,0,0,16,1)), ((1,1,2,17,2),(0,0,2,19,3),(1,1,3,22,2)), ((1,1,1,24,1),),
        ((1,0,0,25,2),),
        ((2,1,0,27,2),(1,0,2,29,1),(1,0,3,30,1),(2,1,1,31,1),(2,1,2,32,2),(3,1,3,34,2),(2,1,3,36,2)),
        ((0,0,1,38,2),(1,0,1,40,1),(2,0,0,41,1),(3,1,1,42,2)), ((3,1,0,44,2),),
        ((2,0,2,46,1),(2,0,1,47,1),(3,1,2,48,2),(3,0,3,50,1)), (), ((2,0,3,51,1),), (), ((3,0,1,52,1),), (),
        ((3,0,0,53,1),), ((3,0,2,54,1),),
    ),
    (
        ((-1,0,0,0,14),), (), (), (), ((-2,3,0,14,2),), (), ((0,1,3,16,3),(1,0,3,19,2)),
        ((0,1,1,21,3),(1,0,0,24,1),(2,1,0,25,4),(0,1,2,29,1)), ((1,0,2,30,1),(2,1,2,31,3)),
        ((1,0,1,34,3),(2,1,1,37,2)), ((0,0,3,39,1),(3,1,1,40,3),(0,0,1,43,1)),
        ((0,1,0,44,2),(3,1,0,46,3),(2,0,0,49,1),(0,0,2,50,1)), ((3,1,2,51,3),(2,0,2,54,1),(2,0,1,55,1)),
        ((2,0,3,56,1),(3,0,1,57,1),(3,1,3,58,2)), ((0,0,0,60,1),(2,1,3,61,1),(3,0,0,62,1)), (),
        ((3,0,2,63,1),), (), ((3,0,3,64,1),), (), (), (),
    ),
    (
        ((-1,0,0,0,15),), ((-2,0,0,15,2),), (), (), (), ((1,1,2,17,3),), ((1,1,0,20,3),(2,0,2,23,1)),
        ((3,1,1,24,2),(2,0,3,26,2)), ((0,1,1,28,3),(3,1,3,31,3),(2,0,0,34,1),(0,1,0,35,3)),
        ((3,1,2,38,2),(2,0,1,40,2),(0,1,2,42,3),(1,0,2,45,1)), ((1,0,0,46,1),(3,0,1,47,1),(0,1,3,48,3)),
        ((1,0,3,51,1),(0,0,1,52,1)), ((1,1,3,53,1),(3,0,3,54,1),(3,1,0,55,2)),
        ((1,1,1,57,1),(0,0,0,58,1),(3,0,2,59,1),(1,0,1,60,1),(0,0,2,61,1)), ((0,0,3,62,1),), (), (), (),
        ((3,0,0,63,1),), (), (), (),
    ),
    (
        ((-1,0,0,0,11),), ((-2,1,0,11,3),(-2,0,0,14,1)), (), (), (), ((2,1,2,15,2),),
        ((3,0,1,17,1),(2,1,0,18,2)), ((3,0,0,20,1),(2,1,3,21,2)), ((3,0,2,23,3),(2,1,1,26,2)),
        ((3,0,3,28,1),(1,1,1,29,2),(2,0,2,31,1)), ((1,1,3,32,2),(2,0,0,34,1),(1,1,2,35,2)),
        ((1,1,0,37,2),(2,0,3,39,1)), ((0,1,1,40,1),(2,0,1,41,1),(0,1,0,42,2)), ((1,0,1,44,1),(0,1,2,45,2)),
        ((1,0,3,47,1),(0,1,3,48,2)), (), ((1,0,2,50,1),(1,0,0,51,1)), (), ((0,0,0,52,1),), (),
        ((0,0,2,53,1),), ((0,0,3,54,1),(0,0,1,55,1)),
    ),
)
ORDER = (13869401, 13924435, 12664421, 575407)


def contract_last(left, right):
    return lax.dot_general(
        left, right, (((1,), (1,)), ((), ())), preferred_element_type=jnp.float32
    )


def whole_kernel(
    count,
    heads,
    patches,
    cls_token,
    pos_embed,
    ln1_gain,
    ln1_bias,
    patch_weight,
    w_query,
    w_key,
    w_value,
    w_out,
    head_w,
    lnf_gain,
    lnf_bias,
    head_bias,
    out,
    own_patches,
    cls_row,
    position,
    gain_row,
    bias_row,
    embed,
    query_w,
    key_w,
    value_w,
    out_w,
    class_w,
    last_gain,
    last_bias,
    class_bias,
    slots,
    basis,
    scaled,
    form,
    folded,
    ends,
    constants,
    kept,
    gathered,
    peak,
    total,
    part,
    from_pair,
    ring,
    result,
    load_sem,
    recv_sem,
    twin_sem,
    sent_sem,
    known_sem,
    tail_send,
    tail_recv,
):
    f32, bf16 = jnp.float32, jnp.bfloat16
    me = lax.axis_index("sample")
    core = me % 2
    side = (me // 2) % 2
    chip = me // 2
    chips = count // 2
    plane = me // PLANE
    images, rows, depth = own_patches.shape
    padded = slots.shape[1]
    lanes = slots.shape[2]
    tiles = padded // TILE_ROWS
    cuts = tuple(TILE_ROWS * (tiles * place // PIECES) for place in range(PIECES + 1))
    width = embed.shape[1]
    inner = query_w.shape[1]
    head_dim = inner // heads
    pairs = heads * images
    spots = basis.shape[0] - 2 * heads - padded
    held_rows = position.shape[0]

    loads = []
    for index, (source, target) in enumerate(
        (
            (patches, own_patches),
            (pos_embed.at[0], position),
            (cls_token, cls_row),
            (ln1_gain, gain_row),
            (ln1_bias, bias_row),
            (patch_weight.at[0], embed),
            (w_query.at[0], query_w),
            (w_key.at[0], key_w),
            (w_value.at[0], value_w),
            (w_out.at[0], out_w),
            (head_w.at[0], class_w),
            (lnf_gain, last_gain),
            (lnf_bias, last_bias),
            (head_bias, class_bias),
        )
    ):
        loads.append(pltpu.make_async_copy(source, target, load_sem.at[index]))
    for load in loads[:5]:
        load.start()

    twin = me + 1 - 2 * core
    beside = plane * PLANE + (1 - side) * 2 + core
    here = tuple(lax.convert_element_type(plane == place, jnp.int32) for place in range(LINE))
    line_of = tuple(
        (place * PLANE + (1 - side) * 2 + core, place * PLANE + side * 2 + core)
        for place in range(LINE)
    )

    barrier = pltpu.get_barrier_semaphore()

    def greet(target):
        pl.semaphore_signal(barrier, inc=1, device_id={"sample": target}, device_id_type=MESH)

    greet(twin)
    greet(beside)

    @pl.when(plane > 0)
    def _():
        greet(me - PLANE)

    @pl.when(plane < LINE - 1)
    def _():
        greet(me + PLANE)

    loads[0].wait()
    for load in loads[5:7]:
        load.start()
    eye = (
        lax.broadcasted_iota(jnp.int32, (padded, depth), 0)
        == lax.broadcasted_iota(jnp.int32, (padded, depth), 1)
    ).astype(bf16)
    flat = own_patches[...].reshape(images * rows, depth)
    slots[me] = contract_last(eye, flat).astype(bf16)
    pl.semaphore_wait(barrier, LINE - here[0] - here[LINE - 1])

    def passing(ref, target, sent_by, got_by):
        return pltpu.make_async_remote_copy(
            src_ref=ref,
            dst_ref=ref,
            send_sem=sent_by,
            recv_sem=got_by,
            device_id={"sample": target},
            device_id_type=MESH,
        )

    def rows_of(part_of):
        return pl.ds(cuts[part_of], cuts[part_of + 1] - cuts[part_of])

    def sent(place, slot):
        to, aside, origin, own, part_of = SENDS[place][slot]
        inside = aside // 2
        source = line_of[origin][own]
        got_by = twin_sem.at[source // 2] if inside else recv_sem.at[source // 2, part_of]
        target = twin if inside else line_of[to][aside]
        ref = slots.at[source, rows_of(part_of)]
        return passing(ref, target, sent_sem.at[PIECES if inside else part_of], got_by)

    def got(source, part_of):
        ref = slots.at[source, rows_of(part_of)]
        passing(ref, twin, sent_sem.at[0], recv_sem.at[source // 2, part_of]).wait_recv()

    def got_from_twin(base):
        ref = slots.at[base + 1 - core]
        passing(ref, twin, sent_sem.at[0], twin_sem.at[base // 2]).wait_recv()

    def all_sent(place):
        for part_of in range(PIECES):
            number = sum(1 for entry in SENDS[place] if entry[1] < 2 and entry[4] == part_of)
            ref = slots.at[pl.ds(0, number), rows_of(part_of)]
            passing(ref, twin, sent_sem.at[part_of], twin_sem.at[0]).wait_send()
        ref = slots.at[pl.ds(0, chips)]
        passing(ref, twin, sent_sem.at[PIECES], twin_sem.at[0]).wait_send()

    def tell(target, far):
        pl.semaphore_signal(
            known_sem.at[far], inc=1, device_id={"sample": target}, device_id_type=MESH
        )

    def learn(place, entered):
        pl.semaphore_wait(known_sem.at[abs(entered - place) - 2], 1)
        if place == 1 and entered == 3:
            tell(me - PLANE, 1)
        if place == 2 and entered == 0:
            tell(me + PLANE, 1)

    for place in (1, 2):

        @pl.when(plane == place)
        def _(place=place):
            tell(me - PLANE, 0)
            tell(me + PLANE, 0)

    def events_at(place, group):
        for origin, own, part_of, low, number in EVENTS[place][group]:
            if origin == -2:
                learn(place, own)
            if origin >= 0:
                got(line_of[origin][own], part_of)
            for slot in range(low, low + number):
                sent(place, slot).start()

    def narrowed(value, low, high, act, busy):
        live = [place for place in range(low, high) if busy(place)]
        if not live:
            return
        if high - low == 1:
            act(low)
            return
        middle = (low + high) // 2
        pl.when(value < middle)(lambda: narrowed(value, low, middle, act, busy))
        pl.when(value >= middle)(lambda: narrowed(value, middle, high, act, busy))

    def events(group):
        narrowed(
            plane,
            0,
            LINE,
            lambda place: events_at(place, group),
            lambda place: bool(EVENTS[place][group]),
        )

    events(0)
    for load in loads[7:]:
        load.start()

    for index in (1, 2, 3, 4):
        loads[index].wait()
    events(1)
    gain = gain_row[...]
    bias = bias_row[...]
    leading = cls_row[...].astype(f32) + position[0:1, :].astype(f32)
    lead = jnp.broadcast_to(layer_norm(leading, gain, bias), (TILE_ROWS, width)).astype(bf16)
    lead_row = lead[:1].astype(f32)

    events(2)
    placed = position[...].astype(f32)
    placed = placed - jnp.mean(placed, axis=1, keepdims=True)
    blank = jnp.zeros((spots - held_rows, width), f32)
    top = 2 * heads
    placed = jnp.concatenate([placed, blank], axis=0)
    basis[top + padded :, :] = placed.astype(bf16)
    bias_high = bias.astype(bf16).astype(f32)
    ending = jnp.concatenate([blank[3:], bias_high, bias - bias_high, lead_row], axis=0)
    ending = jnp.concatenate([jnp.zeros((held_rows, width), f32), ending], axis=0)
    scaled[padded:, :] = (placed * gain + ending).astype(bf16)
    weight = jnp.broadcast_to(jnp.sum(placed * placed, axis=1, keepdims=True), (spots, 128))
    weight = jnp.concatenate([weight, jnp.zeros((-spots % 128, 128), f32)], axis=0)
    weight = jnp.transpose(weight)[:1, :spots]

    loads[5].wait()
    table = embed[...].astype(f32)
    table = table - jnp.mean(table, axis=1, keepdims=True)
    table = jnp.concatenate([table, jnp.zeros((padded - depth, width), f32)], axis=0)
    basis[top : top + padded, :] = table.astype(bf16)
    scaled[:padded, :] = (table * gain).astype(bf16)

    events(3)
    loads[6].wait()
    query = jnp.dot(lead, query_w[...], preferred_element_type=f32)[:1]
    head_row = lax.broadcasted_iota(jnp.int32, (TILE_ROWS, inner), 0)
    column = lax.broadcasted_iota(jnp.int32, (TILE_ROWS, inner), 1)
    own_head = (column >= head_row * head_dim) & (column < (head_row + 1) * head_dim)
    spread = jnp.where(own_head, jnp.broadcast_to(query, (TILE_ROWS, inner)), 0.0).astype(bf16)
    events(4)
    loads[7].wait()
    turned = contract_last(spread, key_w[...])[:heads] * (1.0 / math.sqrt(head_dim))
    first = jnp.sum(turned * lead_row, axis=1, keepdims=True)
    level = jnp.sum(turned * bias, axis=1, keepdims=True)
    constants[...] = jnp.broadcast_to(level, constants.shape)
    basis[:top, :] = split_in_two(turned * gain)

    features = padded + spots
    for part_of in range(GRAM_PARTS):
        events(5 + part_of)
        low = 256 * (pl.cdiv(features, 256) * part_of // GRAM_PARTS)
        high = min(features, 256 * (pl.cdiv(features, 256) * (part_of + 1) // GRAM_PARTS))
        square = contract_last(basis[: top + padded, :], basis[top + low : top + high, :])
        place = low + lax.broadcasted_iota(jnp.int32, (padded, high - low), 1)
        form[top : top + padded, low:high] = jnp.where(
            place < padded, square[top:], 2.0 * square[top:]
        ).astype(bf16)
        form[:top, low:high] = split_in_two(square[:heads] + square[heads:top])
    sizes = jnp.concatenate([jnp.zeros((1, padded), f32), weight], axis=1)
    sizes_high = sizes.astype(bf16).astype(f32)
    sizes = jnp.concatenate(
        [sizes_high, sizes - sizes_high, jnp.zeros((TILE_ROWS - 2, padded + spots), f32)], axis=0
    )
    form[top + padded :, :] = sizes.astype(bf16)

    loads[8].wait()
    first = jnp.broadcast_to(first[None], (images, heads, 1)).reshape(pairs, 1)
    peak[...] = jnp.broadcast_to(first, peak.shape)
    total[...] = jnp.ones(total.shape, f32)
    gathered[...] = jnp.zeros(gathered.shape, f32)

    cells = 2 * lanes
    lane = lax.broadcasted_iota(jnp.int32, (pairs, cells), 1)
    row_image = lax.broadcasted_iota(jnp.int32, (pairs, cells), 0) // heads
    same = (lane % lanes) // rows == row_image
    spot_row = lax.broadcasted_iota(jnp.int32, (spots, cells), 0)
    spot_lane = lax.broadcasted_iota(jnp.int32, (spots, cells), 1)
    spot_at = spot_row - 1 - (spot_lane // lanes) * rows - spot_lane % rows

    order = sum(mine * packed for mine, packed in zip(here, ORDER, strict=True))
    first_step = 5 + GRAM_PARTS
    fold_rows = scaled.shape[0] // FOLD_PARTS

    def base_of(turn):
        code = (order >> (3 * turn)) % 8
        where, own = code // 2, code % 2
        return where * PLANE + 2 * (side * own + (1 - side) * (1 - own))

    def block_of(base):
        block = jnp.concatenate([slots[base], slots[base + 1]], axis=1)
        spot = jnp.where(spot_at == base * rows, 1.0, 0.0).astype(bf16)
        return jnp.concatenate([block, spot], axis=0)

    def front(base):
        block = block_of(base)
        image = jnp.dot(form[...], block, preferred_element_type=f32)
        norm = jnp.sum(
            image[top : top + padded] * block[:padded].astype(f32), axis=0, keepdims=True
        )
        tail = top + padded
        norm = norm + image[tail : tail + 1] + image[tail + 1 : tail + 2]
        rate = lax.rsqrt(norm * (1.0 / width) + epsilon)
        scores = image[:heads] + image[heads:top]
        kept[:heads, :] = scores * rate + constants[:, :1]
        kept[heads:, :] = jnp.broadcast_to(rate, (heads, cells))

    def back(base, scores, rate):
        block = block_of(base)
        scores = jnp.broadcast_to(scores[None], (images, heads, cells)).reshape(pairs, cells)
        scores = jnp.where(same, scores, LOWEST)
        before = peak[:, :1]
        now = jnp.maximum(before, jnp.max(scores, axis=1, keepdims=True))
        shrink = jnp.exp(before - now)
        chance = jnp.where(same, jnp.exp(scores - now), 0.0)
        peak[...] = jnp.broadcast_to(now, peak.shape)
        total[...] = total[...] * shrink + jnp.sum(chance, axis=1, keepdims=True)
        gathered[...] = gathered[...] * shrink + contract_last((chance * rate).astype(bf16), block)

    def fold(part_of):
        low = pl.multiple_of(part_of * fold_rows, TILE_ROWS)
        product = jnp.dot(
            scaled[pl.ds(low, fold_rows), :], value_w[...], preferred_element_type=f32
        )
        folded[pl.ds(low, fold_rows), :] = product.astype(bf16)
        ends[...] = product[fold_rows - ends.shape[0] :]

    def chip_step(turn, carry):
        narrowed(turn, 1, 2 * LINE, lambda index: events(first_step + 2 * index), lambda index: True)
        base = base_of(turn)
        got_from_twin(base)
        scores = kept[:heads, :]
        rate = kept[heads : heads + 1, :]
        back(base_of(turn - 1), scores, rate)
        front(base)

        narrowed(
            turn,
            1,
            2 * LINE,
            lambda index: events(first_step + 2 * index + 1),
            lambda index: index < 2 * LINE - 1,
        )

        @pl.when(turn < FOLD_PARTS)
        def _():
            fold(turn)

        return carry

    events(first_step)
    got_from_twin(base_of(0))
    front(base_of(0))
    events(first_step + 1)
    fold(0)
    lax.fori_loop(1, 2 * LINE, chip_step, 0)
    back(base_of(2 * LINE - 1), kept[:heads, :], kept[heads : heads + 1, :])

    last = ends.shape[0]
    plain = ends[last - 3 : last - 2, :] + ends[last - 2 : last - 1, :]
    lead_value = ends[last - 1 :, :]
    values = jnp.dot(
        gathered[...].astype(bf16), folded[...], preferred_element_type=f32
    )
    share = 1.0 / total[:, :1]
    lead_chance = jnp.exp(first - peak[:, :1]) * share
    values = values * share
    values = values + plain + (lead_value - plain) * lead_chance
    pair_head = lax.broadcasted_iota(jnp.int32, (pairs, inner), 0) % heads
    pair_column = lax.broadcasted_iota(jnp.int32, (pairs, inner), 1)
    mine_only = (pair_column >= pair_head * head_dim) & (pair_column < (pair_head + 1) * head_dim)
    values = jnp.where(mine_only, values, 0.0)
    mixed = jnp.sum(values.reshape(images, heads, inner), axis=1).astype(bf16)
    loads[9].wait()
    hidden = leading + jnp.dot(mixed, out_w[...], preferred_element_type=f32)
    for index in (10, 11, 12, 13):
        loads[index].wait()
    center = hidden - jnp.mean(hidden, axis=-1, keepdims=True)
    shift = last_bias[...]
    shift_high = shift.astype(bf16)
    shift_low = (shift - shift_high.astype(f32)).astype(bf16)
    rows_in = jnp.concatenate(
        [
            center * last_gain[...],
            shift_high.astype(f32),
            shift_low.astype(f32),
            jnp.zeros((TILE_ROWS - images - 2, width), f32),
        ],
        axis=0,
    ).astype(bf16)
    spread_out = jnp.mean(center * center, axis=-1, keepdims=True)
    products = contract_last(rows_in, class_w[...])
    moved = products[images : images + 1] + products[images + 1 : images + 2] + class_bias[...]
    logits = products[:images] * lax.rsqrt(spread_out + epsilon) + moved
    lifted = logits - jnp.max(logits, axis=-1, keepdims=True)
    logp = lifted - jnp.log(jnp.sum(jnp.exp(lifted), axis=-1, keepdims=True))

    piece_width = part.shape[2]
    classes = out.shape[1]
    part[0] = logp[:, :piece_width]
    part[1] = jnp.concatenate(
        [logp[:, piece_width:], jnp.zeros((images, 2 * piece_width - classes), f32)], axis=1
    )
    swap = pltpu.make_async_remote_copy(
        src_ref=part.at[1 - core],
        dst_ref=from_pair,
        send_sem=tail_send.at[0],
        recv_sem=tail_recv.at[0],
        device_id={"sample": twin},
        device_id_type=MESH,
    )
    swap.start()
    swap.wait_recv()
    mine = part[core]
    theirs = from_pair[...]
    high = jnp.maximum(mine, theirs)
    ring[chip] = high + jnp.log(jnp.exp(mine - high) + jnp.exp(theirs - high))

    def pass_on(ref, target):
        return passing(ref, target, tail_send.at[2], tail_recv.at[2])

    for step in range(1, chips):
        other = step - 1 + jnp.minimum(step // jnp.maximum(chip + 1, 1), 1)
        pass_on(ring.at[chip], 2 * other + core).start()
    pass_on(ring.at[pl.ds(0, chips - 1)], twin).wait_recv()
    every = ring[...]
    high = jnp.max(every, axis=0)
    result[core] = high + jnp.log(jnp.sum(jnp.exp(every - high[None]), axis=0)) - math.log(count)
    share = pltpu.make_async_remote_copy(
        src_ref=result.at[core],
        dst_ref=result.at[core],
        send_sem=tail_send.at[1],
        recv_sem=tail_recv.at[1],
        device_id={"sample": twin},
        device_id_type=MESH,
    )
    share.start()

    for place in range(LINE):

        @pl.when(plane == place)
        def _(place=place):
            all_sent(place)

    swap.wait_send()
    pass_on(ring.at[pl.ds(0, chips - 1)], twin).wait_send()
    pltpu.make_async_remote_copy(
        src_ref=result.at[core],
        dst_ref=result.at[1 - core],
        send_sem=tail_send.at[1],
        recv_sem=tail_recv.at[1],
        device_id={"sample": twin},
        device_id_type=MESH,
    ).wait_recv()
    share.wait_send()
    out[:, :piece_width] = result[0]
    out[:, piece_width:] = result[1][:, : classes - piece_width]


def kernel_shards(
    patches,
    patch_weight,
    cls_token,
    pos_embed,
    ln1_gain,
    ln1_bias,
    w_query,
    w_key,
    w_value,
    w_out,
    lnf_gain,
    lnf_bias,
    head_w,
    head_bias,
):
    count = lax.axis_size("sample")
    images, rows, depth = patches.shape
    width = patch_weight.shape[2]
    inner = w_query.shape[2]
    heads = inner // HEAD_DIM
    pairs = heads * images
    chips = count // 2
    classes = head_w.shape[2]
    piece_width = pl.cdiv(classes, 256) * 128
    padded = pl.cdiv(depth, TILE_ROWS) * TILE_ROWS
    tall = FOLD_PARTS * TILE_ROWS
    features = pl.cdiv(padded + pos_embed.shape[1] + 3, tall) * tall
    far = pl.BlockSpec(memory_space=pl.ANY)
    dma = pltpu.SemaphoreType.DMA
    f32, bf16 = jnp.float32, jnp.bfloat16
    class_rows = jnp.swapaxes(head_w, 1, 2)
    given = (
        patches,
        cls_token,
        pos_embed,
        ln1_gain,
        ln1_bias,
        patch_weight,
        w_query,
        w_key,
        w_value,
        w_out,
        class_rows,
        lnf_gain,
        lnf_bias,
        head_bias,
    )
    held = [
        pltpu.VMEM(a.shape[1:] if place and a.ndim == 3 else a.shape, a.dtype)
        for place, a in enumerate(given)
    ]
    return pl.pallas_call(
        functools.partial(whole_kernel, count, heads),
        out_shape=pltpu.VMEM((images, classes), f32),
        in_specs=[far] * len(given),
        out_specs=pl.BlockSpec(memory_space=pltpu.VMEM),
        scratch_shapes=[
            *held,
            pltpu.VMEM((count, padded, images * rows), bf16),
            pltpu.VMEM((2 * heads + features, width), bf16),
            pltpu.VMEM((features, width), bf16),
            pltpu.VMEM((padded + 2 * heads + TILE_ROWS, features), bf16),
            pltpu.VMEM((features, inner), bf16),
            pltpu.VMEM((TILE_ROWS, inner), f32),
            pltpu.VMEM((heads, 128), f32),
            pltpu.VMEM((2 * heads, 2 * images * rows), f32),
            pltpu.VMEM((pairs, features), f32),
            pltpu.VMEM((pairs, 128), f32),
            pltpu.VMEM((pairs, 128), f32),
            pltpu.VMEM((2, images, piece_width), f32),
            pltpu.VMEM((images, piece_width), f32),
            pltpu.VMEM((chips, images, piece_width), f32),
            pltpu.VMEM((2, images, piece_width), f32),
            dma((len(given),)),
            dma((chips, PIECES)),
            dma((chips,)),
            dma((PIECES + 1,)),
            pltpu.SemaphoreType.REGULAR((LINE - 2,)),
            dma((3,)),
            dma((3,)),
        ],
        compiler_params=pltpu.CompilerParams(
            collective_id=0, has_side_effects=True, vmem_limit_bytes=60 << 20
        ),
    )(*given)


def takes_kernel(mesh, patches):
    count = mesh.shape["sample"]
    rows = patches.shape[1] // count
    images = patches.shape[0] // mesh.shape["group"]
    return count == PLANE * LINE and rows % TILE_ROWS == 0 and images * rows == 128


def solution(mesh):
    placed = (
        P("group", "sample", None),
        P("sample", None, None),
        P("sample", None),
        P("sample", None, None),
        P("sample", None),
        P("sample", None),
        P("sample", None, None),
        P("sample", None, None),
        P("sample", None, None),
        P("sample", None, None),
        P("sample", None),
        P("sample", None),
        P("sample", None, None),
        P("sample", None),
    )

    def run(*arrays):
        step = kernel_shards if takes_kernel(mesh, arrays[0]) else shards
        return jax.shard_map(
            step, mesh=mesh, in_specs=placed, out_specs=P("group", None), check_vma=False
        )(*arrays)

    return run
```
